32 devices in a mesh: rep: 1 (over z), dp: 32 (over x, y, core).
Axes of the slice: x: 4, y: 4, z: 1, core: 2. Of those that a mesh axis runs over, the one named last changes fastest.
The devices are a block of a 4x4x8 slice.
Arguments:
- x: bfloat16 [32, 2048, 512], P(('rep', 'dp'))
- dy: bfloat16 [32, 2048, 512], P(('rep', 'dp'))
- wq: bfloat16 [2, 512, 768], replicated
- wk: bfloat16 [2, 512, 128], replicated
- wv: bfloat16 [2, 512, 128], replicated
- wo: bfloat16 [2, 768, 512], replicated
- w_gate: bfloat16 [2, 512, 2048], replicated
- w_up: bfloat16 [2, 512, 2048], replicated
- w_down: bfloat16 [2, 2048, 512], replicated
- m_wq: float32 [2, 512, 768], P(None, 'dp')
- m_wk: float32 [2, 512, 128], P(None, 'dp')
- m_wv: float32 [2, 512, 128], P(None, 'dp')
- m_wo: float32 [2, 768, 512], P(None, 'dp')
- m_w_gate: float32 [2, 512, 2048], P(None, 'dp')
- m_w_up: float32 [2, 512, 2048], P(None, 'dp')
- m_w_down: float32 [2, 2048, 512], P(None, 'dp')
- v_wq: float32 [2, 512, 768], P(None, 'dp')
- v_wk: float32 [2, 512, 128], P(None, 'dp')
- v_wv: float32 [2, 512, 128], P(None, 'dp')
- v_wo: float32 [2, 768, 512], P(None, 'dp')
- v_w_gate: float32 [2, 512, 2048], P(None, 'dp')
- v_w_up: float32 [2, 512, 2048], P(None, 'dp')
- v_w_down: float32 [2, 2048, 512], P(None, 'dp')
Outputs:
- output 1: bfloat16 [2, 512, 768], P('rep')
- output 2: bfloat16 [2, 512, 128], P('rep')
- output 3: bfloat16 [2, 512, 128], P('rep')
- output 4: bfloat16 [2, 768, 512], P('rep')
- output 5: bfloat16 [2, 512, 2048], P('rep')
- output 6: bfloat16 [2, 512, 2048], P('rep')
- output 7: bfloat16 [2, 2048, 512], P('rep')
- output 8: float32 [2, 512, 768], P('rep', 'dp')
- output 9: float32 [2, 512, 128], P('rep', 'dp')
- output 10: float32 [2, 512, 128], P('rep', 'dp')
- output 11: float32 [2, 768, 512], P('rep', 'dp')
- output 12: float32 [2, 512, 2048], P('rep', 'dp')
- output 13: float32 [2, 512, 2048], P('rep', 'dp')
- output 14: float32 [2, 2048, 512], P('rep', 'dp')
- output 15: float32 [2, 512, 768], P('rep', 'dp')
- output 16: float32 [2, 512, 128], P('rep', 'dp')
- output 17: float32 [2, 512, 128], P('rep', 'dp')
- output 18: float32 [2, 768, 512], P('rep', 'dp')
- output 19: float32 [2, 512, 2048], P('rep', 'dp')
- output 20: float32 [2, 512, 2048], P('rep', 'dp')
- output 21: float32 [2, 2048, 512], P('rep', 'dp')
All inputs are finite; a program needn't handle non-finite values.
Results may differ from the reference program's by a relative error of at most 0.024.
Values are sent between devices in bfloat16 or wider.
A program may use at most 768 MiB of HBM per device.

```python
import jax
import jax.numpy as jnp
from jax import lax

SEQUENCES = 32
TOKENS = 2048
D = 512
HEADS = 6
KV_HEADS = 1
HEAD = 128
FF = 2048
LAYERS = 2
THETA = 10000
NAMES = ("wq", "wk", "wv", "wo", "w_gate", "w_up", "w_down")
SHAPES = {
    "wq": (LAYERS, D, HEADS * HEAD),
    "wk": (LAYERS, D, KV_HEADS * HEAD),
    "wv": (LAYERS, D, KV_HEADS * HEAD),
    "wo": (LAYERS, HEADS * HEAD, D),
    "w_gate": (LAYERS, D, FF),
    "w_up": (LAYERS, D, FF),
    "w_down": (LAYERS, FF, D),
}


def bump(key, n, height):
    away = (jnp.arange(n, dtype=jnp.int32) - jax.random.randint(key, (), 0, n, jnp.int32)) % n
    return jnp.where(away < n // 8, height, 1.0)


def together(key, own, strength):
    shared = jax.random.normal(key, own.shape[1:], jnp.float32)
    return (own + strength * shared) * lax.rsqrt(1 + strength * strength)


def setup_inputs(seed: int = 0, part: int = 0) -> dict:
    kx, kdy, ka, kb, kz, kf, kh, kl, *keys = jax.random.split(jax.random.key(seed), 8 + 3 * len(NAMES))
    kx, kdy, ka, kb = (jax.random.fold_in(k, part) for k in (kx, kdy, ka, kb))
    kw, km, kv = (keys[i::3] for i in range(3))
    shape = (SEQUENCES, TOKENS, D)
    much_x, much_dy = jax.random.uniform(kz, (2,), jnp.float32, 0.0, 1.0)
    loud = 2.0 ** jax.random.uniform(jax.random.fold_in(kz, 1), (), jnp.float32, -1.0, 2.0)
    layers = 2.0 ** jax.random.uniform(kl, (LAYERS, 1, 1), jnp.float32, -1.0, 1.0)
    times = {"wq": 1.0, "wk": 1.0, "wv": 2.0, "wo": layers, "w_gate": 1.0, "w_up": bump(kh, FF, 4.0), "w_down": layers}
    x = together(ka, jax.random.normal(kx, shape, jnp.float32), much_x) * bump(kf, D, 4.0)
    dy = together(kb, jax.random.normal(kdy, shape, jnp.float32), much_dy)
    drawn = {"x": x.astype(jnp.bfloat16), "dy": (loud * dy * (SEQUENCES * TOKENS) ** -0.5).astype(jnp.bfloat16)}
    for key, name in zip(kw, NAMES, strict=True):
        drawn[name] = (jax.random.normal(key, SHAPES[name], jnp.float32) * SHAPES[name][1] ** -0.5 * times[name]).astype(jnp.bfloat16)
    for key, name in zip(km, NAMES, strict=True):
        drawn[f"m_{name}"] = 0.1 * jax.random.normal(key, SHAPES[name], jnp.float32)
    for key, name in zip(kv, NAMES, strict=True):
        drawn[f"v_{name}"] = jax.random.uniform(key, SHAPES[name], jnp.float32, 0.02, 0.06)
    return drawn


def matmul(a, w):
    return jnp.dot(a, w, preferred_element_type=jnp.float32).astype(jnp.bfloat16)


def normed(h):
    wide = h.astype(jnp.float32)
    scale = lax.rsqrt(jnp.mean(wide**2, -1, keepdims=True) + 1e-6)
    return (wide * scale).astype(jnp.bfloat16)


def turned(t, theta):
    half = t.shape[-1] // 2
    angle = jnp.arange(t.shape[0], dtype=jnp.float32)[:, None] * theta ** (-jnp.arange(half, dtype=jnp.float32) / half)
    cos, sin = jnp.cos(angle)[:, None], jnp.sin(angle)[:, None]
    a, b = t[..., :half].astype(jnp.float32), t[..., half:].astype(jnp.float32)
    return jnp.concatenate([a * cos - b * sin, b * cos + a * sin], -1).astype(jnp.bfloat16)


def seen_by(q, k, v):
    tokens, kv = q.shape[0], k.shape[1]
    q = q.reshape(tokens, kv, -1, q.shape[-1])
    scores = jnp.einsum("tgsd,ugd->gstu", q.astype(jnp.float32), k.astype(jnp.float32)) * q.shape[-1] ** -0.5
    place = jnp.arange(tokens)
    weights = jax.nn.softmax(jnp.where(place[:, None] >= place, scores, -jnp.inf), -1).astype(jnp.bfloat16)
    return jnp.einsum("gstu,ugd->tgsd", weights.astype(jnp.float32), v.astype(jnp.float32)).astype(jnp.bfloat16).reshape(tokens, -1)


def layer(h, w):
    a = normed(h)
    q, k = (turned(matmul(a, w[name]).reshape(h.shape[0], -1, HEAD), THETA) for name in ("wq", "wk"))
    h = h + matmul(seen_by(q, k, matmul(a, w["wv"]).reshape(h.shape[0], -1, HEAD)), w["wo"])
    b = normed(h)
    gate = jnp.dot(b, w["w_gate"], preferred_element_type=jnp.float32)
    up = jnp.dot(b, w["w_up"], preferred_element_type=jnp.float32)
    return h + matmul((jax.nn.silu(gate) * up).astype(jnp.bfloat16), w["w_down"])


def adamw(w, m, v, g):
    m = 0.9 * m + 0.1 * g
    v = 0.95 * v + 0.05 * g * g
    step = m * lax.rsqrt(v + 1e-8) + 0.1 * w
    return (w - 0.02 * step).astype(jnp.bfloat16), m, v


def clipped(gradients, sum_of_squares, count):
    factor = jnp.minimum(1.0, 0.5 * lax.rsqrt(sum_of_squares / count + 1e-30))
    return [g * factor for g in gradients]


def stack(weights, h):
    return lax.scan(lambda h, w: (layer(h, w), None), h, weights)[0]


def reference(x, dy, wq, wk, wv, wo, w_gate, w_up, w_down, m_wq, m_wk, m_wv, m_wo, m_w_gate, m_w_up, m_w_down, v_wq, v_wk, v_wv, v_wo, v_w_gate, v_w_up, v_w_down):
    weights = dict(zip(NAMES, (wq, wk, wv, wo, w_gate, w_up, w_down), strict=True))

    def take(so_far, sequence):
        h, by_y = sequence
        _, back = jax.vjp(stack, weights, h)
        by_weights, by_h = back(by_y)
        return jax.tree.map(lambda total, term: total + term.astype(jnp.float32), so_far, by_weights), by_h

    none_yet = {name: jnp.zeros(w.shape, jnp.float32) for name, w in weights.items()}
    by_weights, by_x = lax.scan(take, none_yet, (x, dy))
    gradients = [by_weights[name].astype(jnp.bfloat16).astype(jnp.float32) for name in NAMES]
    gradients = clipped(gradients, sum(jnp.sum(g * g) for g in gradients), sum(g.size for g in gradients))
    first = (m_wq, m_wk, m_wv, m_wo, m_w_gate, m_w_up, m_w_down)
    second = (v_wq, v_wk, v_wv, v_wo, v_w_gate, v_w_up, v_w_down)
    new = [adamw(weights[name].astype(jnp.float32), m, v, g) for name, m, v, g in zip(NAMES, first, second, gradients, strict=True)]
    return tuple(one[which] for which in range(3) for one in new)
```

```python
import functools

import jax
import jax.numpy as jnp
import numpy as np
from jax import lax
from jax.experimental import pallas as pl
from jax.experimental.pallas import tpu as pltpu
from jax.sharding import PartitionSpec as P

NAMES = ("wq", "wk", "wv", "wo", "w_gate", "w_up", "w_down")
HEAD = 128
THETA = 10000
NEG = -1e30
HIDDEN = 2 * NEG
LOG2E = 1.4426950408889634
VMEM = 60 * 2**20
TILE = 512
LOW, WIDE = jnp.bfloat16, jnp.float32


def _dot(a, b, ca=1, cb=0):
    return lax.dot_general(a, b, (((ca,), (cb,)), ((), ())), preferred_element_type=WIDE)


def _call(kernel, grid, ins, outs, scratch, name, args, flops, order="arbitrary"):
    moved = sum(a.size * a.dtype.itemsize for a in (*args, *(o[0] for o in outs)))
    return pl.pallas_call(
        kernel,
        grid=grid,
        in_specs=ins,
        out_specs=[o[1] for o in outs],
        out_shape=[o[0] for o in outs],
        scratch_shapes=scratch,
        compiler_params=pltpu.CompilerParams(dimension_semantics=(order,), vmem_limit_bytes=VMEM),
        cost_estimate=pl.CostEstimate(flops=flops, transcendentals=0, bytes_accessed=moved),
        name=name,
    )(*args)


def _rows(cols):
    return pl.BlockSpec((TILE, cols), lambda i: (i, 0))


def _heads(n):
    return pl.BlockSpec((n, TILE, HEAD), lambda i: (0, i, 0))


def _whole(*shape):
    return pl.BlockSpec(shape, lambda i: (0,) * len(shape))


def _of_layer(w, number):
    return pl.BlockSpec((1, *w.shape[1:]), lambda i: (number, 0, 0))


def _out(shape, dtype, spec):
    return jax.ShapeDtypeStruct(shape, dtype), spec


def _scale(h):
    return lax.rsqrt(jnp.mean(h * h, -1, keepdims=True) + 1e-6)


def _turn(t, cos, sin):
    t = t.astype(WIDE)
    return (t * cos + pltpu.roll(t, HEAD // 2, 1) * sin).astype(LOW)


def turns(tokens):
    half = HEAD // 2
    angle = np.arange(tokens)[:, None] * float(THETA) ** (-np.arange(half) / half)
    cos, sin = np.cos(angle), np.sin(angle)
    return jnp.asarray(np.concatenate([cos, cos], 1), WIDE), jnp.asarray(np.concatenate([-sin, sin], 1), WIDE)


def _project(h, wq_ref, wk_ref, wv_ref, cos_ref, sin_ref, q_ref, k_ref, v_ref):
    a = (h * _scale(h)).astype(LOW)
    cos, sin = cos_ref[...], sin_ref[...]
    q = _dot(a, wq_ref[0]).astype(LOW)
    for n in range(q_ref.shape[0]):
        q_ref[n] = _turn(q[:, n * HEAD : (n + 1) * HEAD], cos, sin)
    k_ref[...] = _turn(_dot(a, wk_ref[0]).astype(LOW), cos, sin)
    v_ref[...] = _dot(a, wv_ref[0]).astype(LOW)


def _first_kernel(h_ref, *refs):
    _project(h_ref[...].astype(WIDE), *refs)


def _qkv_outs(tokens, heads):
    return [_out((heads, tokens, HEAD), LOW, _heads(heads))] + [_out((tokens, HEAD), LOW, _rows(HEAD))] * 2


def first(h, w, number, tables):
    tokens, d = h.shape
    args = [h, w["wq"], w["wk"], w["wv"], *tables]
    cols = w["wq"].shape[2]
    return _call(_first_kernel, (tokens // TILE,), [_rows(d)] + [_of_layer(x, number) for x in args[1:4]] + [_rows(HEAD)] * 2,
                 _qkv_outs(tokens, cols // HEAD), [], "first", args, 2 * tokens * d * (cols + 2 * HEAD))


def _attend_kernel(q_ref, k_ref, v_ref, o_ref, lse_ref, top_s, mix_s):
    heads = q_ref.shape[0]
    block_q = pl.program_id(0)
    scale = HEAD**-0.5
    e = scale * LOG2E
    top_s[...] = jnp.full(top_s.shape, NEG, WIDE)
    mix_s[...] = jnp.zeros(mix_s.shape, WIDE)
    ones = jnp.ones((8, TILE), LOW)

    def block(j, masked):
        here = pl.ds(pl.multiple_of(j * TILE, TILE), TILE)
        k, values = k_ref[here, :], jnp.concatenate([v_ref[here, :].T, ones], axis=0)
        if masked:
            ok = lax.broadcasted_iota(jnp.int32, (TILE, TILE), 1) >= lax.broadcasted_iota(jnp.int32, (TILE, TILE), 0)
        scores = [_dot(k, q_ref[n], 1, 1) for n in range(heads)]
        weights, keeps = [], []
        for n, s in enumerate(scores):
            if masked:
                s = jnp.where(ok, s, HIDDEN)
            old = top_s[n : n + 1, :]
            top = jnp.maximum(old, s.max(axis=0, keepdims=True))
            top_s[n : n + 1, :] = top
            weights.append(jnp.exp2((s - top) * e).astype(LOW))
            keeps.append(jnp.exp2((old - top) * e))
        for n, (p, keep) in enumerate(zip(weights, keeps)):
            mix_s[n] = mix_s[n] * keep + _dot(values, p)

    lax.fori_loop(0, block_q, lambda j, _: block(j, False), None)
    block(block_q, True)
    for n in range(heads):
        total = mix_s[n, HEAD : HEAD + 1, :]
        o_ref[:, n * HEAD : (n + 1) * HEAD] = (mix_s[n, :HEAD, :] * (1 / total)).T.astype(LOW)
        lse_ref[n : n + 1, :] = top_s[n : n + 1, :] * scale + jnp.log(total)


def attend(q, k, v):
    heads, tokens, _ = q.shape
    return _call(_attend_kernel, (tokens // TILE,), [_heads(heads), _whole(tokens, HEAD), _whole(tokens, HEAD)],
                 [_out((tokens, heads * HEAD), LOW, _rows(heads * HEAD)),
                  _out((heads, tokens), WIDE, pl.BlockSpec((heads, TILE), lambda i: (0, i)))],
                 [pltpu.VMEM((heads, TILE), WIDE), pltpu.VMEM((heads, HEAD + 8, TILE), WIDE)],
                 "attend", [q, k, v], 2 * heads * tokens * tokens * HEAD)


def _attend_back_kernel(q_ref, k_ref, v_ref, o_ref, do_ref, lse_ref, dq_ref, dk_ref, dv_ref, dq_s, dk_s, dv_s):
    heads = q_ref.shape[0]
    block_q = pl.program_id(0)
    scale = HEAD**-0.5
    e = scale * LOG2E

    @pl.when(block_q == 0)
    def _():
        dk_s[...] = jnp.zeros_like(dk_s)
        dv_s[...] = jnp.zeros_like(dv_s)

    dq_s[...] = jnp.zeros_like(dq_s)
    of = lambda n: (slice(None), slice(n * HEAD, (n + 1) * HEAD))
    lses = [lse_ref[n : n + 1, :] * LOG2E for n in range(heads)]
    deltas = [(do_ref[of(n)].astype(WIDE) * o_ref[of(n)].astype(WIDE)).T.sum(0, keepdims=True) for n in range(heads)]

    def block(j, masked):
        here = pl.ds(pl.multiple_of(j * TILE, TILE), TILE)
        k, v = k_ref[here, :], v_ref[here, :]
        if masked:
            ok = lax.broadcasted_iota(jnp.int32, (TILE, TILE), 1) >= lax.broadcasted_iota(jnp.int32, (TILE, TILE), 0)
        scores = [_dot(k, q_ref[n], 1, 1) for n in range(heads)]
        dps = [_dot(v, do_ref[of(n)], 1, 1) for n in range(heads)]
        k_turned = k.T
        for n in range(heads):
            p = jnp.exp2(scores[n] * e - lses[n])
            if masked:
                p = jnp.where(ok, p, 0.0)
            ds = (p * (dps[n] - deltas[n])).astype(LOW)
            dv_s[here, :] += _dot(p.astype(LOW), do_ref[of(n)])
            dk_s[here, :] += _dot(ds, q_ref[n])
            dq_s[n] += _dot(k_turned, ds)

    lax.fori_loop(0, block_q, lambda j, _: block(j, False), None)
    block(block_q, True)
    for n in range(heads):
        dq_ref[of(n)] = (dq_s[n] * scale).T.astype(LOW)

    @pl.when(block_q == pl.num_programs(0) - 1)
    def _():
        dk_ref[...] = (dk_s[...] * scale).astype(LOW)
        dv_ref[...] = dv_s[...].astype(LOW)


def attend_back(q, k, v, o, do, lse):
    heads, tokens, _ = q.shape
    wide, kv = _rows(heads * HEAD), _whole(tokens, HEAD)
    return _call(_attend_back_kernel, (tokens // TILE,), [_heads(heads), kv, kv, wide, wide, pl.BlockSpec((heads, TILE), lambda i: (0, i))],
                 [_out((tokens, heads * HEAD), LOW, wide)] + [_out((tokens, HEAD), LOW, kv)] * 2,
                 [pltpu.VMEM((heads, HEAD, TILE), WIDE)] + [pltpu.VMEM((tokens, HEAD), WIDE)] * 2,
                 "attend_back", [q, k, v, o, do, lse], 5 * heads * tokens * tokens * HEAD)


def _after_attention(o_ref, h_ref, wo_ref):
    return (h_ref[...].astype(WIDE) + _dot(o_ref[...], wo_ref[0]).astype(LOW).astype(WIDE)).astype(LOW)


def _middle_kernel(o_ref, h_ref, wo_ref, wg_ref, wu_ref, wd_ref, wq_ref, wk_ref, wv_ref, cos_ref, sin_ref, mid_ref, next_ref, *outs):
    mid_ref[...] = _after_attention(o_ref, h_ref, wo_ref)
    mid = mid_ref[...].astype(WIDE)
    b = (mid * _scale(mid)).astype(LOW)
    total = None
    for at in range(0, wg_ref.shape[2], TILE):
        here = slice(at, at + TILE)
        gate, up = _dot(b, wg_ref[0, :, here]), _dot(b, wu_ref[0, :, here])
        part = _dot((gate * jax.nn.sigmoid(gate) * up).astype(LOW), wd_ref[0, here, :])
        total = part if total is None else total + part
    after = (mid + total.astype(LOW).astype(WIDE)).astype(LOW)
    next_ref[...] = after
    _project(after.astype(WIDE), wq_ref, wk_ref, wv_ref, cos_ref, sin_ref, *outs)


def middle(o, h, w, number, tables):
    tokens, d = h.shape
    names = ("wo", "w_gate", "w_up", "w_down")
    args = [o, h, *(w[n] for n in names), w["wq"], w["wk"], w["wv"], *tables]
    specs = [_rows(o.shape[1]), _rows(d)] + [_of_layer(w[n], number) for n in names]
    specs += [_of_layer(w[n], number + 1) for n in ("wq", "wk", "wv")] + [_rows(HEAD)] * 2
    size = sum(x.size for x in w.values()) // w["wq"].shape[0]
    return _call(_middle_kernel, (tokens // TILE,), specs,
                 [_out((tokens, d), LOW, _rows(d))] * 2 + _qkv_outs(tokens, o.shape[1] // HEAD), [], "middle", args, 2 * tokens * size)


def _back_kernel(last, *refs):
    dy_ref, o_ref, h_ref, wo_ref, wg_ref, wu_ref, wd_ref, dh_ref, do_ref, dwo_ref, dwg_ref, dwu_ref, dwd_ref, dwo_s, dwg_s, dwu_s, dwd_s = refs
    sums = ((dwo_ref, dwo_s), (dwg_ref, dwg_s), (dwu_ref, dwu_s), (dwd_ref, dwd_s))

    @pl.when(pl.program_id(0) == 0)
    def _():
        for _, s in sums:
            s[...] = jnp.zeros_like(s)

    mid = (_after_attention(o_ref, h_ref, wo_ref) if last else h_ref[...]).astype(WIDE)
    scale = _scale(mid)
    b = (mid * scale).astype(LOW)
    dy = dy_ref[...]
    dy_turned, b_turned = dy.T, b.T
    db = None
    for at in range(0, wg_ref.shape[2], TILE):
        here = slice(at, at + TILE)
        gate, up = _dot(b, wg_ref[0, :, here]), _dot(b, wu_ref[0, :, here])
        dact = _dot(dy, wd_ref[0, here, :], 1, 1).astype(LOW).astype(WIDE)
        some = jax.nn.sigmoid(gate)
        silu = gate * some
        act = (silu * up).astype(LOW)
        dup = (dact * silu).astype(LOW)
        dgate = (dact * up * (some + silu * (1 - some))).astype(LOW)
        part = _dot(dgate, wg_ref[0, :, here], 1, 1) + _dot(dup, wu_ref[0, :, here], 1, 1)
        db = part if db is None else db + part
        dwd_s[:, here] += _dot(dy_turned, act)
        dwg_s[:, here] += _dot(b_turned, dgate)
        dwu_s[:, here] += _dot(b_turned, dup)
    dh = _norm_back(dy.astype(WIDE), mid, scale, db)
    dh_ref[...] = dh
    do_ref[...] = _dot(dh, wo_ref[0], 1, 1).astype(LOW)
    dwo_s[...] += _dot(o_ref[...].T, dh)

    @pl.when(pl.program_id(0) == pl.num_programs(0) - 1)
    def _():
        for ref, s in sums[:3]:
            ref[...] = s[...].astype(LOW)
        dwd_ref[...] = dwd_s[...].T.astype(LOW)


def _norm_back(dy, h, scale, db):
    return (dy + scale * (db - h * (scale * scale * jnp.mean(db * h, -1, keepdims=True)))).astype(LOW)


def back(dy, o, h, w, number, last):
    tokens, d = dy.shape
    names = ("wo", "w_gate", "w_up", "w_down")
    args = [dy, o, h, *(w[n] for n in names)]
    wide = _rows(o.shape[1])
    shapes = [w[n].shape[1:] for n in names]
    turned = [*shapes[:3], shapes[3][::-1]]
    return _call(functools.partial(_back_kernel, last), (tokens // TILE,), [_rows(d), wide, _rows(d)] + [_of_layer(w[n], number) for n in names],
                 [_out((tokens, d), LOW, _rows(d)), _out((tokens, o.shape[1]), LOW, wide)] + [_out(s, LOW, _whole(*s)) for s in shapes],
                 [pltpu.VMEM(s, WIDE) for s in turned], "back", args, 6 * tokens * sum(s[0] * s[1] for s in shapes))


def _start_kernel(more, *refs):
    h_ref, dq_ref, dk_ref, dv_ref, cos_ref, sin_ref = refs[:6]
    refs = refs[6:]
    if more:
        dh_ref, wq_ref, wk_ref, wv_ref, dx_ref = refs[:5]
        refs = refs[5:]
    outs, sums = refs[:3], refs[3:]

    @pl.when(pl.program_id(0) == 0)
    def _():
        for s in sums:
            s[...] = jnp.zeros_like(s)

    h = h_ref[...].astype(WIDE)
    scale = _scale(h)
    a_turned = (h * scale).astype(LOW).T
    cos, sin = cos_ref[...], -sin_ref[...]
    dq = jnp.concatenate([_turn(dq_ref[:, at : at + HEAD], cos, sin) for at in range(0, dq_ref.shape[1], HEAD)], axis=1)
    dk, dv = _turn(dk_ref[...], cos, sin), dv_ref[...]
    for s, by in zip(sums, (dq, dk, dv)):
        s[...] += _dot(a_turned, by)
    if more:
        da = _dot(dq, wq_ref[0], 1, 1) + _dot(dk, wk_ref[0], 1, 1) + _dot(dv, wv_ref[0], 1, 1)
        dx_ref[...] = _norm_back(dh_ref[...].astype(WIDE), h, scale, da)

    @pl.when(pl.program_id(0) == pl.num_programs(0) - 1)
    def _():
        for ref, s in zip(outs, sums):
            ref[...] = s[...].astype(LOW)


def start(h, dq, dk, dv, tables, dh, w, number):
    tokens, d = h.shape
    more = number > 0
    names = ("wq", "wk", "wv")
    shapes = [w[n].shape[1:] for n in names]
    args = [h, dq, dk, dv, *tables] + ([dh, *(w[n] for n in names)] if more else [])
    specs = [_rows(d), _rows(dq.shape[1])] + [_rows(HEAD)] * 4 + ([_rows(d)] + [_of_layer(w[n], number) for n in names] if more else [])
    outs = [_out((tokens, d), LOW, _rows(d))] if more else []
    got = _call(functools.partial(_start_kernel, more), (tokens // TILE,), specs, outs + [_out(s, LOW, _whole(*s)) for s in shapes],
                [pltpu.VMEM(s, WIDE) for s in shapes], "start", args, 4 * tokens * sum(s[0] * s[1] for s in shapes))
    return (got[0] if more else None), got[-3:]


def adamw(w, m, v, g):
    m = 0.9 * m + 0.1 * g
    v = 0.95 * v + 0.05 * g * g
    step = m * lax.rsqrt(v + 1e-8) + 0.1 * w
    return (w - 0.02 * step).astype(LOW), m, v


def gradients(x, dy, w):
    layers = w["wq"].shape[0]
    tables = turns(x.shape[0])
    kept, h = [], x
    q, k, v = first(x, w, 0, tables)
    for number in range(layers):
        o, lse = attend(q, k, v)
        kept.append([h, q, k, v, o, lse, h])
        if number < layers - 1:
            kept[number][6], h, q, k, v = middle(o, h, w, number, tables)
    grads = [None] * layers
    for number in reversed(range(layers)):
        h, q, k, v, o, lse, mid = kept[number]
        dh, do, *late = back(dy, o, mid, w, number, number == layers - 1)
        dq, dk, dv = attend_back(q, k, v, o, do, lse)
        dy, early = start(h, dq, dk, dv, tables, dh, w, number)
        grads[number] = dict(zip(NAMES, (*early, *late)))
    return grads


SIDE, CORES = 4, 2
WHERE = pl.DeviceIdType.MESH


class Place:
    def __init__(self):
        me = lax.axis_index("dp")
        self.core = lax.rem(me, CORES)
        chip = lax.div(me, CORES)
        self.at = (lax.div(chip, SIDE), lax.rem(chip, SIDE))
        self.partner = me + 1 - 2 * self.core

    def along(self, axis, by):
        x, y = (lax.rem(p + SIDE + by, SIDE) if a == axis else p for a, p in enumerate(self.at))
        return (x * SIDE + y) * CORES + self.core

    def shifted(self, axis, by):
        return lax.rem(self.at[axis] + SIDE + by, SIDE)


def meet(devices):
    barrier = pltpu.get_barrier_semaphore()
    for d in devices:
        pl.semaphore_signal(barrier, inc=1, device_id={"dp": d}, device_id_type=WHERE)
    pl.semaphore_wait(barrier, len(devices))


def send(src, dst, sems, device):
    return pltpu.make_async_remote_copy(src_ref=src, dst_ref=dst, send_sem=sems[0], recv_sem=sems[1], device_id={"dp": device}, device_id_type=WHERE)


class Item:
    def __init__(self, name, half, axis, way):
        self.name, self.half, self.axis, self.way = name, half, axis, way

    def mine(self, ref, *at):
        return ref.at[at] if self.half is None else ref.at[(*at, self.half)]


ITEMS = (
    Item("w_gate", None, 0, 1),
    Item("w_up", None, 1, 1),
    Item("w_down", 0, 0, -1),
    Item("w_down", 1, 1, -1),
    Item("wq", None, 0, -1),
    Item("wo", None, 1, -1),
    Item("wk", None, 0, -1),
    Item("wv", None, 1, -1),
)


def cut(name, rows):
    block = rows // (SIDE * SIDE * CORES)
    return (SIDE, SIDE, CORES, 2, block // 2) if name == "w_down" else (SIDE, SIDE, CORES, block)


def item_shape(item, shapes):
    rows, cols = shapes[item.name]
    return (cut(item.name, rows)[-1], cols)


class Scatter:
    SEMS = 8

    @staticmethod
    def scratch(shape):
        rows, cols = shape
        lots = lambda *lead: pltpu.VMEM((*lead, rows, cols), jnp.bfloat16)
        return [lots(SIDE, SIDE), lots(SIDE, SIDE), lots(3, SIDE), lots(3, SIDE), lots(3), lots(3),
                pltpu.SemaphoreType.DMA((Scatter.SEMS,)), pltpu.SemaphoreType.DMA((Scatter.SEMS,))]

    def __init__(self, item, place, given, scratch):
        self.item, self.place, self.given = item, place, given
        self.own, self.pair, self.s1, self.r1, self.s2, self.r2, self.ssem, self.rsem = scratch
        a, e, d = item.axis, 1 - item.axis, item.way
        p = place
        self.a, self.e = p.at[a], p.at[e]
        self.here = lambda i, j: (i, j) if a == 0 else (j, i)
        self.a_two, self.a_back, self.a_on = p.shifted(a, 2), p.shifted(a, -d), p.shifted(a, d)
        self.e_two, self.e_back, self.e_on = p.shifted(e, 2), p.shifted(e, -d), p.shifted(e, d)
        at = lambda n: (self.ssem.at[n], self.rsem.at[n])
        on1, back1, on2, back2 = p.along(a, d), p.along(a, -d), p.along(e, d), p.along(e, -d)
        self.moves = [
            send(self.mine(1 - p.core), self.pair, at(0), p.partner),
            send(self.s1.at[0], self.r1.at[0], at(1), on1),
            send(self.s1.at[1], self.r1.at[1], at(2), back1),
            send(self.s1.at[2], self.r1.at[2], at(3), on1),
            send(self.s2.at[0], self.r2.at[0], at(4), on2),
            send(self.s2.at[1], self.r2.at[1], at(5), back2),
            send(self.s2.at[2], self.r2.at[2], at(6), on2),
        ]
        self.load = pltpu.make_async_copy(self.mine(p.core), self.own, self.ssem.at[7])

    def mine(self, core):
        every = slice(None)
        return self.item.mine(self.given, every, every, core)

    def chip(self, i, j):
        at = self.here(i, j)
        return self.own[at].astype(jnp.float32) + self.pair[at].astype(jnp.float32)

    def first(self):
        self.moves[0].start()
        self.load.start()

    def step1(self):
        self.load.wait()
        self.moves[0].wait_recv()

        def one(j, _):
            self.s1[0, j] = self.chip(self.a_two, j).astype(jnp.bfloat16)
            self.s1[1, j] = self.chip(self.a_back, j).astype(jnp.bfloat16)

        lax.fori_loop(0, SIDE, one, None)
        self.moves[1].start()
        self.moves[2].start()

    def step2(self):
        self.moves[1].wait_recv()

        def one(j, _):
            self.s1[2, j] = (self.chip(self.a_on, j) + self.r1[0, j].astype(jnp.float32)).astype(jnp.bfloat16)

        lax.fori_loop(0, SIDE, one, None)
        self.moves[3].start()

    def row(self, j):
        return self.chip(self.a, j) + self.r1[1, j].astype(jnp.float32) + self.r1[2, j].astype(jnp.float32)

    def step3(self):
        self.moves[2].wait_recv()
        self.moves[3].wait_recv()
        self.s2[0] = self.row(self.e_two).astype(jnp.bfloat16)
        self.s2[1] = self.row(self.e_back).astype(jnp.bfloat16)
        self.moves[4].start()
        self.moves[5].start()

    def step4(self):
        self.moves[4].wait_recv()
        self.s2[2] = (self.row(self.e_on) + self.r2[0].astype(jnp.float32)).astype(jnp.bfloat16)
        self.moves[6].start()

    def last(self):
        self.moves[5].wait_recv()
        self.moves[6].wait_recv()
        total = self.row(self.e) + self.r2[1].astype(jnp.float32) + self.r2[2].astype(jnp.float32)
        for move in self.moves:
            move.wait_send()
        return total.astype(jnp.bfloat16)


def neighbours(place, two=False):
    found = [place.partner] + [place.along(axis, by) for axis in (0, 1) for by in (1, -1)]
    return found + [place.along(axis, 2) for axis in (0, 1)] if two else found


def _fold(x):
    rows, cols = x.shape
    x = x.reshape(rows // 8, 8, cols).sum(0)
    return sum(x[:, at : at + 128] for at in range(0, cols, 128))


def _sum_kernel(layers, shapes, *refs):
    names = list(NAMES)
    given = [dict(zip(names, refs[n * 7 : n * 7 + 7])) for n in range(layers)]
    refs = refs[7 * layers :]
    outs, refs = dict(zip(names, refs[:7])), refs[7:]
    squares_ref, refs = refs[0], refs[1:]
    squares_s, squares_r, square_sems, refs = refs[0], refs[1], refs[2], refs[3:]
    place = Place()
    meet(neighbours(place, True))
    parts = []
    for layer in reversed(range(layers)):
        for item in ITEMS:
            parts.append((layer, Scatter(item, place, given[layer][item.name], refs[:8])))
            refs = refs[8:]
    for step in ("first", "step1", "step2", "step3", "step4"):
        for _, part in parts:
            getattr(part, step)()
    squares = jnp.zeros((8, 128), jnp.float32)
    for layer, part in parts:
        total = part.last()
        outs[part.item.name][(layer,) if part.item.half is None else (layer, part.item.half)] = total
        wide = total.astype(jnp.float32)
        squares += _fold(wide * wide)
    rounds = [[place.partner], [place.along(0, by) for by in (1, 2, 3)], [place.along(1, by) for by in (1, 2, 3)]]
    slot = 0
    for n, devices in enumerate(rounds):
        squares_s[n] = squares
        moves = []
        for device in devices:
            moves.append(send(squares_s.at[n], squares_r.at[slot], (square_sems.at[0, slot], square_sems.at[1, slot]), device))
            slot += 1
        for move in moves:
            move.start()
        for move in moves:
            move.wait_recv()
        squares = squares + sum(squares_r[at] for at in range(slot - len(devices), slot))
        for move in moves:
            move.wait_send()
    squares_ref[...] = squares


def block_shape(name, layers, shapes):
    rows, cols = shapes[name]
    return (layers, *cut(name, rows)[3:], cols)


def summed(grads, layers, shapes):
    given = [grads[n][name].reshape(*cut(name, shapes[name][0]), shapes[name][1]) for n in range(layers) for name in NAMES]
    scratch = [pltpu.VMEM((3, 8, 128), jnp.float32), pltpu.VMEM((7, 8, 128), jnp.float32), pltpu.SemaphoreType.DMA((2, 7))]
    for _ in range(layers):
        for item in ITEMS:
            scratch += Scatter.scratch(item_shape(item, shapes))
    out = pl.pallas_call(
        functools.partial(_sum_kernel, layers, shapes),
        out_shape=[jax.ShapeDtypeStruct(block_shape(name, layers, shapes), jnp.bfloat16) for name in NAMES]
        + [jax.ShapeDtypeStruct((8, 128), jnp.float32)],
        in_specs=[pl.BlockSpec(memory_space=pl.ANY)] * len(given),
        out_specs=[pl.BlockSpec(memory_space=pltpu.VMEM)] * 8,
        scratch_shapes=scratch,
        compiler_params=pltpu.CompilerParams(collective_id=0, has_side_effects=True, vmem_limit_bytes=60 * 2**20),
        name="sum_gradients",
    )(*given)
    return dict(zip(NAMES, out[:7])), out[7]


def _step_kernel(count, *refs):
    squares_ref, refs = refs[0], refs[1:]
    w, g, m, v = (refs[n * 7 : n * 7 + 7] for n in range(4))
    refs = refs[28:]
    new_w, new_m, new_v = (refs[n * 7 : n * 7 + 7] for n in range(3))
    held, sem = refs[21:28], refs[28]
    me = lax.axis_index("dp")
    loads = [pltpu.make_async_copy(w[n].at[:, me], held[n], sem.at[n]) for n in range(7)]
    for load in loads:
        load.start()
    factor = jnp.minimum(1.0, 0.5 * lax.rsqrt(jnp.sum(squares_ref[...]) / count + 1e-30))
    for n in range(7):
        loads[n].wait()
        layers, rows, cols = held[n].shape
        for layer in range(layers):
            for at in range(0, rows, 8):
                here = (layer, slice(at, at + 8))
                new_w[n][here], new_m[n][here], new_v[n][here] = adamw(
                    held[n][here].astype(jnp.float32), m[n][here], v[n][here], g[n][here].astype(jnp.float32) * factor)


def stepped(squares, weights, g, m, v, shapes, count):
    layers, devices = weights[0].shape[0], SIDE * SIDE * CORES
    blocks = [(layers, shapes[name][0] // devices, shapes[name][1]) for name in NAMES]
    whole = pl.BlockSpec(memory_space=pltpu.VMEM)
    out = pl.pallas_call(
        functools.partial(_step_kernel, count),
        out_shape=[jax.ShapeDtypeStruct(b, t) for t in (jnp.bfloat16, jnp.float32, jnp.float32) for b in blocks],
        in_specs=[whole] + [pl.BlockSpec(memory_space=pl.ANY)] * 7 + [whole] * 21,
        out_specs=[whole] * 21,
        scratch_shapes=[pltpu.VMEM(b, jnp.bfloat16) for b in blocks] + [pltpu.SemaphoreType.DMA((7,))],
        compiler_params=pltpu.CompilerParams(vmem_limit_bytes=60 * 2**20),
        name="adamw",
    )(squares, *(w.reshape(layers, devices, b[1], b[2]) for w, b in zip(weights, blocks)),
      *(g[name].reshape(b) for name, b in zip(NAMES, blocks)), *m, *v)
    return out[:7], out[7:14], out[14:]


class Gather:
    SENDS, RECVS = 11, 10

    @staticmethod
    def scratch():
        return [pltpu.SemaphoreType.DMA((Gather.SENDS,)), pltpu.SemaphoreType.DMA((Gather.RECVS,))]

    def __init__(self, item, place, block, out, scratch):
        ssem, rsem = scratch
        p, d = place, item.way
        a, e = item.axis, 1 - item.axis
        every = slice(None)
        cut_at = lambda *at: out.at[(every, *at)] if item.half is None else out.at[(every, *at, item.half)]
        self.block = block if item.half is None else block.at[:, item.half]
        one = lambda i: cut_at(*((i, p.at[1]) if a == 0 else (p.at[0], i)), p.core)
        row = lambda j: cut_at(*((every, j) if a == 0 else (j, every)), p.core)
        on1, back1, on2, back2 = p.along(a, d), p.along(a, -d), p.along(e, d), p.along(e, -d)
        me, back = p.at[a], p.shifted(a, -d)
        here, e_back, e_on, e_two = p.at[e], p.shifted(e, -d), p.shifted(e, d), p.shifted(e, 2)
        at = lambda n: (ssem.at[n], rsem.at[n])
        self.keep = pltpu.make_async_copy(self.block, one(me), ssem.at[10])
        self.to_on = send(self.block, one(me), at(0), on1)
        self.to_back = send(self.block, one(me), at(1), back1)
        self.pass_on = send(one(back), one(back), at(2), on1)
        self.row_on = send(row(here), row(here), at(3), on2)
        self.row_back = send(row(here), row(here), at(4), back2)
        self.row_pass = send(row(e_back), row(e_back), at(5), on2)
        self.pairs = [send(row(j), row(j), at(6 + n), p.partner) for n, j in enumerate((here, e_back, e_on, e_two))]

    def first(self):
        self.to_on.start()
        self.to_back.start()
        self.keep.start()

    def step1(self):
        self.to_on.wait_recv()
        self.pass_on.start()

    def step2(self):
        self.to_back.wait_recv()
        self.pass_on.wait_recv()
        self.keep.wait()
        self.row_on.start()
        self.row_back.start()
        self.pairs[0].start()

    def step3(self):
        self.row_on.wait_recv()
        self.row_pass.start()
        self.pairs[1].start()

    def step4(self):
        self.row_back.wait_recv()
        self.pairs[2].start()

    def step5(self):
        self.row_pass.wait_recv()
        self.pairs[3].start()

    def last(self):
        for pair in self.pairs:
            pair.wait_recv()
        for move in (self.to_on, self.to_back, self.pass_on, self.row_on, self.row_back, self.row_pass, *self.pairs):
            move.wait_send()


def _gather_kernel(*refs):
    blocks, outs, scratch = dict(zip(NAMES, refs[:7])), dict(zip(NAMES, refs[7:14])), refs[14:]
    place = Place()
    meet(neighbours(place))
    parts = [Gather(item, place, blocks[item.name], outs[item.name], scratch[2 * n : 2 * n + 2]) for n, item in enumerate(ITEMS)]
    for step in ("first", "step1", "step2", "step3", "step4", "step5", "last"):
        for part in parts:
            getattr(part, step)()


def gathered(blocks, layers, shapes):
    out = pl.pallas_call(
        _gather_kernel,
        out_shape=[jax.ShapeDtypeStruct((layers, *cut(name, shapes[name][0]), shapes[name][1]), jnp.bfloat16) for name in NAMES],
        in_specs=[pl.BlockSpec(memory_space=pltpu.VMEM)] * 7,
        out_specs=[pl.BlockSpec(memory_space=pl.ANY)] * 7,
        scratch_shapes=[s for _ in ITEMS for s in Gather.scratch()],
        compiler_params=pltpu.CompilerParams(collective_id=1, has_side_effects=True, vmem_limit_bytes=60 * 2**20),
        name="gather_weights",
    )(*(b.reshape(block_shape(name, layers, shapes)) for name, b in zip(NAMES, blocks)))
    return [o.reshape(layers, *shapes[name]) for name, o in zip(NAMES, out)]


def finished(grads, weights, m, v):
    layers = weights[0].shape[0]
    shapes = {name: w.shape[1:] for name, w in zip(NAMES, weights)}
    g, squares = summed(grads, layers, shapes)
    count = sum(w.size for w in weights)
    new_w, new_m, new_v = stepped(squares, weights, g, m, v, shapes, count)
    return (*gathered(new_w, layers, shapes), *new_m, *new_v)


def solution(mesh):

    def step(x, dy, *arrays):
        weights, m, v = (arrays[i : i + 7] for i in (0, 7, 14))
        return finished(gradients(x[0], dy[0], dict(zip(NAMES, weights))), weights, m, v)

    states, all_of, cut_rows = P(("rep", "dp"), None, None), P(None, None, None), P(None, "dp", None)
    return jax.shard_map(
        step,
        mesh=mesh,
        in_specs=(states, states) + (all_of,) * 7 + (cut_rows,) * 14,
        out_specs=(P("rep", None, None),) * 7 + (P("rep", "dp", None),) * 14,
        check_vma=False,
    )
```

```python
import functools

import jax
import jax.numpy as jnp
import numpy as np
from jax import lax
from jax.experimental import pallas as pl
from jax.experimental.pallas import tpu as pltpu
from jax.sharding import PartitionSpec as P

NAMES = ("wq", "wk", "wv", "wo", "w_gate", "w_up", "w_down")
HEAD = 128
THETA = 10000
NEG = -1e30
HIDDEN = 2 * NEG
LOG2E = 1.4426950408889634
VMEM = 60 * 2**20
TILE = 512
HALF = TILE // 2
SHORT = 64
AHEAD = 3
EIGHT = 8
PARTS = 3
SCALE = HEAD**-0.5
LOW, WIDE = jnp.bfloat16, jnp.float32
ANY = pl.BlockSpec(memory_space=pl.ANY)

SIDE, CORES = 4, 2
DEVICES = SIDE * SIDE * CORES
STREAMS = 4
WHERE = pl.DeviceIdType.MESH
LATE, EARLY = ("w_gate", "w_up", "w_down", "wo"), ("wq", "wk", "wv")


def pieces(shapes):
    width, row, found = shapes["w_down"][1], 0, []
    for name in LATE:
        rows, cols = shapes[name][0] // DEVICES, shapes[name][1]
        for column in range(0, cols, width):
            found.append((name, row, 0, rows, column, width))
            row += rows
    late, lane = row, 0
    for name in EARLY:
        rows, cols = shapes[name][0] // DEVICES, shapes[name][1]
        for column in range(0, cols, HEAD):
            found.append((name, row, lane, rows, column, HEAD))
            lane = (lane + HEAD) % width
            row += rows if lane == 0 else 0
    return found, late, row


def shapes_of(w):
    return {name: x.shape[1:] for name, x in w.items()}


def _dot(a, b, ca=1, cb=0):
    return lax.dot_general(a, b, (((ca,), (cb,)), ((), ())), preferred_element_type=WIDE)


def _dot_t(a, b):
    return _dot(a, b, 1, 1)


def _loop(count, body):
    lax.fori_loop(0, count, body, None)


def _at(first, size):
    return pl.ds(pl.multiple_of(first, size), size)


def _part(n, size=HEAD):
    return slice(n * size, n * size + size)


def _step():
    return pl.program_id(0)


def _last():
    return _step() == pl.num_programs(0) - 1


def _seen(shape, queries, ahead=0):
    place = [lax.broadcasted_iota(jnp.int32, shape, axis) for axis in (queries, 1 - queries)]
    return place[0] + ahead >= place[1]


def _split(refs, *counts):
    groups = []
    for count in counts:
        groups.append(refs[:count])
        refs = refs[count:]
    return *groups, refs


def _call(kernel, grid, ins, outs, scratch, name, args, flops, **params):
    moved = sum(a.size * a.dtype.itemsize for a in (*args, *(o[0] for o in outs)))
    return pl.pallas_call(
        kernel,
        grid=grid,
        in_specs=ins,
        out_specs=[o[1] for o in outs],
        out_shape=[o[0] for o in outs],
        scratch_shapes=scratch,
        compiler_params=pltpu.CompilerParams(dimension_semantics=("arbitrary",), vmem_limit_bytes=VMEM, **params),
        cost_estimate=pl.CostEstimate(flops=flops, transcendentals=0, bytes_accessed=moved),
        name=name,
    )(*args)


def _rows(cols):
    return pl.BlockSpec((TILE, cols), lambda i: (i, 0))


def _heads(n):
    return pl.BlockSpec((n, TILE, HEAD), lambda i: (0, i, 0))


def _whole(*shape):
    return pl.BlockSpec(shape, lambda i: (0,) * len(shape))


def _of_layer(w, number):
    return pl.BlockSpec((1, *w.shape[1:]), lambda i: (number, 0, 0))


def _out(shape, dtype, spec):
    return jax.ShapeDtypeStruct(shape, dtype), spec


def _scale(h):
    return lax.rsqrt(jnp.mean(h * h, -1, keepdims=True) + 1e-6)


def _turn(t, cos, sin):
    t = t.astype(WIDE)
    return (t * cos + pltpu.roll(t, HEAD // 2, 1) * sin).astype(LOW)


def turns(tokens):
    half = HEAD // 2
    places = np.concatenate([np.arange(SHORT), np.arange(0, tokens, SHORT)])
    angle = places[:, None] * float(THETA) ** (-np.arange(half) / half)
    return jnp.asarray(np.concatenate([np.cos(angle), np.sin(angle)], 1), WIDE)


def _both(t):
    r = pltpu.roll(t, HEAD // 2, 1)
    first = lax.broadcasted_iota(jnp.int32, t.shape, 1) < HEAD // 2
    return jnp.where(first, t, r), jnp.where(first, -r, t)


def _turns(table_ref):
    cos, sin = _both(table_ref[:SHORT, :])
    many = TILE // SHORT
    far = _both(table_ref[pl.ds(pl.multiple_of(SHORT + _step() * many, many), many), :])
    coses, sines = [], []
    for n in range(many):
        far_cos, far_sin = (t[n : n + 1, :] for t in far)
        coses.append(far_cos * cos - far_sin * sin)
        sines.append(far_sin * cos + far_cos * sin)
    return jnp.concatenate(coses, 0), jnp.concatenate(sines, 0)


def _project(h, wq_ref, wk_ref, wv_ref, table_ref, q_ref, k_ref, v_ref):
    a = (h * _scale(h)).astype(LOW)
    cos, sin = _turns(table_ref)
    q = _dot(a, wq_ref[0]).astype(LOW)
    for n in range(q_ref.shape[0]):
        q_ref[n] = _turn(q[:, _part(n)], cos, sin)
    k_ref[...] = _turn(_dot(a, wk_ref[0]).astype(LOW), cos, sin)
    v_ref[...] = _dot(a, wv_ref[0]).astype(LOW)


def _first_kernel(h_ref, *refs):
    _project(h_ref[...].astype(WIDE), *refs)


def _qkv_outs(tokens, heads):
    return [_out((heads, tokens, HEAD), LOW, _heads(heads))] + [_out((tokens, HEAD), LOW, _rows(HEAD))] * 2


def first(h, w, number, table):
    tokens, d = h.shape
    args = [h, w["wq"], w["wk"], w["wv"], table]
    cols = w["wq"].shape[2]
    return _call(_first_kernel, (tokens // TILE,), [_rows(d)] + [_of_layer(x, number) for x in args[1:4]] + [_whole(*table.shape)],
                 _qkv_outs(tokens, cols // HEAD), [], "first", args, 2 * tokens * d * (cols + 2 * HEAD))


def _attend_kernel(q_ref, k_ref, v_ref, o_ref, turned_ref, qt_ref, lse_ref, top_s, mix_s):
    heads = q_ref.shape[0]
    block_q = _step()
    e = SCALE * LOG2E
    top_s[...] = jnp.full(top_s.shape, NEG, WIDE)
    mix_s[...] = jnp.zeros(mix_s.shape, WIDE)
    def block(first_half, halves, low, masked):
        size = halves * HALF
        here = _at(first_half * HALF, size)
        k, values = k_ref[here, :], jnp.concatenate([v_ref[here, :].T, jnp.ones((EIGHT, size), LOW)])
        if masked:
            ok = _seen((size, TILE - low), 1)
        score = lambda n: _dot_t(k, q_ref[n, low:, :])
        ready = [score(n) for n in range(AHEAD)]
        for n in range(heads):
            if n + AHEAD < heads:
                ready.append(score(n + AHEAD))
            s = jnp.where(ok, ready[n], HIDDEN) if masked else ready[n]
            row = slice(n, n + 1)
            old = top_s[row, low:]
            top = jnp.maximum(old, s.max(0, keepdims=True))
            top_s[row, low:] = top
            mix_s[n, :, low:] = mix_s[n, :, low:] * jnp.exp2((old - top) * e) + _dot(values, jnp.exp2((s - top) * e).astype(LOW))

    _loop(block_q, lambda j, _: block(2 * j, 2, 0, False))
    block(2 * block_q, 1, 0, True)
    block(2 * block_q + 1, 1, HALF, True)
    for n in range(heads):
        total, row = mix_s[n, HEAD : HEAD + 1, :], slice(n, n + 1)
        turned = (mix_s[n, :HEAD, :] * (1 / total)).astype(LOW)
        turned_ref[_part(n), :] = turned
        o_ref[:, _part(n)] = turned.T
        qt_ref[n] = q_ref[n].T
        lse_ref[row, :] = top_s[row, :] * SCALE + jnp.log(total)
    lse_ref[heads:, :] = jnp.zeros((EIGHT - heads, TILE), WIDE)


def _columns(rows):
    return pl.BlockSpec((rows, TILE), lambda i: (0, i))


def _head_columns(heads):
    return pl.BlockSpec((heads, HEAD, TILE), lambda i: (0, 0, i))


def attend(q, k, v):
    heads, tokens, _ = q.shape
    inner = heads * HEAD
    return _call(_attend_kernel, (tokens // TILE,), [_heads(heads), _whole(tokens, HEAD), _whole(tokens, HEAD)],
                 [_out((tokens, inner), LOW, _rows(inner)), _out((inner, tokens), LOW, _columns(inner)),
                  _out((heads, HEAD, tokens), LOW, _head_columns(heads)), _out((EIGHT, tokens), WIDE, _columns(EIGHT))],
                 [pltpu.VMEM((heads, TILE), WIDE), pltpu.VMEM((heads, HEAD + EIGHT, TILE), WIDE)],
                 "attend", [q, k, v], 2 * heads * tokens * tokens * HEAD)


def _attend_back_kernel(many, refs):
    ins, stacks, (dq_ref, dk_ref, dv_ref), sums, (squares_ref,), held, refs = _split(refs, 8, many, 3, many, 1, 5)
    q_ref, qt_ref, k_ref, v_ref, do_ref, dot_ref, lse_ref, delta_ref = ins
    dq_s, dk_s, dv_s, beside_s, take_s = held
    heads = q_ref.shape[0]
    block_q = _step()
    steps = k_ref.shape[0] // TILE
    e = SCALE * LOG2E
    place = Place()
    parts = [Scatter(place, s, refs[_part(at, 9)]) for at, s in enumerate(stacks)]

    def travel(step, tick, *ticks):
        one, other = (n * steps * steps // 16 for n in ticks)

        if parts:
            @pl.when((tick == one) | (tick == other))
            def _():
                for part in parts:
                    getattr(part, step)(jnp.where(tick == other, 1, 0))

    @pl.when(block_q == 0)
    def _():
        if parts:
            meet(neighbours(place))
        for part in parts:
            part.begin()
        lane = lax.broadcasted_iota(jnp.int32, (HALF, HEAD), 1)

        def clear(n, _):
            dk_s[n] = jnp.zeros((HEAD, HALF), WIDE)
            dv_s[n] = jnp.zeros((HEAD, HALF), WIDE)

        def take(n, _):
            for which in (0, 1):
                mine = (lane % EIGHT == n) & (lane // (EIGHT * PARTS) == which)
                take_s[which, n] = jnp.where(mine, -1.0, 0.0).astype(LOW)

        _loop(2 * steps, clear)
        _loop(heads, take)

    dq_s[...] = jnp.zeros_like(dq_s)
    of = lambda n: (slice(None), _part(n))
    lines = []
    for rest in (lse_ref[...] * (1 / SCALE), delta_ref[...]):
        for _ in range(PARTS):
            lines.append(rest.astype(LOW).astype(WIDE))
            rest = rest - lines[-1]
    lines.append(jnp.zeros((HEAD - EIGHT * len(lines), TILE), WIDE))
    beside_s[...] = jnp.concatenate(lines).T.astype(LOW)

    def block(keys, low):
        here = _at(keys * HALF, HALF)
        k, v = k_ref[here, :], v_ref[here, :]
        ok = _seen((TILE - low, HALF), 0, (2 * block_q - keys) * HALF + low)
        beside = lambda x: jnp.concatenate([x, beside_s[low:, :]], 1)
        score = lambda n: (_dot_t(beside(q_ref[n, low:, :]), jnp.concatenate([k, take_s[0, n]], 1)),
                           _dot_t(beside(do_ref[low:, _part(n)]), jnp.concatenate([v, take_s[1, n]], 1)))
        s, dp = score(0)
        dk, dv = None, None
        for n in range(heads):
            after = score(n + 1) if n + 1 < heads else (None, None)
            p = jnp.where(ok, jnp.exp2(s * e), 0.0)
            ds = (p * dp).astype(LOW)
            more_v, more_k = _dot(dot_ref[_part(n), low:], p.astype(LOW)), _dot(qt_ref[n, :, low:], ds)
            dv, dk = (dv + more_v, dk + more_k) if n else (more_v, more_k)
            dq_s[n, low:, :] += _dot(ds, k)
            s, dp = after
        dk_s[keys] += dk
        dv_s[keys] += dv

    def one(j, _):
        tick = block_q * block_q + j
        travel("step1", tick, 3, 4)
        travel("step2", tick, 7, 9)
        travel("step3", tick, 11, 13)
        travel("step4", tick, 14, 15)
        block(j, 0)

    _loop(2 * block_q + 1, one)
    block(2 * block_q + 1, HALF)
    for n in range(heads):
        dq_ref[of(n)] = (dq_s[n] * SCALE).astype(LOW)

    @pl.when(block_q == steps - 1)
    def _():
        def turn(n, _):
            here = _at(n * HALF, HALF)
            dk_ref[here, :] = (dk_s[n] * SCALE).T.astype(LOW)
            dv_ref[here, :] = dv_s[n].T.astype(LOW)

        _loop(2 * steps, turn)
        squares_ref[...] = sum((part.end(out) for part, out in zip(parts, sums)), jnp.zeros((EIGHT, HEAD), WIDE))


def attend_back(q, qt, k, v, do, dot, lse, delta, stacks, number):
    heads, tokens, _ = q.shape
    wide, kv = _rows(heads * HEAD), _whole(tokens, HEAD)
    rows = [s.shape[2] for s in stacks]
    width = stacks[0].shape[3] if stacks else HEAD
    scratch = [pltpu.VMEM((heads, TILE, HEAD), WIDE)] + [pltpu.VMEM((tokens // HALF, HEAD, HALF), WIDE)] * 2
    scratch += [pltpu.VMEM((TILE, HEAD), LOW), pltpu.VMEM((2, heads, HALF, HEAD), LOW)]
    got = _call(lambda *refs: _attend_back_kernel(len(rows), refs), (tokens // TILE,),
                [_heads(heads), _head_columns(heads), kv, kv, wide, _columns(heads * HEAD)] + [_columns(EIGHT)] * 2 + [ANY] * len(rows),
                [_out((tokens, heads * HEAD), LOW, wide)] + [_out((tokens, HEAD), LOW, kv)] * 2
                + [_out((n, width), LOW, _whole(n, width)) for n in rows] + [_out((EIGHT, HEAD), WIDE, _whole(EIGHT, HEAD))],
                scratch + [s for n in rows for s in Scatter.scratch(n, width)],
                "attend_back", [q, qt, k, v, do, dot, lse, delta, *stacks], 5 * heads * tokens * tokens * HEAD, collective_id=number, has_side_effects=True)
    return got[:3], got[3:-1], got[-1]


class Chunks:
    @staticmethod
    def scratch(d, hidden):
        n = hidden // TILE
        return [pltpu.VMEM((n, d, TILE), LOW)] * 2 + [pltpu.VMEM((n, TILE, d), LOW), pltpu.SemaphoreType.DMA((n, 3))]

    def __init__(self, number, refs, held):
        self.number, self.refs, self.held, self.sem = number, refs, held[:3], held[3]
        self.count = held[0].shape[0]

    def copies(self, c):
        units = _at(c * TILE, TILE)
        every = slice(None)
        return [pltpu.make_async_copy(ref.at[at], held.at[c], self.sem.at[c, n]) for n, (ref, held, at) in enumerate(
            zip(self.refs, self.held, ((self.number, every, units), (self.number, every, units), (self.number, units, every))))]

    def fetch(self):
        @pl.when(_step() == 0)
        def _():
            for c in range(self.count):
                for copy in self.copies(c):
                    copy.start()

    def chunk(self, c):
        @pl.when(_step() == 0)
        def _():
            for copy in self.copies(c):
                copy.wait()

        return [held[c] for held in self.held]


def _after_attention(o_ref, h_ref, wo_ref):
    return (h_ref[...].astype(WIDE) + _dot(o_ref[...], wo_ref[0]).astype(LOW).astype(WIDE)).astype(LOW)


def _middle_kernel(number, o_ref, h_ref, wo_ref, wg_ref, wu_ref, wd_ref, wq_ref, wk_ref, wv_ref, table_ref, mid_ref, next_ref, q_ref, k_ref, v_ref,
                   b_s, total_s, *held):
    chunks = Chunks(number, (wg_ref, wu_ref, wd_ref), held)
    chunks.fetch()
    mid_ref[...] = _after_attention(o_ref, h_ref, wo_ref)
    mid = mid_ref[...].astype(WIDE)
    b_s[...] = (mid * _scale(mid)).astype(LOW)
    total_s[...] = jnp.zeros_like(total_s)

    def one(c, _):
        wg, wu, wd = chunks.chunk(c)
        gate, up = _dot(b_s[...], wg), _dot(b_s[...], wu)
        total_s[...] += _dot((gate * jax.nn.sigmoid(gate) * up).astype(LOW), wd)

    _loop(chunks.count, one)
    after = (mid_ref[...].astype(WIDE) + total_s[...].astype(LOW).astype(WIDE)).astype(LOW)
    next_ref[...] = after
    _project(after.astype(WIDE), wq_ref, wk_ref, wv_ref, table_ref, q_ref, k_ref, v_ref)


def middle(o, h, w, number, table):
    tokens, d = h.shape
    args = [o, h, *(w[n] for n in ("wo", "w_gate", "w_up", "w_down", "wq", "wk", "wv")), table]
    specs = [_rows(o.shape[1]), _rows(d), _of_layer(w["wo"], number)] + [ANY] * 3
    specs += [_of_layer(w[n], number + 1) for n in ("wq", "wk", "wv")] + [_whole(*table.shape)]
    size = sum(x.size for x in w.values()) // w["wq"].shape[0]
    return _call(functools.partial(_middle_kernel, number), (tokens // TILE,), specs,
                 [_out((tokens, d), LOW, _rows(d))] * 2 + _qkv_outs(tokens, o.shape[1] // HEAD),
                 [pltpu.VMEM((TILE, d), LOW), pltpu.VMEM((TILE, d), WIDE)] + Chunks.scratch(d, w["w_gate"].shape[2]),
                 "middle", args, 2 * tokens * size)


def _back_kernel(number, last, found, dy_ref, o_ref, turned_ref, h_ref, wo_ref, wg_ref, wu_ref, wd_ref, dh_ref, do_ref, dot_ref, delta_ref, stack_ref,
                 mid_s, b_s, bt_s, dyt_s, db_s, wo_s, gate_s, up_s, down_s, out_s, out_sem, *held):
    first = _step() == 0
    chunks = Chunks(number, (wg_ref, wu_ref, wd_ref), held)
    chunks.fetch()
    mid_s[...] = (_after_attention(o_ref, h_ref, wo_ref) if last else h_ref[...]).astype(WIDE)
    scale = _scale(mid_s[...])
    b = (mid_s[...] * scale).astype(LOW)
    b_s[...] = b
    bt_s[...] = b.T
    dyt_s[...] = dy_ref[...].T
    db_s[...] = jnp.zeros_like(db_s)

    def add(ref, at, more):
        ref[at] = jnp.where(first, 0.0, ref[at]) + more

    def one(c, _):
        wg, wu, wd = chunks.chunk(c)
        gate, up = _dot(b_s[...], wg), _dot(b_s[...], wu)
        dact = _dot_t(dy_ref[...], wd).astype(LOW).astype(WIDE)
        some = jax.nn.sigmoid(gate)
        silu = gate * some
        act = (silu * up).astype(LOW)
        dup = (dact * silu).astype(LOW)
        dgate = (dact * up * (some + silu * (1 - some))).astype(LOW)
        add(down_s, c, _dot(dyt_s[...], act))
        add(gate_s, c, _dot(bt_s[...], dgate))
        add(up_s, c, _dot(bt_s[...], dup))
        db_s[...] += _dot_t(dgate, wg) + _dot_t(dup, wu)

    _loop(chunks.count, one)
    dh = _norm_back(dy_ref[...].astype(WIDE), mid_s[...], scale, db_s[...])
    dh_ref[...] = dh
    do_ref[...] = _dot_t(dh, wo_ref[0]).astype(LOW)
    add(wo_s, slice(None), _dot(turned_ref[...], dh))
    dot_ref[...] = do_ref[...].T
    heads = dot_ref.shape[0] // HEAD
    for n in range(heads):
        delta_ref[n : n + 1, :] = (dot_ref[_part(n), :].astype(WIDE) * turned_ref[_part(n), :].astype(WIDE)).sum(0, keepdims=True)
    delta_ref[heads:, :] = jnp.zeros((EIGHT - heads, TILE), WIDE)

    @pl.when(_last())
    def _():
        row = {name: (at, rows) for name, at, _, rows, column, _ in found if not column}
        every = slice(None)
        many = TILE // row["w_down"][1]

        def copies(c):
            for name in ("w_gate", "w_up", "w_down"):
                at, rows = row[name]
                here = (_at(c * many, many), pl.ds(at, rows)) if name == "w_down" else (every, pl.ds(pl.multiple_of(at + c * rows, EIGHT), rows))
                yield here, pltpu.make_async_copy(out_s.at[here], stack_ref.at[here], out_sem.at[c])

        def put(c, _):
            for (here, copy), value in zip(copies(c), (gate_s[c], up_s[c], down_s[c].T)):
                out_s[here] = value.reshape(-1, here[1].size, value.shape[1]).astype(LOW)
                copy.start()

        _loop(chunks.count, put)
        at, rows = row["wo"]
        here = (every, pl.ds(at, rows))
        out_s[here] = wo_s[...].reshape(DEVICES, rows, wo_s.shape[1]).astype(LOW)
        copy = pltpu.make_async_copy(out_s.at[here], stack_ref.at[here], out_sem.at[chunks.count])
        copy.start()
        for c in range(chunks.count):
            for _, some in copies(c):
                some.wait()
        copy.wait()


def _norm_back(dy, h, scale, db):
    return (dy + scale * (db - h * (scale * scale * jnp.mean(db * h, -1, keepdims=True)))).astype(LOW)


def back(dy, o, turned, h, w, number, last):
    tokens, d = dy.shape
    args = [dy, o, turned, h, *(w[n] for n in ("wo", "w_gate", "w_up", "w_down"))]
    inner, hidden = o.shape[1], w["w_gate"].shape[2]
    n = hidden // TILE
    found, late, _ = pieces(shapes_of(w))
    scratch = [pltpu.VMEM((TILE, d), WIDE), pltpu.VMEM((TILE, d), LOW)] + [pltpu.VMEM((d, TILE), LOW)] * 2 + [pltpu.VMEM((TILE, d), WIDE)]
    scratch += [pltpu.VMEM((inner, d), WIDE)] + [pltpu.VMEM((n, d, TILE), WIDE)] * 3 + [pltpu.VMEM((DEVICES, late, d), LOW)]
    scratch += [pltpu.SemaphoreType.DMA((n + 1,))]
    return _call(functools.partial(_back_kernel, number, last, found), (tokens // TILE,),
                 [_rows(d), _rows(inner) if last else ANY, _columns(inner), _rows(d), _of_layer(w["wo"], number)] + [ANY] * 3,
                 [_out((tokens, d), LOW, _rows(d)), _out((tokens, inner), LOW, _rows(inner)), _out((inner, tokens), LOW, _columns(inner)),
                  _out((EIGHT, tokens), WIDE, _columns(EIGHT)), _out((DEVICES, late, d), LOW, ANY)],
                 scratch + Chunks.scratch(d, hidden), "back", args, 6 * tokens * d * (inner + 3 * hidden))


def _start_kernel(more, found, late, *refs):
    (h_ref, dq_ref, dk_ref, dv_ref, table_ref), backs, (stack_ref,), sums = _split(refs, 5, 5 * more, 1)
    if more:
        dh_ref, wq_ref, wk_ref, wv_ref, dx_ref = backs
    h = h_ref[...].astype(WIDE)
    scale = _scale(h)
    a_turned = (h * scale).astype(LOW).T
    cos, sin = _turns(table_ref)
    dq = jnp.concatenate([_turn(dq_ref[:, at : at + HEAD], cos, -sin) for at in range(0, dq_ref.shape[1], HEAD)], axis=1)
    dk, dv = _turn(dk_ref[...], cos, -sin), dv_ref[...]
    for s, by in zip(sums, (dq, dk, dv)):
        s[...] = jnp.where(_step() == 0, 0.0, s[...]) + _dot(a_turned, by)
    if more:
        da = _dot_t(dq, wq_ref[0]) + _dot_t(dk, wk_ref[0]) + _dot_t(dv, wv_ref[0])
        dx_ref[...] = _norm_back(dh_ref[...].astype(WIDE), h, scale, da)

    @pl.when(_last())
    def _():
        for name, row, lane, rows, column, columns in found:
            if name in EARLY:
                value = sums[EARLY.index(name)][:, pl.ds(column, columns)]
                stack_ref[:, pl.ds(row - late, rows), pl.ds(lane, columns)] = value.reshape(DEVICES, rows, columns).astype(LOW)


def start(h, dq, dk, dv, table, dh, w, number):
    tokens, d = h.shape
    more = number > 0
    shapes = [w[n].shape[1:] for n in EARLY]
    found, late, rows = pieces(shapes_of(w))
    args = [h, dq, dk, dv, table] + ([dh, *(w[n] for n in EARLY)] if more else [])
    specs = [_rows(d), _rows(dq.shape[1])] + [_rows(HEAD)] * 2 + [_whole(*table.shape)]
    specs += [_rows(d)] + [_of_layer(w[n], number) for n in EARLY] if more else []
    stack = (DEVICES, rows - late, d)
    outs = ([_out((tokens, d), LOW, _rows(d))] if more else []) + [_out(stack, LOW, _whole(*stack))]
    got = _call(functools.partial(_start_kernel, more, found, late), (tokens // TILE,), specs, outs,
                [pltpu.VMEM(s, WIDE) for s in shapes], "start", args, 4 * tokens * sum(s[0] * s[1] for s in shapes))
    return (got[0] if more else None), got[-1]


def gradients(x, dy, w):
    layers = w["wq"].shape[0]
    table = turns(x.shape[0])
    kept, h = [], x
    q, k, v = first(x, w, 0, table)
    for number in range(layers):
        o, turned, qt, lse = attend(q, k, v)
        kept.append([h, q, k, v, o, turned, qt, lse])
        if number < layers - 1:
            mid, h, q, k, v = middle(o, h, w, number, table)
        kept[number].append(mid if number < layers - 1 else h)
    late, early, squares, waiting = [None] * layers, [None] * layers, [], []
    by_device = lambda stack: stack.reshape(SIDE * SIDE, CORES, *stack.shape[1:])
    for number in reversed(range(layers)):
        h, q, k, v, o, turned, qt, lse, mid = kept[number]
        dh, do, dot, delta, stack = back(dy, o, turned, mid, w, number, number == layers - 1)
        (dq, dk, dv), sums, square = attend_back(q, qt, k, v, do, dot, lse, delta, [by_device(stack), *waiting], number)
        late[number] = sums[0]
        if waiting:
            early[number + 1] = sums[1]
        squares.append(square)
        dy, stack = start(h, dq, dk, dv, table, dh, w, number)
        waiting = [by_device(stack)]
    return late, early, waiting[0], squares


class Place:
    def __init__(self):
        self.me = lax.axis_index("dp")
        self.core, self.chip = lax.rem(self.me, CORES), lax.div(self.me, CORES)
        self.at = (lax.div(self.chip, SIDE), lax.rem(self.chip, SIDE))
        self.partner = self.me + 1 - 2 * self.core

    def along(self, axis, by):
        x, y = (lax.rem(p + SIDE + by, SIDE) if a == axis else p for a, p in enumerate(self.at))
        return (x * SIDE + y) * CORES + self.core

    def shifted(self, axis, by):
        return lax.rem(self.at[axis] + SIDE + by, SIDE)


def neighbours(place, two=False):
    found = [place.partner] + [place.along(axis, by) for axis in (0, 1) for by in (1, -1)]
    return found + [place.along(axis, 2) for axis in (0, 1)] if two else found


def meet(devices):
    barrier = pltpu.get_barrier_semaphore()
    for d in devices:
        pl.semaphore_signal(barrier, inc=1, device_id={"dp": d}, device_id_type=WHERE)
    pl.semaphore_wait(barrier, len(devices))


def send(src, dst, sems, device):
    return pltpu.make_async_remote_copy(src_ref=src, dst_ref=dst, send_sem=sems[0], recv_sem=sems[1], device_id={"dp": device}, device_id_type=WHERE)


class Streams:
    def __init__(self, place):
        self.place = place

    def of(self, s):
        axis, way = lax.rem(s, 2), 1 - 2 * lax.div(s, 2)
        x, y = self.place.at
        across, down = SIDE - (SIDE - 1) * axis, 1 + (SIDE - 1) * axis
        return x + axis * (y - x), y + axis * (x - y), way, lambda i, j: i * across + j * down

    def device(self, chip):
        return chip * CORES + self.place.core


def near(place, by):
    return lax.rem(place + SIDE + by, SIDE)


class Scatter(Streams):
    @staticmethod
    def scratch(rows, width):
        chips, n = SIDE * SIDE, STREAMS
        shapes = [(chips, rows, width)] * 2 + [(n, 3, SIDE, rows, width // n)] * 2 + [(n, 3, rows, width // n)] * 2
        return [pltpu.VMEM(s, LOW) for s in shapes] + [pltpu.SemaphoreType.DMA((n, 6))] * 2 + [pltpu.SemaphoreType.DMA((2, 3))]

    def __init__(self, place, given, scratch, direct=False):
        super().__init__(place)
        self.given, self.direct = given, direct
        self.own, self.pair, self.s1, self.r1, self.s2, self.r2, self.ssem, self.rsem, self.sem = scratch
        self.rows, self.width = self.own.shape[1:]

    def _pair(self, half):
        lanes, every = _at(half * (self.width // 2), self.width // 2), slice(None)
        return send(self.given.at[:, 1 - self.place.core, :, lanes], self.pair.at[every, every, lanes], (self.sem.at[half, 0], self.sem.at[half, 1]), self.place.partner)

    def _load(self, half):
        lanes, every = _at(half * (self.width // 2), self.width // 2), slice(None)
        return pltpu.make_async_copy(self.given.at[:, self.place.core, :, lanes], self.own.at[every, every, lanes], self.sem.at[half, 2])

    def _stream(self, s):
        a, b, way, number = self.of(s)
        lanes = _at(s * HEAD, HEAD)
        along = (way, -way, 2) if self.direct else (way, -way, way)

        def move(n):
            axis, n = divmod(n, 3)
            to = number(a, near(b, along[n])) if axis else number(near(a, along[n]), b)
            src, dst, n6 = (self.s2, self.r2, n + 3) if axis else (self.s1, self.r1, n)
            return send(src.at[s, n], dst.at[s, n], (self.ssem.at[s, n6], self.rsem.at[s, n6]), self.device(to))

        def chip(i, j):
            n = number(i, j)
            return self.own[n, :, lanes].astype(WIDE) + self.pair[n, :, lanes].astype(WIDE)

        def row(j):
            terms = (0, 1, 2) if self.direct else (1, 2)
            return sum((self.r1[s, n, j].astype(WIDE) for n in terms), chip(a, j))

        return a, b, way, move, lanes, chip, row

    def _each(self, half, body):
        lax.fori_loop(2 * half, 2 * half + 2, lambda s, _: body(s, *self._stream(s)), None)

    def begin(self):
        def one(half, _):
            self._pair(half).start()
            self._load(half).start()

        _loop(2, one)

    def step1(self, half):
        self._load(half).wait()
        self._pair(half).wait_recv()

        def body(s, a, b, way, move, lanes, chip, row):
            to = (near(a, way), near(a, -way), near(a, 2)) if self.direct else (near(a, 2), near(a, -way))

            def one(j, _):
                for n, i in enumerate(to):
                    self.s1[s, n, j] = chip(i, j).astype(LOW)

            _loop(SIDE, one)
            for n in range(len(to)):
                move(n).start()

        self._each(half, body)

    def step2(self, half):
        def body(s, a, b, way, move, lanes, chip, row):
            move(0).wait_recv()

            def one(j, _):
                self.s1[s, 2, j] = (chip(near(a, way), j) + self.r1[s, 0, j].astype(WIDE)).astype(LOW)

            _loop(SIDE, one)
            move(2).start()

        self._each(half, body)

    def step3(self, half):
        def body(s, a, b, way, move, lanes, chip, row):
            for n in (0, 1, 2)[not self.direct :]:
                move(n).wait_recv()
            to = (near(b, way), near(b, -way), near(b, 2)) if self.direct else (near(b, 2), near(b, -way))
            for n, j in enumerate(to):
                self.s2[s, n] = row(j).astype(LOW)
                move(3 + n).start()

        self._each(half, body)

    def step4(self, half):
        def body(s, a, b, way, move, lanes, chip, row):
            move(3).wait_recv()
            self.s2[s, 2] = (row(near(b, way)) + self.r2[s, 0].astype(WIDE)).astype(LOW)
            move(5).start()

        self._each(half, body)

    def end(self, out):
        def body(s, squares):
            a, b, way, move, lanes, chip, row = self._stream(s)
            terms = (0, 1, 2)[not self.direct :]
            for n in terms:
                move(3 + n).wait_recv()
            out[:, lanes] = sum((self.r2[s, n].astype(WIDE) for n in terms), row(b)).astype(LOW)
            for n in range(6):
                move(n).wait_send()
            wide = out[:, lanes].astype(WIDE)
            return squares + (wide * wide).reshape(self.rows // EIGHT, EIGHT, HEAD).sum(0)

        squares = lax.fori_loop(0, STREAMS, body, jnp.zeros((EIGHT, HEAD), WIDE))
        _loop(2, lambda half, _: self._pair(half).wait_send())
        return squares


class Gather(Streams):
    MOVES = 31

    @staticmethod
    def scratch():
        return [pltpu.SemaphoreType.DMA((STREAMS, Gather.MOVES))] * 2

    def __init__(self, place, out, scratch):
        super().__init__(place)
        self.out, (self.ssem, self.rsem) = out, scratch

    def _move(self, s, n, chip, to):
        ref = self.out.at[:, chip, self.place.core, :, _at(s * HEAD, HEAD)]
        return send(ref, ref, (self.ssem.at[s, n], self.rsem.at[s, n]), to)

    def _stream(self, s):
        a, b, way, number = self.of(s)
        place = lambda p, k: near(p, jnp.where(k == 1, -way, jnp.where(k == 2, way, jnp.where(k == 3, 2, 0))))
        on1, back1, on2, back2 = number(near(a, way), b), number(near(a, -way), b), number(a, near(b, way)), number(a, near(b, -way))
        first = lambda n: self._move(s, n, number(place(a, jnp.where(n == 2, 1, 0)), b), self.device(jnp.where(n == 1, back1, on1)))
        on = lambda k: self._move(s, 3 + k, number(place(a, k), b), self.device(on2))
        back = lambda k: self._move(s, 7 + k, number(place(a, k), b), self.device(back2))
        over = lambda k: self._move(s, 11 + k, number(place(a, k), near(b, -way)), self.device(on2))
        pair = lambda k, r: self._move(s, 15 + SIDE * r + k, number(place(a, k), place(b, r)), self.place.partner)
        return first, on, back, over, pair

    def run(self):
        def each(body):
            _loop(STREAMS, lambda s, _: body(*self._stream(s)))

        def spread(on, back, pair, k):
            on(k).start()
            back(k).start()
            pair(k, 0).start()

        def own(first, on, back, over, pair):
            first(0).start()
            first(1).start()

        each(own)
        each(lambda first, on, back, over, pair: spread(on, back, pair, 0))

        def arrive(k, _):
            def body(first, on, back, over, pair):
                first(k - 1).wait_recv()

                @pl.when(k == 1)
                def _():
                    first(2).start()

                spread(on, back, pair, k)

            each(body)

        lax.fori_loop(1, SIDE, arrive, None)

        def rows(k, _):
            def body(first, on, back, over, pair):
                on(k).wait_recv()
                over(k).start()
                pair(k, 1).start()
                back(k).wait_recv()
                pair(k, 2).start()

            each(body)

        _loop(SIDE, rows)

        def far(k, _):
            def body(first, on, back, over, pair):
                over(k).wait_recv()
                pair(k, 3).start()

            each(body)

        _loop(SIDE, far)

        def done(n, _):
            def body(s, _):
                move = self._move(s, n, 0, self.place.partner)
                move.wait_send()

                @pl.when(n >= 15)
                def _():
                    move.wait_recv()

            _loop(STREAMS, body)

        _loop(self.MOVES, done)


def adamw(w, m, v, g):
    m = 0.9 * m + 0.1 * g
    v = 0.95 * v + 0.05 * g * g
    step = m * lax.rsqrt(v + 1e-8) + 0.1 * w
    return (w - 0.02 * step).astype(LOW), m, v


def _fetch(refs, held, sem):
    copies = [pltpu.make_async_copy(ref, to, sem.at[n]) for n, (ref, to) in enumerate(zip(refs, held, strict=True))]
    for copy in copies:
        copy.start()
    return copies


def _beside(sums_s, late_rows, layers):
    parts = (pl.ds(0, late_rows), pl.ds(late_rows, sums_s.shape[1] - late_rows))
    return [sums_s.at[layer, part] for part in parts for layer in range(layers)]


def _finish_kernel(shapes, layers, count, *refs):
    many = len(NAMES)
    sums, squares_refs, (stack,), w, m, v, outs, (sums_s,), squares_held, w_s, m_s, v_s, (sem,), part, square_refs, streams = _split(
        refs, 2 * layers - 1, layers, 1, many, many, many, 3, 1, layers, many, many, many, 1, 9, 3)
    all_ref, own_ref, factor_ref = outs
    squares_s, squares_r, square_sems = square_refs
    found, late_rows, rows = pieces(shapes)
    place = Place()
    meet(neighbours(place, True))
    scatter = Scatter(place, stack, part, True)
    scatter.begin()
    to = _beside(sums_s, late_rows, layers)
    own = to.pop(layers)
    loads = _fetch([*sums, *squares_refs, *(x.at[:, place.me] for x in w), *m, *v], [*to, *squares_held, *w_s, *m_s, *v_s], sem)
    for step in (scatter.step1, scatter.step3):
        _loop(2, lambda half, _: step(half))
    squares = scatter.end(own_ref)
    own[...] = own_ref[...]
    for load in loads:
        load.wait()
    for ref in squares_held:
        squares += ref[...]
    x, y = place.at

    def share(n, squares):
        others = jnp.where(n == 0, 1, SIDE - 1)
        squares_s[n] = squares

        def to(by):
            chip = jnp.where(n == 1, near(x, by), x) * SIDE + jnp.where(n == 2, near(y, by), y)
            device = jnp.where(n == 0, place.partner, chip * CORES + place.core)
            return send(squares_s.at[n], squares_r.at[n, by], (square_sems.at[0, n, by], square_sems.at[1, n, by]), device)

        lax.fori_loop(1, others + 1, lambda by, _: to(by).start(), None)

        def arrive(by, total):
            to(by).wait()
            return total + squares_r[n, by]

        return lax.fori_loop(1, others + 1, arrive, squares)

    squares = lax.fori_loop(0, 3, share, squares)
    factor = jnp.minimum(1.0, 0.5 * lax.rsqrt(jnp.sum(squares) / count + 1e-30))
    factor_ref[...] = jnp.full(factor_ref.shape, factor, WIDE)

    def new(layer, _):
        for name, row, lane, size, column, columns in found:
            n, here, at = NAMES.index(name), (layer, slice(None), pl.ds(column, columns)), (pl.ds(row, size), pl.ds(lane, columns))
            all_ref[(layer, place.chip, place.core, *at)] = adamw(w_s[n][here].astype(WIDE), m_s[n][here], v_s[n][here], sums_s[(layer, *at)].astype(WIDE) * factor)[0]

    _loop(layers, new)
    Gather(place, all_ref, streams).run()


def _outputs_kernel(shapes, layers, *refs):
    many = len(NAMES)
    sums, (factor_ref, all_ref), m, v, new_w, new_m, new_v, (sums_s, factor_s), m_s, v_s, (sem, out_sem) = _split(
        refs, 2 * layers, 2, many, many, many, many, many, 2, many, many)
    found, late_rows, _ = pieces(shapes)
    loads = _fetch([*sums, factor_ref, *m, *v], [*_beside(sums_s, late_rows, layers), factor_s, *m_s, *v_s], sem)
    every = slice(None)
    copies = []
    for name, row, lane, size, column, columns in found:
        copies.append(pltpu.make_async_copy(all_ref.at[:, :, :, pl.ds(row, size), pl.ds(lane, columns)],
                                            new_w[NAMES.index(name)].at[:, :, :, :, pl.ds(column, columns)], out_sem))
        copies[-1].start()
    for load in loads:
        load.wait()
    factor = factor_s[0:1, 0:1]

    def new(layer, _):
        for name, row, lane, size, column, columns in found:
            n, here = NAMES.index(name), (layer, every, pl.ds(column, columns))
            g = sums_s[layer, pl.ds(row, size), pl.ds(lane, columns)].astype(WIDE) * factor
            _, new_m[n][here], new_v[n][here] = adamw(g, m_s[n][here], v_s[n][here], g)

    _loop(layers, new)
    for copy in copies:
        copy.wait()


def finished(late, early, stack, squares, weights, m, v):
    layers = weights[0].shape[0]
    shapes = {name: w.shape[1:] for name, w in zip(NAMES, weights)}
    _, late_rows, rows = pieces(shapes)
    width = shapes["w_down"][1]
    blocks = [(layers, shapes[name][0] // DEVICES, shapes[name][1]) for name in NAMES]
    whole = pl.BlockSpec(memory_space=pltpu.VMEM)
    mine = rows - late_rows
    held = lambda arrays: [pltpu.VMEM(a.shape, a.dtype) for a in arrays]
    given = [*late, *early[1:], *squares]
    moments = [*m, *v]
    sums_s = pltpu.VMEM((layers, rows, width), LOW)
    every, own, factor = pl.pallas_call(
        functools.partial(_finish_kernel, shapes, layers, sum(w.size for w in weights)),
        out_shape=[pltpu.VMEM((layers, SIDE * SIDE, CORES, rows, width), LOW), jax.ShapeDtypeStruct((mine, width), LOW), jax.ShapeDtypeStruct((EIGHT, HEAD), WIDE)],
        in_specs=[ANY] * (len(given) + 1 + len(weights) + len(moments)),
        out_specs=[whole] * 3,
        scratch_shapes=[sums_s] + held(squares) + [pltpu.VMEM(b, LOW) for b in blocks] + held(moments)
        + [pltpu.SemaphoreType.DMA((len(given) + len(weights) + len(moments),))] + Scatter.scratch(mine, width)
        + [pltpu.VMEM((3, EIGHT, HEAD), WIDE), pltpu.VMEM((3, SIDE, EIGHT, HEAD), WIDE), pltpu.SemaphoreType.DMA((2, 3, SIDE))] + Gather.scratch(),
        compiler_params=pltpu.CompilerParams(collective_id=layers, has_side_effects=True, vmem_limit_bytes=VMEM // 2),
        name="finish",
    )(*given, stack, *(w.reshape(layers, DEVICES, *b[1:]) for w, b in zip(weights, blocks)), *moments)
    given = [*late, own, *early[1:], factor]
    out = pl.pallas_call(
        functools.partial(_outputs_kernel, shapes, layers),
        out_shape=[jax.ShapeDtypeStruct((layers, SIDE * SIDE, CORES, *b[1:]), LOW) for b in blocks] + [jax.ShapeDtypeStruct(b, WIDE) for b in blocks * 2],
        in_specs=[ANY] * len(given) + [whole] + [ANY] * len(moments),
        out_specs=[ANY] * len(blocks) + [whole] * len(moments),
        scratch_shapes=[sums_s] + held([factor]) + held(moments) + [pltpu.SemaphoreType.DMA((len(given) + len(moments),)), pltpu.SemaphoreType.DMA],
        compiler_params=pltpu.CompilerParams(vmem_limit_bytes=VMEM // 6),
        name="outputs",
    )(*given, pltpu.with_memory_space_constraint(every, pltpu.VMEM), *moments)
    return (*(o.reshape(layers, *shapes[name]) for name, o in zip(NAMES, out[:7])), *out[7:])


def solution(mesh):

    def step(x, dy, *arrays):
        weights, m, v = (arrays[i : i + 7] for i in (0, 7, 14))
        return finished(*gradients(x[0], dy[0], dict(zip(NAMES, weights))), weights, m, v)

    states, all_of, cut_rows = P(("rep", "dp"), None, None), P(None, None, None), P(None, "dp", None)
    return jax.shard_map(
        step,
        mesh=mesh,
        in_specs=(states, states) + (all_of,) * 7 + (cut_rows,) * 14,
        out_specs=(P("rep", None, None),) * 7 + (P("rep", "dp", None),) * 14,
        check_vma=False,
    )
```

```python
import functools

import jax
import jax.numpy as jnp
import numpy as np
from jax import lax
from jax.experimental import pallas as pl
from jax.experimental.pallas import tpu as pltpu
from jax.sharding import PartitionSpec as P

NAMES = ("wq", "wk", "wv", "wo", "w_gate", "w_up", "w_down")
HEAD = 128
THETA = 10000
NEG = -1e30
HIDDEN = 2 * NEG
LOG2E = 1.4426950408889634
VMEM = 60 * 2**20
TILE = 512
HALF = TILE // 2
SHORT = 64
AHEAD = 3
EIGHT = 8
PARTS = 3
SCALE = HEAD**-0.5
LOW, WIDE = jnp.bfloat16, jnp.float32
ANY = pl.BlockSpec(memory_space=pl.ANY)
ALL = slice(None)

SIDE, CORES = 4, 2
DEVICES = SIDE * SIDE * CORES
STREAMS = 4
WHERE = pl.DeviceIdType.MESH
LATE, EARLY = ("w_gate", "w_up", "w_down", "wo"), ("wq", "wk", "wv")


def pieces(shapes):
    width, row, found = shapes["w_down"][1], 0, []
    for name in LATE:
        rows, cols = shapes[name][0] // DEVICES, shapes[name][1]
        for column in range(0, cols, width):
            found.append((name, row, 0, rows, column, width))
            row += rows
    late, lane = row, 0
    for name in EARLY:
        rows, cols = shapes[name][0] // DEVICES, shapes[name][1]
        for column in range(0, cols, HEAD):
            found.append((name, row, lane, rows, column, HEAD))
            lane = (lane + HEAD) % width
            row += rows if lane == 0 else 0
    return found, late, row


def shapes_of(w):
    return {name: x.shape[1:] for name, x in w.items()}


def _dot(a, b, ca=1, cb=0):
    return lax.dot_general(a, b, (((ca,), (cb,)), ((), ())), preferred_element_type=WIDE)


def _dot_t(a, b):
    return _dot(a, b, 1, 1)


def _loop(count, body):
    lax.fori_loop(0, count, body, None)


def _at(first, size):
    return pl.ds(pl.multiple_of(first, size), size)


def _part(n, size=HEAD):
    return slice(n * size, n * size + size)


def _step():
    return pl.program_id(0)


def _last():
    return _step() == pl.num_programs(0) - 1


def _seen(shape, queries, ahead=0):
    place = [lax.broadcasted_iota(jnp.int32, shape, axis) for axis in (queries, 1 - queries)]
    return place[0] + ahead >= place[1]


def _split(refs, *counts):
    groups = []
    for count in counts:
        groups.append(refs[:count])
        refs = refs[count:]
    return *groups, refs


def far(x):
    return pltpu.with_memory_space_constraint(x, pltpu.HBM)


def _call(kernel, grid, ins, outs, scratch, name, args, flops, **params):
    moved = sum(a.size * a.dtype.itemsize for a in (*args, *(o[0] for o in outs)))
    return pl.pallas_call(
        kernel,
        grid=grid,
        in_specs=ins,
        out_specs=[o[1] for o in outs],
        out_shape=[o[0] for o in outs],
        scratch_shapes=scratch,
        compiler_params=pltpu.CompilerParams(dimension_semantics=("arbitrary",), vmem_limit_bytes=VMEM, **params),
        cost_estimate=pl.CostEstimate(flops=flops, transcendentals=0, bytes_accessed=moved),
        name=name,
    )(*args)


def _rows(cols):
    return pl.BlockSpec((TILE, cols), lambda i: (i, 0))


def _heads(n):
    return pl.BlockSpec((n, TILE, HEAD), lambda i: (0, i, 0))


def _whole(*shape):
    return pl.BlockSpec(shape, lambda i: (0,) * len(shape))


def _of_layer(w, number):
    return pl.BlockSpec((1, *w.shape[1:]), lambda i: (number, 0, 0))


def _out(shape, dtype, spec):
    return jax.ShapeDtypeStruct(shape, dtype), spec


def _scale(h):
    return lax.rsqrt(jnp.mean(h * h, -1, keepdims=True) + 1e-6)


def _turn(t, cos, sin):
    t = t.astype(WIDE)
    return (t * cos + pltpu.roll(t, HEAD // 2, 1) * sin).astype(LOW)


def turns(tokens):
    half = HEAD // 2
    places = np.concatenate([np.arange(SHORT), np.arange(0, tokens, SHORT)])
    angle = places[:, None] * float(THETA) ** (-np.arange(half) / half)
    return jnp.asarray(np.concatenate([np.cos(angle), np.sin(angle)], 1), WIDE)


def _both(t):
    r = pltpu.roll(t, HEAD // 2, 1)
    first = lax.broadcasted_iota(jnp.int32, t.shape, 1) < HEAD // 2
    return jnp.where(first, t, r), jnp.where(first, -r, t)


def _turns(table_ref):
    cos, sin = _both(table_ref[:SHORT, :])
    many = TILE // SHORT
    far = _both(table_ref[pl.ds(pl.multiple_of(SHORT + _step() * many, many), many), :])
    coses, sines = [], []
    for n in range(many):
        far_cos, far_sin = (t[n : n + 1, :] for t in far)
        coses.append(far_cos * cos - far_sin * sin)
        sines.append(far_sin * cos + far_cos * sin)
    return jnp.concatenate(coses, 0), jnp.concatenate(sines, 0)


def _project(h, wq_ref, wk_ref, wv_ref, table_ref, q_ref, k_ref, v_ref):
    a = (h * _scale(h)).astype(LOW)
    cos, sin = _turns(table_ref)
    q = _dot(a, wq_ref[0]).astype(LOW)
    for n in range(q_ref.shape[0]):
        q_ref[n] = _turn(q[:, _part(n)], cos, sin)
    k_ref[...] = _turn(_dot(a, wk_ref[0]).astype(LOW), cos, sin)
    v_ref[...] = _dot(a, wv_ref[0]).astype(LOW)


def _first_kernel(h_ref, *refs):
    _project(h_ref[...].astype(WIDE), *refs)


def _qkv_outs(tokens, heads):
    return [_out((heads, tokens, HEAD), LOW, _heads(heads))] + [_out((tokens, HEAD), LOW, _rows(HEAD))] * 2


def first(h, w, number, table):
    tokens, d = h.shape
    args = [h, w["wq"], w["wk"], w["wv"], table]
    cols = w["wq"].shape[2]
    return _call(_first_kernel, (tokens // TILE,), [_rows(d)] + [_of_layer(x, number) for x in args[1:4]] + [_whole(*table.shape)],
                 _qkv_outs(tokens, cols // HEAD), [], "first", args, 2 * tokens * d * (cols + 2 * HEAD))


def _attend_kernel(q_ref, k_ref, v_ref, o_ref, turned_ref, qt_ref, lse_ref, top_s, mix_s):
    heads = q_ref.shape[0]
    block_q = _step()
    e = SCALE * LOG2E
    top_s[...] = jnp.full(top_s.shape, NEG, WIDE)
    mix_s[...] = jnp.zeros(mix_s.shape, WIDE)
    def block(first_half, halves, low, masked):
        size = halves * HALF
        here = _at(first_half * HALF, size)
        k, values = k_ref[here, :], jnp.concatenate([v_ref[here, :].T, jnp.ones((EIGHT, size), LOW)])
        if masked:
            ok = _seen((size, TILE - low), 1)
        score = lambda n: _dot_t(k, q_ref[n, low:, :])
        ready = [score(n) for n in range(AHEAD)]
        for n in range(heads):
            if n + AHEAD < heads:
                ready.append(score(n + AHEAD))
            s = jnp.where(ok, ready[n], HIDDEN) if masked else ready[n]
            row = slice(n, n + 1)
            old = top_s[row, low:]
            top = jnp.maximum(old, s.max(0, keepdims=True))
            top_s[row, low:] = top
            mix_s[n, :, low:] = mix_s[n, :, low:] * jnp.exp2((old - top) * e) + _dot(values, jnp.exp2((s - top) * e).astype(LOW))

    _loop(block_q, lambda j, _: block(2 * j, 2, 0, False))
    block(2 * block_q, 1, 0, True)
    block(2 * block_q + 1, 1, HALF, True)
    for n in range(heads):
        total, row = mix_s[n, HEAD : HEAD + 1, :], slice(n, n + 1)
        turned = (mix_s[n, :HEAD, :] * (1 / total)).astype(LOW)
        turned_ref[_part(n), :] = turned
        o_ref[:, _part(n)] = turned.T
        qt_ref[n] = q_ref[n].T
        lse_ref[row, :] = top_s[row, :] * SCALE + jnp.log(total)
    lse_ref[heads:, :] = jnp.zeros((EIGHT - heads, TILE), WIDE)


def _columns(rows):
    return pl.BlockSpec((rows, TILE), lambda i: (0, i))


def _head_columns(heads):
    return pl.BlockSpec((heads, HEAD, TILE), lambda i: (0, 0, i))


def attend(q, k, v):
    heads, tokens, _ = q.shape
    inner = heads * HEAD
    return _call(_attend_kernel, (tokens // TILE,), [_heads(heads), _whole(tokens, HEAD), _whole(tokens, HEAD)],
                 [_out((tokens, inner), LOW, _rows(inner)), _out((inner, tokens), LOW, _columns(inner)),
                  _out((heads, HEAD, tokens), LOW, _head_columns(heads)), _out((EIGHT, tokens), WIDE, _columns(EIGHT))],
                 [pltpu.VMEM((heads, TILE), WIDE), pltpu.VMEM((heads, HEAD + EIGHT, TILE), WIDE)],
                 "attend", [q, k, v], 2 * heads * tokens * tokens * HEAD)


def _attend_back_kernel(many, refs):
    ins, stacks, (dq_ref, dk_ref, dv_ref), sums, (squares_ref,), held, refs = _split(refs, 8, many, 3, many, 1, 5)
    q_ref, qt_ref, k_ref, v_ref, do_ref, dot_ref, lse_ref, delta_ref = ins
    dq_s, dk_s, dv_s, beside_s, take_s = held
    heads = q_ref.shape[0]
    block_q = _step()
    steps = k_ref.shape[0] // TILE
    e = SCALE * LOG2E
    place = Place()
    parts = [Scatter(place, s, refs[_part(at, 9)]) for at, s in enumerate(stacks)]

    def travel(step, tick, *ticks):
        one, other = (n * steps * steps // 16 for n in ticks)

        if parts:
            @pl.when((tick == one) | (tick == other))
            def _():
                for part in parts:
                    getattr(part, step)(jnp.where(tick == other, 1, 0))

    @pl.when(block_q == 0)
    def _():
        if parts:
            meet(neighbours(place))
        for part in parts:
            part.begin()
        lane = lax.broadcasted_iota(jnp.int32, (HALF, HEAD), 1)

        def clear(n, _):
            dk_s[n] = jnp.zeros((HEAD, HALF), WIDE)
            dv_s[n] = jnp.zeros((HEAD, HALF), WIDE)

        def take(n, _):
            for which in (0, 1):
                mine = (lane % EIGHT == n) & (lane // (EIGHT * PARTS) == which)
                take_s[which, n] = jnp.where(mine, -1.0, 0.0).astype(LOW)

        _loop(2 * steps, clear)
        _loop(heads, take)

    dq_s[...] = jnp.zeros_like(dq_s)
    of = lambda n: (ALL, _part(n))
    lines = []
    for rest in (lse_ref[...] * (1 / SCALE), delta_ref[...]):
        for _ in range(PARTS):
            lines.append(rest.astype(LOW).astype(WIDE))
            rest = rest - lines[-1]
    lines.append(jnp.zeros((HEAD - EIGHT * len(lines), TILE), WIDE))
    beside_s[...] = jnp.concatenate(lines).T.astype(LOW)

    def block(keys, low):
        here = _at(keys * HALF, HALF)
        k, v = k_ref[here, :], v_ref[here, :]
        ok = _seen((TILE - low, HALF), 0, (2 * block_q - keys) * HALF + low)
        beside = lambda x: jnp.concatenate([x, beside_s[low:, :]], 1)
        score = lambda n: (_dot_t(beside(q_ref[n, low:, :]), jnp.concatenate([k, take_s[0, n]], 1)),
                           _dot_t(beside(do_ref[low:, _part(n)]), jnp.concatenate([v, take_s[1, n]], 1)))
        s, dp = score(0)
        dk, dv = None, None
        for n in range(heads):
            after = score(n + 1) if n + 1 < heads else (None, None)
            p = jnp.where(ok, jnp.exp2(s * e), 0.0)
            ds = (p * dp).astype(LOW)
            more_v, more_k = _dot(dot_ref[_part(n), low:], p.astype(LOW)), _dot(qt_ref[n, :, low:], ds)
            dv, dk = (dv + more_v, dk + more_k) if n else (more_v, more_k)
            dq_s[n, low:, :] += _dot(ds, k)
            s, dp = after
        dk_s[keys] += dk
        dv_s[keys] += dv

    def one(j, _):
        tick = block_q * block_q + j
        travel("step1", tick, 3, 4)
        travel("step2", tick, 7, 9)
        travel("step3", tick, 11, 13)
        travel("step4", tick, 14, 15)
        block(j, 0)

    _loop(2 * block_q + 1, one)
    block(2 * block_q + 1, HALF)
    for n in range(heads):
        dq_ref[of(n)] = (dq_s[n] * SCALE).astype(LOW)

    @pl.when(block_q == steps - 1)
    def _():
        def turn(n, _):
            here = _at(n * HALF, HALF)
            dk_ref[here, :] = (dk_s[n] * SCALE).T.astype(LOW)
            dv_ref[here, :] = dv_s[n].T.astype(LOW)

        _loop(2 * steps, turn)
        squares_ref[...] = sum((part.end(out) for part, out in zip(parts, sums)), jnp.zeros((EIGHT, HEAD), WIDE))


def attend_back(q, qt, k, v, do, dot, lse, delta, stacks, number):
    heads, tokens, _ = q.shape
    wide, kv = _rows(heads * HEAD), _whole(tokens, HEAD)
    rows = [s.shape[2] for s in stacks]
    width = stacks[0].shape[3] if stacks else HEAD
    scratch = [pltpu.VMEM((heads, TILE, HEAD), WIDE)] + [pltpu.VMEM((tokens // HALF, HEAD, HALF), WIDE)] * 2
    scratch += [pltpu.VMEM((TILE, HEAD), LOW), pltpu.VMEM((2, heads, HALF, HEAD), LOW)]
    got = _call(lambda *refs: _attend_back_kernel(len(rows), refs), (tokens // TILE,),
                [_heads(heads), _head_columns(heads), kv, kv, wide, _columns(heads * HEAD)] + [_columns(EIGHT)] * 2 + [ANY] * len(rows),
                [_out((tokens, heads * HEAD), LOW, wide)] + [_out((tokens, HEAD), LOW, kv)] * 2
                + [_out((n, width), LOW, _whole(n, width)) for n in rows] + [_out((EIGHT, HEAD), WIDE, _whole(EIGHT, HEAD))],
                scratch + [s for n in rows for s in Scatter.scratch(n, width)],
                "attend_back", [q, qt, k, v, do, dot, lse, delta, *(far(s) for s in stacks)], 5 * heads * tokens * tokens * HEAD, collective_id=number, has_side_effects=True)
    return got[:3], got[3:-1], got[-1]


class Chunks:
    @staticmethod
    def scratch(d, hidden):
        n = hidden // TILE
        return [pltpu.VMEM((n, d, TILE), LOW)] * 2 + [pltpu.VMEM((n, TILE, d), LOW), pltpu.SemaphoreType.DMA((n, 3))]

    def __init__(self, number, refs, held):
        self.number, self.refs, self.held, self.sem = number, refs, held[:3], held[3]
        self.count = held[0].shape[0]

    def copies(self, c):
        units = _at(c * TILE, TILE)
        every = ALL
        return [pltpu.make_async_copy(ref.at[at], held.at[c], self.sem.at[c, n]) for n, (ref, held, at) in enumerate(
            zip(self.refs, self.held, ((self.number, every, units), (self.number, every, units), (self.number, units, every))))]

    def fetch(self):
        @pl.when(_step() == 0)
        def _():
            for c in range(self.count):
                for copy in self.copies(c):
                    copy.start()

    def chunk(self, c):
        @pl.when(_step() == 0)
        def _():
            for copy in self.copies(c):
                copy.wait()

        return [held[c] for held in self.held]


def _slot(n):
    return lax.rem(n, 2)


class Passing:
    @staticmethod
    def scratch(many):
        return [pltpu.VMEM((2, TILE, TILE), WIDE)] * many + [pltpu.SemaphoreType.DMA((2, many))]

    def __init__(self, refs, held, out):
        self.refs, self.held, self.sem, self.out = refs, held[:-1], held[-1], out
        self.count = refs[0].shape[0]
        self.first, self.total = _step() * self.count, pl.num_programs(0) * self.count

    def _each(self, n):
        slot, chunk, rows = _slot(n), lax.rem(n, self.count), _at(lax.div(n, self.count) * TILE, TILE)
        for at, (ref, held) in enumerate(zip(self.refs, self.held)):
            ends = (held.at[slot], ref.at[chunk, rows, :])
            yield pltpu.make_async_copy(*(ends if self.out else ends[::-1]), self.sem.at[slot, at])

    def start(self, n):
        for copy in self._each(n):
            copy.start()

    def wait(self, n):
        for copy in self._each(n):
            copy.wait()


def _after_attention(o_ref, h_ref, wo_ref):
    return (h_ref[...].astype(WIDE) + _dot(o_ref[...], wo_ref[0]).astype(LOW).astype(WIDE)).astype(LOW)


def _middle_kernel(number, o_ref, h_ref, wo_ref, wg_ref, wu_ref, wd_ref, wq_ref, wk_ref, wv_ref, table_ref, mid_ref, next_ref, q_ref, k_ref, v_ref,
                   gate_ref, up_ref, b_s, total_s, *held):
    held, passed = _split(held, 4)
    chunks, passing = Chunks(number, (wg_ref, wu_ref, wd_ref), held), Passing((gate_ref, up_ref), passed, True)
    chunks.fetch()
    mid_ref[...] = _after_attention(o_ref, h_ref, wo_ref)
    mid = mid_ref[...].astype(WIDE)
    b_s[...] = (mid * _scale(mid)).astype(LOW)
    total_s[...] = jnp.zeros_like(total_s)

    def one(c, _):
        wg, wu, wd = chunks.chunk(c)
        n = passing.first + c
        pl.when(n > 1)(lambda: passing.wait(n - 2))
        gate, up = _dot(b_s[...], wg), _dot(b_s[...], wu)
        for slots, value in zip(passing.held, (gate, up)):
            slots[_slot(n)] = value
        total_s[...] += _dot((gate * jax.nn.sigmoid(gate) * up).astype(LOW), wd)
        passing.start(n)

    _loop(chunks.count, one)
    after = (mid_ref[...].astype(WIDE) + total_s[...].astype(LOW).astype(WIDE)).astype(LOW)
    next_ref[...] = after
    _project(after.astype(WIDE), wq_ref, wk_ref, wv_ref, table_ref, q_ref, k_ref, v_ref)
    for left in (2, 1):
        pl.when(_last())(lambda: passing.wait(passing.first + chunks.count - left))


def middle(o, h, w, number, table):
    tokens, d = h.shape
    args = [o, h, w["wo"], *(far(w[n]) for n in ("w_gate", "w_up", "w_down")), *(w[n] for n in EARLY), table]
    specs = [_rows(o.shape[1]), _rows(d), _of_layer(w["wo"], number)] + [ANY] * 3
    specs += [_of_layer(w[n], number + 1) for n in ("wq", "wk", "wv")] + [_whole(*table.shape)]
    size = sum(x.size for x in w.values()) // w["wq"].shape[0]
    hidden = w["w_gate"].shape[2]
    return _call(functools.partial(_middle_kernel, number), (tokens // TILE,), specs,
                 [_out((tokens, d), LOW, _rows(d))] * 2 + _qkv_outs(tokens, o.shape[1] // HEAD) + [_out((hidden // TILE, tokens, TILE), WIDE, ANY)] * 2,
                 [pltpu.VMEM((TILE, d), LOW), pltpu.VMEM((TILE, d), WIDE)] + Chunks.scratch(d, hidden) + Passing.scratch(2),
                 "middle", args, 2 * tokens * size)


def _back_kernel(number, last, found, dy_ref, o_ref, turned_ref, h_ref, wo_ref, wg_ref, wu_ref, wd_ref, gate_ref, up_ref, dh_ref, do_ref, dot_ref, delta_ref, stack_ref,
                 mid_s, b_s, bt_s, dyt_s, db_s, wo_s, gate_s, up_s, down_s, out_s, out_sem, *held):
    first = _step() == 0
    held, passed = _split(held, 4)
    chunks, passing = Chunks(number, (wg_ref, wu_ref, wd_ref), held), None
    if not last:
        passing = Passing((gate_ref, up_ref), passed, False)
        pl.when(first)(lambda: passing.start(0))
    chunks.fetch()
    mid_s[...] = (_after_attention(o_ref, h_ref, wo_ref) if last else h_ref[...]).astype(WIDE)
    scale = _scale(mid_s[...])
    b = (mid_s[...] * scale).astype(LOW)
    b_s[...] = b
    bt_s[...] = b.T
    dyt_s[...] = dy_ref[...].T
    db_s[...] = jnp.zeros_like(db_s)

    def add(ref, at, more):
        ref[at] = jnp.where(first, 0.0, ref[at]) + more

    def one(c, _):
        wg, wu, wd = chunks.chunk(c)
        if last:
            gate, up = _dot(b_s[...], wg), _dot(b_s[...], wu)
        else:
            n = passing.first + c
            pl.when(n < passing.total - 1)(lambda: passing.start(n + 1))
            passing.wait(n)
            gate, up = (slots[_slot(n)] for slots in passing.held)
        dact = _dot_t(dy_ref[...], wd).astype(LOW).astype(WIDE)
        some = jax.nn.sigmoid(gate)
        silu = gate * some
        act = (silu * up).astype(LOW)
        dup = (dact * silu).astype(LOW)
        dgate = (dact * up * (some + silu * (1 - some))).astype(LOW)
        add(down_s, c, _dot(dyt_s[...], act))
        add(gate_s, c, _dot(bt_s[...], dgate))
        add(up_s, c, _dot(bt_s[...], dup))
        db_s[...] += _dot_t(dgate, wg) + _dot_t(dup, wu)

    _loop(chunks.count, one)
    dh = _norm_back(dy_ref[...].astype(WIDE), mid_s[...], scale, db_s[...])
    dh_ref[...] = dh
    do_ref[...] = _dot_t(dh, wo_ref[0]).astype(LOW)
    add(wo_s, ALL, _dot(turned_ref[...], dh))
    dot_ref[...] = do_ref[...].T
    heads = dot_ref.shape[0] // HEAD
    for n in range(heads):
        delta_ref[n : n + 1, :] = (dot_ref[_part(n), :].astype(WIDE) * turned_ref[_part(n), :].astype(WIDE)).sum(0, keepdims=True)
    delta_ref[heads:, :] = jnp.zeros((EIGHT - heads, TILE), WIDE)

    @pl.when(_last())
    def _():
        row = {name: (at, rows) for name, at, _, rows, column, _ in found if not column}
        every = ALL
        many = TILE // row["w_down"][1]

        def copies(c):
            for name in ("w_gate", "w_up", "w_down"):
                at, rows = row[name]
                here = (_at(c * many, many), pl.ds(at, rows)) if name == "w_down" else (every, pl.ds(pl.multiple_of(at + c * rows, EIGHT), rows))
                yield here, pltpu.make_async_copy(out_s.at[here], stack_ref.at[here], out_sem.at[c])

        def put(c, _):
            for (here, copy), value in zip(copies(c), (gate_s[c], up_s[c], down_s[c].T)):
                out_s[here] = value.reshape(-1, here[1].size, value.shape[1]).astype(LOW)
                copy.start()

        _loop(chunks.count, put)
        at, rows = row["wo"]
        here = (every, pl.ds(at, rows))
        out_s[here] = wo_s[...].reshape(DEVICES, rows, wo_s.shape[1]).astype(LOW)
        copy = pltpu.make_async_copy(out_s.at[here], stack_ref.at[here], out_sem.at[chunks.count])
        copy.start()
        for c in range(chunks.count):
            for _, some in copies(c):
                some.wait()
        copy.wait()


def _norm_back(dy, h, scale, db):
    return (dy + scale * (db - h * (scale * scale * jnp.mean(db * h, -1, keepdims=True)))).astype(LOW)


def back(dy, o, turned, h, gates, w, number, last):
    tokens, d = dy.shape
    args = [dy, o if last else far(o), turned, h, w["wo"], *(far(w[n]) for n in ("w_gate", "w_up", "w_down")), *gates]
    inner, hidden = o.shape[1], w["w_gate"].shape[2]
    n = hidden // TILE
    found, late, _ = pieces(shapes_of(w))
    scratch = [pltpu.VMEM((TILE, d), WIDE), pltpu.VMEM((TILE, d), LOW)] + [pltpu.VMEM((d, TILE), LOW)] * 2 + [pltpu.VMEM((TILE, d), WIDE)]
    scratch += [pltpu.VMEM((inner, d), WIDE)] + [pltpu.VMEM((n, d, TILE), WIDE)] * 3 + [pltpu.VMEM((DEVICES, late, d), LOW)]
    scratch += [pltpu.SemaphoreType.DMA((n + 1,))]
    return _call(functools.partial(_back_kernel, number, last, found), (tokens // TILE,),
                 [_rows(d), _rows(inner) if last else ANY, _columns(inner), _rows(d), _of_layer(w["wo"], number)] + [ANY] * 5,
                 [_out((tokens, d), LOW, _rows(d)), _out((tokens, inner), LOW, _rows(inner)), _out((inner, tokens), LOW, _columns(inner)),
                  _out((EIGHT, tokens), WIDE, _columns(EIGHT)), _out((DEVICES, late, d), LOW, ANY)],
                 scratch + Chunks.scratch(d, hidden) + ([] if last else Passing.scratch(2)), "back", args, 6 * tokens * d * (inner + 3 * hidden))


def _start_kernel(more, found, late, *refs):
    (h_ref, dq_ref, dk_ref, dv_ref, table_ref), backs, (stack_ref,), sums = _split(refs, 5, 5 * more, 1)
    if more:
        dh_ref, wq_ref, wk_ref, wv_ref, dx_ref = backs
    h = h_ref[...].astype(WIDE)
    scale = _scale(h)
    a_turned = (h * scale).astype(LOW).T
    cos, sin = _turns(table_ref)
    dq = jnp.concatenate([_turn(dq_ref[:, at : at + HEAD], cos, -sin) for at in range(0, dq_ref.shape[1], HEAD)], axis=1)
    dk, dv = _turn(dk_ref[...], cos, -sin), dv_ref[...]
    for s, by in zip(sums, (dq, dk, dv)):
        s[...] = jnp.where(_step() == 0, 0.0, s[...]) + _dot(a_turned, by)
    if more:
        da = _dot_t(dq, wq_ref[0]) + _dot_t(dk, wk_ref[0]) + _dot_t(dv, wv_ref[0])
        dx_ref[...] = _norm_back(dh_ref[...].astype(WIDE), h, scale, da)

    @pl.when(_last())
    def _():
        for name, row, lane, rows, column, columns in found:
            if name in EARLY:
                value = sums[EARLY.index(name)][:, pl.ds(column, columns)]
                stack_ref[:, pl.ds(row - late, rows), pl.ds(lane, columns)] = value.reshape(DEVICES, rows, columns).astype(LOW)


def start(h, dq, dk, dv, table, dh, w, number):
    tokens, d = h.shape
    more = number > 0
    shapes = [w[n].shape[1:] for n in EARLY]
    found, late, rows = pieces(shapes_of(w))
    args = [h, dq, dk, dv, table] + ([dh, *(w[n] for n in EARLY)] if more else [])
    specs = [_rows(d), _rows(dq.shape[1])] + [_rows(HEAD)] * 2 + [_whole(*table.shape)]
    specs += [_rows(d)] + [_of_layer(w[n], number) for n in EARLY] if more else []
    stack = (DEVICES, rows - late, d)
    outs = ([_out((tokens, d), LOW, _rows(d))] if more else []) + [_out(stack, LOW, _whole(*stack))]
    got = _call(functools.partial(_start_kernel, more, found, late), (tokens // TILE,), specs, outs,
                [pltpu.VMEM(s, WIDE) for s in shapes], "start", args, 4 * tokens * sum(s[0] * s[1] for s in shapes))
    return (got[0] if more else None), got[-1]


def gradients(x, dy, w):
    layers = w["wq"].shape[0]
    table = turns(x.shape[0])
    kept, h = [], x
    q, k, v = first(x, w, 0, table)
    for number in range(layers):
        o, turned, qt, lse = attend(q, k, v)
        kept.append([h, q, k, v, o, turned, qt, lse])
        if number < layers - 1:
            mid, h, q, k, v, *gates = middle(o, h, w, number, table)
            kept[number] += [mid, gates]
        else:
            kept[number] += [h, [h, h]]
    late, early, squares, waiting = [None] * layers, [None] * layers, [], []
    by_device = lambda stack: stack.reshape(SIDE * SIDE, CORES, *stack.shape[1:])
    for number in reversed(range(layers)):
        h, q, k, v, o, turned, qt, lse, mid, gates = kept[number]
        dh, do, dot, delta, stack = back(dy, o, turned, mid, gates, w, number, number == layers - 1)
        (dq, dk, dv), sums, square = attend_back(q, qt, k, v, do, dot, lse, delta, [by_device(stack), *waiting], number)
        late[number] = sums[0]
        if waiting:
            early[number + 1] = sums[1]
        squares.append(square)
        dy, stack = start(h, dq, dk, dv, table, dh, w, number)
        waiting = [by_device(stack)]
    return late, early, waiting[0], squares


class Place:
    def __init__(self):
        self.me = lax.axis_index("dp")
        self.core, self.chip = lax.rem(self.me, CORES), lax.div(self.me, CORES)
        self.at = (lax.div(self.chip, SIDE), lax.rem(self.chip, SIDE))
        self.partner = self.me + 1 - 2 * self.core

    def along(self, axis, by):
        x, y = (lax.rem(p + SIDE + by, SIDE) if a == axis else p for a, p in enumerate(self.at))
        return (x * SIDE + y) * CORES + self.core

    def shifted(self, axis, by):
        return lax.rem(self.at[axis] + SIDE + by, SIDE)


def neighbours(place, two=False):
    found = [place.partner] + [place.along(axis, by) for axis in (0, 1) for by in (1, -1)]
    return found + [place.along(axis, 2) for axis in (0, 1)] if two else found


def meet(devices):
    barrier = pltpu.get_barrier_semaphore()
    for d in devices:
        pl.semaphore_signal(barrier, inc=1, device_id={"dp": d}, device_id_type=WHERE)
    pl.semaphore_wait(barrier, len(devices))


def send(src, dst, sems, device):
    return pltpu.make_async_remote_copy(src_ref=src, dst_ref=dst, send_sem=sems[0], recv_sem=sems[1], device_id={"dp": device}, device_id_type=WHERE)


class Streams:
    def __init__(self, place):
        self.place = place

    def of(self, s):
        axis, way = lax.rem(s, 2), 1 - 2 * lax.div(s, 2)
        x, y = self.place.at
        across, down = SIDE - (SIDE - 1) * axis, 1 + (SIDE - 1) * axis
        return x + axis * (y - x), y + axis * (x - y), way, lambda i, j: i * across + j * down

    def device(self, chip):
        return chip * CORES + self.place.core


def near(place, by):
    return lax.rem(place + SIDE + by, SIDE)


class Scatter(Streams):
    @staticmethod
    def scratch(rows, width):
        chips, n = SIDE * SIDE, STREAMS
        shapes = [(chips, rows, width)] * 2 + [(n, 3, SIDE, rows, width // n)] * 2 + [(n, 3, rows, width // n)] * 2
        return [pltpu.VMEM(s, LOW) for s in shapes] + [pltpu.SemaphoreType.DMA((n, 6))] * 2 + [pltpu.SemaphoreType.DMA((2, 3))]

    def __init__(self, place, given, scratch, direct=False):
        super().__init__(place)
        self.given, self.direct = given, direct
        self.straight = tuple(range(3))[not direct :]
        self.own, self.pair, self.s1, self.r1, self.s2, self.r2, self.ssem, self.rsem, self.sem = scratch
        self.rows, self.width = self.own.shape[1:]

    def _half(self, half):
        size = self.width // 2
        return _at(half * size, size)

    def _pair(self, half):
        lanes = self._half(half)
        return send(self.given.at[:, 1 - self.place.core, :, lanes], self.pair.at[ALL, ALL, lanes], (self.sem.at[half, 0], self.sem.at[half, 1]), self.place.partner)

    def _load(self, half):
        lanes = self._half(half)
        return pltpu.make_async_copy(self.given.at[:, self.place.core, :, lanes], self.own.at[ALL, ALL, lanes], self.sem.at[half, 2])

    def _stream(self, s):
        a, b, way, number = self.of(s)
        lanes = _at(s * HEAD, HEAD)
        along = (way, -way, 2) if self.direct else (way, -way, way)

        def move(n):
            axis, n = divmod(n, 3)
            to = number(a, near(b, along[n])) if axis else number(near(a, along[n]), b)
            src, dst, n6 = (self.s2, self.r2, n + 3) if axis else (self.s1, self.r1, n)
            return send(src.at[s, n], dst.at[s, n], (self.ssem.at[s, n6], self.rsem.at[s, n6]), self.device(to))

        def chip(i, j):
            n = number(i, j)
            return self.own[n, :, lanes].astype(WIDE) + self.pair[n, :, lanes].astype(WIDE)

        def row(j):
            terms = self.straight
            return sum((self.r1[s, n, j].astype(WIDE) for n in terms), chip(a, j))

        return a, b, way, move, lanes, chip, row

    def _each(self, half, body):
        lax.fori_loop(2 * half, 2 * half + 2, lambda s, _: body(s, *self._stream(s)), None)

    def begin(self):
        def one(half, _):
            self._pair(half).start()
            self._load(half).start()

        _loop(2, one)

    def step1(self, half):
        self._load(half).wait()
        self._pair(half).wait_recv()

        def body(s, a, b, way, move, lanes, chip, row):
            to = (near(a, way), near(a, -way), near(a, 2)) if self.direct else (near(a, 2), near(a, -way))

            def one(j, _):
                for n, i in enumerate(to):
                    self.s1[s, n, j] = chip(i, j).astype(LOW)

            _loop(SIDE, one)
            for n in range(len(to)):
                move(n).start()

        self._each(half, body)

    def step2(self, half):
        def body(s, a, b, way, move, lanes, chip, row):
            move(0).wait_recv()

            def one(j, _):
                self.s1[s, 2, j] = (chip(near(a, way), j) + self.r1[s, 0, j].astype(WIDE)).astype(LOW)

            _loop(SIDE, one)
            move(2).start()

        self._each(half, body)

    def step3(self, half):
        def body(s, a, b, way, move, lanes, chip, row):
            for n in self.straight:
                move(n).wait_recv()
            to = (near(b, way), near(b, -way), near(b, 2)) if self.direct else (near(b, 2), near(b, -way))
            for n, j in enumerate(to):
                self.s2[s, n] = row(j).astype(LOW)
                move(3 + n).start()

        self._each(half, body)

    def step4(self, half):
        def body(s, a, b, way, move, lanes, chip, row):
            move(3).wait_recv()
            self.s2[s, 2] = (row(near(b, way)) + self.r2[s, 0].astype(WIDE)).astype(LOW)
            move(5).start()

        self._each(half, body)

    def end(self, out):
        def body(s, squares):
            a, b, way, move, lanes, chip, row = self._stream(s)
            terms = self.straight
            for n in terms:
                move(3 + n).wait_recv()
            out[:, lanes] = sum((self.r2[s, n].astype(WIDE) for n in terms), row(b)).astype(LOW)
            for n in range(6):
                move(n).wait_send()
            wide = out[:, lanes].astype(WIDE)
            return squares + (wide * wide).reshape(self.rows // EIGHT, EIGHT, HEAD).sum(0)

        squares = lax.fori_loop(0, STREAMS, body, jnp.zeros((EIGHT, HEAD), WIDE))
        _loop(2, lambda half, _: self._pair(half).wait_send())
        return squares


class Gather(Streams):
    MOVES = 31

    @staticmethod
    def scratch():
        return [pltpu.SemaphoreType.DMA((STREAMS, Gather.MOVES))] * 2

    def __init__(self, place, out, scratch):
        super().__init__(place)
        self.out, (self.ssem, self.rsem) = out, scratch

    def _move(self, s, n, chip, to):
        ref = self.out.at[:, chip, self.place.core, :, _at(s * HEAD, HEAD)]
        return send(ref, ref, (self.ssem.at[s, n], self.rsem.at[s, n]), to)

    def _stream(self, s):
        a, b, way, number = self.of(s)
        place = lambda p, k: near(p, jnp.where(k == 1, -way, jnp.where(k == 2, way, jnp.where(k == 3, 2, 0))))
        on1, back1, on2, back2 = number(near(a, way), b), number(near(a, -way), b), number(a, near(b, way)), number(a, near(b, -way))
        first = lambda n: self._move(s, n, number(place(a, jnp.where(n == 2, 1, 0)), b), self.device(jnp.where(n == 1, back1, on1)))
        on = lambda k: self._move(s, 3 + k, number(place(a, k), b), self.device(on2))
        back = lambda k: self._move(s, 7 + k, number(place(a, k), b), self.device(back2))
        over = lambda k: self._move(s, 11 + k, number(place(a, k), near(b, -way)), self.device(on2))
        pair = lambda k, r: self._move(s, 15 + SIDE * r + k, number(place(a, k), place(b, r)), self.place.partner)
        return first, on, back, over, pair

    def run(self):
        def each(body):
            _loop(STREAMS, lambda s, _: body(*self._stream(s)))

        def spread(on, back, pair, k):
            on(k).start()
            back(k).start()
            pair(k, 0).start()

        def own(first, on, back, over, pair):
            first(0).start()
            first(1).start()

        each(own)
        each(lambda first, on, back, over, pair: spread(on, back, pair, 0))

        def arrive(k, _):
            def body(first, on, back, over, pair):
                first(k - 1).wait_recv()

                @pl.when(k == 1)
                def _():
                    first(2).start()

                spread(on, back, pair, k)

            each(body)

        lax.fori_loop(1, SIDE, arrive, None)

        def rows(k, _):
            def body(first, on, back, over, pair):
                on(k).wait_recv()
                over(k).start()
                pair(k, 1).start()
                back(k).wait_recv()
                pair(k, 2).start()

            each(body)

        _loop(SIDE, rows)

        def far(k, _):
            def body(first, on, back, over, pair):
                over(k).wait_recv()
                pair(k, 3).start()

            each(body)

        _loop(SIDE, far)

        def done(n, _):
            def body(s, _):
                move = self._move(s, n, 0, self.place.partner)
                move.wait_send()

                @pl.when(n >= 15)
                def _():
                    move.wait_recv()

            _loop(STREAMS, body)

        _loop(self.MOVES, done)


def adamw(w, m, v, g):
    m = 0.9 * m + 0.1 * g
    v = 0.95 * v + 0.05 * g * g
    step = m * lax.rsqrt(v + 1e-8) + 0.1 * w
    return (w - 0.02 * step).astype(LOW), m, v


def _fetch(refs, held, sem):
    copies = [pltpu.make_async_copy(ref, to, sem.at[n]) for n, (ref, to) in enumerate(zip(refs, held, strict=True))]
    for copy in copies:
        copy.start()
    return copies


def _beside(sums_s, late_rows, layers):
    parts = (pl.ds(0, late_rows), pl.ds(late_rows, sums_s.shape[1] - late_rows))
    return [sums_s.at[layer, part] for part in parts for layer in range(layers)]


def _finish_kernel(shapes, layers, count, *refs):
    many = len(NAMES)
    sums, squares_refs, (stack,), w, m, v, outs, (sums_s,), squares_held, w_s, m_s, v_s, (sem,), part, square_refs, streams = _split(
        refs, 2 * layers - 1, layers, 1, many, many, many, 3, 1, layers, many, many, many, 1, 9, 3)
    all_ref, own_ref, factor_ref = outs
    squares_s, squares_r, square_sems = square_refs
    found, late_rows, rows = pieces(shapes)
    place = Place()
    meet(neighbours(place, True))
    scatter = Scatter(place, stack, part, True)
    scatter.begin()
    to = _beside(sums_s, late_rows, layers)
    own = to.pop(layers)
    loads = _fetch([*sums, *squares_refs, *(x.at[:, place.me] for x in w), *m, *v], [*to, *squares_held, *w_s, *m_s, *v_s], sem)
    for step in (scatter.step1, scatter.step3):
        _loop(2, lambda half, _: step(half))
    squares = scatter.end(own_ref)
    own[...] = own_ref[...]
    for load in loads:
        load.wait()
    for ref in squares_held:
        squares += ref[...]
    x, y = place.at

    def share(n, squares):
        others = jnp.where(n == 0, 1, SIDE - 1)
        squares_s[n] = squares

        def to(by):
            chip = jnp.where(n == 1, near(x, by), x) * SIDE + jnp.where(n == 2, near(y, by), y)
            device = jnp.where(n == 0, place.partner, chip * CORES + place.core)
            return send(squares_s.at[n], squares_r.at[n, by], (square_sems.at[0, n, by], square_sems.at[1, n, by]), device)

        lax.fori_loop(1, others + 1, lambda by, _: to(by).start(), None)

        def arrive(by, total):
            to(by).wait()
            return total + squares_r[n, by]

        return lax.fori_loop(1, others + 1, arrive, squares)

    squares = lax.fori_loop(0, 3, share, squares)
    factor = jnp.minimum(1.0, 0.5 * lax.rsqrt(jnp.sum(squares) / count + 1e-30))
    factor_ref[...] = jnp.full(factor_ref.shape, factor, WIDE)

    def new(layer, _):
        for name, row, lane, size, column, columns in found:
            n, here, at = NAMES.index(name), (layer, ALL, pl.ds(column, columns)), (pl.ds(row, size), pl.ds(lane, columns))
            all_ref[(layer, place.chip, place.core, *at)] = adamw(w_s[n][here].astype(WIDE), m_s[n][here], v_s[n][here], sums_s[(layer, *at)].astype(WIDE) * factor)[0]

    _loop(layers, new)
    Gather(place, all_ref, streams).run()


def _outputs_kernel(shapes, layers, *refs):
    many = len(NAMES)
    sums, (own_ref, factor_ref, all_ref), m, v, new_w, new_m, new_v, (sums_s,), m_s, v_s, (sem, out_sem) = _split(
        refs, 2 * layers - 1, 3, many, many, many, many, many, 1, many, many)
    found, late_rows, _ = pieces(shapes)
    to = _beside(sums_s, late_rows, layers)
    to.pop(layers)[...] = own_ref[...]
    loads = _fetch([*sums, *m, *v], [*to, *m_s, *v_s], sem)
    every = ALL
    copies = []
    for name, row, lane, size, column, columns in found:
        copies.append(pltpu.make_async_copy(all_ref.at[:, :, :, pl.ds(row, size), pl.ds(lane, columns)],
                                            new_w[NAMES.index(name)].at[:, :, :, :, pl.ds(column, columns)], out_sem))
        copies[-1].start()
    for load in loads:
        load.wait()
    factor = factor_ref[0:1, 0:1]

    def new(layer, _):
        for name, row, lane, size, column, columns in found:
            n, here = NAMES.index(name), (layer, every, pl.ds(column, columns))
            g = sums_s[layer, pl.ds(row, size), pl.ds(lane, columns)].astype(WIDE) * factor
            _, new_m[n][here], new_v[n][here] = adamw(g, m_s[n][here], v_s[n][here], g)

    _loop(layers, new)
    for copy in copies:
        copy.wait()


def finished(late, early, stack, squares, weights, m, v):
    layers = weights[0].shape[0]
    shapes = {name: w.shape[1:] for name, w in zip(NAMES, weights)}
    _, late_rows, rows = pieces(shapes)
    width = shapes["w_down"][1]
    blocks = [(layers, shapes[name][0] // DEVICES, shapes[name][1]) for name in NAMES]
    whole = pl.BlockSpec(memory_space=pltpu.VMEM)
    mine = rows - late_rows
    held = lambda arrays: [pltpu.VMEM(a.shape, a.dtype) for a in arrays]
    given = [*late, *early[1:], *squares]
    moments = [*m, *v]
    sums_s = pltpu.VMEM((layers, rows, width), LOW)
    every, own, factor = pl.pallas_call(
        functools.partial(_finish_kernel, shapes, layers, sum(w.size for w in weights)),
        out_shape=[pltpu.VMEM((layers, SIDE * SIDE, CORES, rows, width), LOW), jax.ShapeDtypeStruct((mine, width), LOW), jax.ShapeDtypeStruct((EIGHT, HEAD), WIDE)],
        in_specs=[ANY] * (len(given) + 1 + len(weights) + len(moments)),
        out_specs=[whole] * 3,
        scratch_shapes=[sums_s] + held(squares) + [pltpu.VMEM(b, LOW) for b in blocks] + held(moments)
        + [pltpu.SemaphoreType.DMA((len(given) + len(weights) + len(moments),))] + Scatter.scratch(mine, width)
        + [pltpu.VMEM((3, EIGHT, HEAD), WIDE), pltpu.VMEM((3, SIDE, EIGHT, HEAD), WIDE), pltpu.SemaphoreType.DMA((2, 3, SIDE))] + Gather.scratch(),
        compiler_params=pltpu.CompilerParams(collective_id=layers, has_side_effects=True, vmem_limit_bytes=VMEM // 2),
        name="finish",
    )(*(far(x) for x in (*given, stack, *(w.reshape(layers, DEVICES, *b[1:]) for w, b in zip(weights, blocks)), *moments)))
    given = [*late, *early[1:]]
    out = pl.pallas_call(
        functools.partial(_outputs_kernel, shapes, layers),
        out_shape=[jax.ShapeDtypeStruct((layers, SIDE * SIDE, CORES, *b[1:]), LOW) for b in blocks] + [jax.ShapeDtypeStruct(b, WIDE) for b in blocks * 2],
        in_specs=[ANY] * len(given) + [whole] * 3 + [ANY] * len(moments),
        out_specs=[ANY] * len(blocks) + [whole] * len(moments),
        scratch_shapes=[sums_s] + held(moments) + [pltpu.SemaphoreType.DMA((len(given) + len(moments),)), pltpu.SemaphoreType.DMA],
        compiler_params=pltpu.CompilerParams(vmem_limit_bytes=VMEM // 6),
        name="outputs",
    )(*(far(x) for x in given), own, factor, pltpu.with_memory_space_constraint(every, pltpu.VMEM), *(far(x) for x in moments))
    return (*(o.reshape(layers, *shapes[name]) for name, o in zip(NAMES, out[:7])), *out[7:])


def solution(mesh):

    def step(x, dy, *arrays):
        weights, m, v, _ = _split(arrays, *[len(NAMES)] * 3)
        return finished(*gradients(x[0], dy[0], dict(zip(NAMES, weights))), weights, m, v)

    states, all_of, cut_rows, many = P(("rep", "dp")), P(), P(None, "dp"), len(NAMES)
    return jax.shard_map(
        step,
        mesh=mesh,
        in_specs=(states, states) + (all_of,) * many + (cut_rows,) * 2 * many,
        out_specs=(P("rep"),) * many + (P("rep", "dp"),) * 2 * many,
        check_vma=False,
    )
```

```python
import functools

import jax
import jax.numpy as jnp
import numpy as np
from jax import lax
from jax.experimental import pallas as pl
from jax.experimental.pallas import tpu as pltpu
from jax.sharding import PartitionSpec as P

NAMES = ("wq", "wk", "wv", "wo", "w_gate", "w_up", "w_down")
HEAD = 128
THETA = 10000
NEG = -1e30
HIDDEN = 2 * NEG
LOG2E = 1.4426950408889634
VMEM = 60 * 2**20
TILE = 512
HALF = TILE // 2
HALVES = (slice(0, HALF), slice(HALF, TILE))
SHORT = 64
AHEAD = 3
EIGHT = 8
PARTS = 3
SCALE = HEAD**-0.5
LOW, WIDE = jnp.bfloat16, jnp.float32
ANY = pl.BlockSpec(memory_space=pl.ANY)
ALL = slice(None)

SIDE, CORES = 4, 2
DEVICES = SIDE * SIDE * CORES
STREAMS = 4
WHERE = pl.DeviceIdType.MESH
LATE, EARLY = ("w_gate", "w_up", "w_down", "wo"), ("wq", "wk", "wv")


def pieces(shapes):
    width, row, found = shapes["w_down"][1], 0, []
    for name in LATE:
        rows, cols = shapes[name][0] // DEVICES, shapes[name][1]
        for column in range(0, cols, width):
            found.append((name, row, 0, rows, column, width))
            row += rows
    late, lane = row, 0
    for name in EARLY:
        rows, cols = shapes[name][0] // DEVICES, shapes[name][1]
        for column in range(0, cols, HEAD):
            found.append((name, row, lane, rows, column, HEAD))
            lane = (lane + HEAD) % width
            row += rows if lane == 0 else 0
    return found, late, row


def shapes_of(w):
    return {name: x.shape[1:] for name, x in w.items()}


def _dot(a, b, ca=1, cb=0):
    return lax.dot_general(a, b, (((ca,), (cb,)), ((), ())), preferred_element_type=WIDE)


def _dot_t(a, b):
    return _dot(a, b, 1, 1)


def _loop(count, body):
    lax.fori_loop(0, count, body, None)


def _at(first, size):
    return pl.ds(pl.multiple_of(first, size), size)


def _part(n, size=HEAD):
    return slice(n * size, n * size + size)


def _step():
    return pl.program_id(0)


def _last():
    return _step() == pl.num_programs(0) - 1


def _seen(shape, queries, ahead=0):
    place = [lax.broadcasted_iota(jnp.int32, shape, axis) for axis in (queries, 1 - queries)]
    return place[0] + ahead >= place[1]


def _split(refs, *counts):
    groups = []
    for count in counts:
        groups.append(refs[:count])
        refs = refs[count:]
    return *groups, refs


def far(x):
    return pltpu.with_memory_space_constraint(x, pltpu.HBM)


def _call(kernel, grid, ins, outs, scratch, name, args, flops, **params):
    moved = sum(a.size * a.dtype.itemsize for a in (*args, *(o[0] for o in outs)))
    return pl.pallas_call(
        kernel,
        grid=grid,
        in_specs=ins,
        out_specs=[o[1] for o in outs],
        out_shape=[o[0] for o in outs],
        scratch_shapes=scratch,
        compiler_params=pltpu.CompilerParams(dimension_semantics=("arbitrary",), vmem_limit_bytes=VMEM, **params),
        cost_estimate=pl.CostEstimate(flops=flops, transcendentals=0, bytes_accessed=moved),
        name=name,
    )(*args)


def _rows(cols):
    return pl.BlockSpec((TILE, cols), lambda i: (i, 0))


def _heads(n):
    return pl.BlockSpec((n, TILE, HEAD), lambda i: (0, i, 0))


def _whole(*shape):
    return pl.BlockSpec(shape, lambda i: (0,) * len(shape))


def _of_layer(w, number):
    return pl.BlockSpec((1, *w.shape[1:]), lambda i: (number, 0, 0))


def _out(shape, dtype, spec):
    return jax.ShapeDtypeStruct(shape, dtype), spec


def _scale(h):
    return lax.rsqrt(jnp.mean(h * h, -1, keepdims=True) + 1e-6)


def _turn(t, cos, sin):
    t = t.astype(WIDE)
    return (t * cos + pltpu.roll(t, HEAD // 2, 1) * sin).astype(LOW)


def turns(tokens):
    half = HEAD // 2
    places = np.concatenate([np.arange(SHORT), np.arange(0, tokens, SHORT)])
    angle = places[:, None] * float(THETA) ** (-np.arange(half) / half)
    return jnp.asarray(np.concatenate([np.cos(angle), np.sin(angle)], 1), WIDE)


def _both(t):
    r = pltpu.roll(t, HEAD // 2, 1)
    first = lax.broadcasted_iota(jnp.int32, t.shape, 1) < HEAD // 2
    return jnp.where(first, t, r), jnp.where(first, -r, t)


def _turns(table_ref):
    cos, sin = _both(table_ref[:SHORT, :])
    many = TILE // SHORT
    far = _both(table_ref[pl.ds(pl.multiple_of(SHORT + _step() * many, many), many), :])
    coses, sines = [], []
    for n in range(many):
        far_cos, far_sin = (t[n : n + 1, :] for t in far)
        coses.append(far_cos * cos - far_sin * sin)
        sines.append(far_sin * cos + far_cos * sin)
    return jnp.concatenate(coses, 0), jnp.concatenate(sines, 0)


def _project(h, wq_ref, wk_ref, wv_ref, table_ref, q_ref, k_ref, v_ref):
    cos, sin = _turns(table_ref)
    for here in HALVES:
        a = (h[here] * _scale(h[here])).astype(LOW)
        q = _dot(a, wq_ref[0]).astype(LOW)
        for n in range(q_ref.shape[0]):
            q_ref[n, here, :] = _turn(q[:, _part(n)], cos[here], sin[here])
        k_ref[here, :] = _turn(_dot(a, wk_ref[0]).astype(LOW), cos[here], sin[here])
        v_ref[here, :] = _dot(a, wv_ref[0]).astype(LOW)


def _first_kernel(h_ref, *refs):
    _project(h_ref[...].astype(WIDE), *refs)


def _qkv_outs(tokens, heads):
    return [_out((heads, tokens, HEAD), LOW, _heads(heads))] + [_out((tokens, HEAD), LOW, _rows(HEAD))] * 2


def first(h, w, number, table):
    tokens, d = h.shape
    args = [h, w["wq"], w["wk"], w["wv"], table]
    cols = w["wq"].shape[2]
    return _call(_first_kernel, (tokens // TILE,), [_rows(d)] + [_of_layer(x, number) for x in args[1:4]] + [_whole(*table.shape)],
                 _qkv_outs(tokens, cols // HEAD), [], "first", args, 2 * tokens * d * (cols + 2 * HEAD))


def _attend_kernel(q_ref, k_ref, v_ref, o_ref, turned_ref, qt_ref, lse_ref, top_s, mix_s):
    heads = q_ref.shape[0]
    block_q = _step()
    e = SCALE * LOG2E
    top_s[...] = jnp.full(top_s.shape, NEG, WIDE)
    mix_s[...] = jnp.zeros(mix_s.shape, WIDE)
    def block(first_half, halves, low, masked):
        size = halves * HALF
        here = _at(first_half * HALF, size)
        k, values = k_ref[here, :], jnp.concatenate([v_ref[here, :].T, jnp.ones((EIGHT, size), LOW)])
        if masked:
            ok = _seen((size, TILE - low), 1)
        score = lambda n: _dot_t(k, q_ref[n, low:, :])
        ready = [score(n) for n in range(AHEAD)]
        for n in range(heads):
            if n + AHEAD < heads:
                ready.append(score(n + AHEAD))
            s = jnp.where(ok, ready[n], HIDDEN) if masked else ready[n]
            row = slice(n, n + 1)
            old = top_s[row, low:]
            top = jnp.maximum(old, s.max(0, keepdims=True))
            top_s[row, low:] = top
            mix_s[n, :, low:] = mix_s[n, :, low:] * jnp.exp2((old - top) * e) + _dot(values, jnp.exp2((s - top) * e).astype(LOW))

    _loop(block_q, lambda j, _: block(2 * j, 2, 0, False))
    block(2 * block_q, 1, 0, True)
    block(2 * block_q + 1, 1, HALF, True)
    for n in range(heads):
        total, row = mix_s[n, HEAD : HEAD + 1, :], slice(n, n + 1)
        turned = (mix_s[n, :HEAD, :] * (1 / total)).astype(LOW)
        turned_ref[_part(n), :] = turned
        o_ref[:, _part(n)] = turned.T
        qt_ref[n] = q_ref[n].T
        lse_ref[row, :] = top_s[row, :] * SCALE + jnp.log(total)
    lse_ref[heads:, :] = jnp.zeros((EIGHT - heads, TILE), WIDE)


def _columns(rows):
    return pl.BlockSpec((rows, TILE), lambda i: (0, i))


def _head_columns(heads):
    return pl.BlockSpec((heads, HEAD, TILE), lambda i: (0, 0, i))


def attend(q, k, v):
    heads, tokens, _ = q.shape
    inner = heads * HEAD
    return _call(_attend_kernel, (tokens // TILE,), [_heads(heads), _whole(tokens, HEAD), _whole(tokens, HEAD)],
                 [_out((tokens, inner), LOW, _rows(inner)), _out((inner, tokens), LOW, _columns(inner)),
                  _out((heads, HEAD, tokens), LOW, _head_columns(heads)), _out((EIGHT, tokens), WIDE, _columns(EIGHT))],
                 [pltpu.VMEM((heads, TILE), WIDE), pltpu.VMEM((heads, HEAD + EIGHT, TILE), WIDE)],
                 "attend", [q, k, v], 2 * heads * tokens * tokens * HEAD)


def _attend_back_kernel(many, refs):
    ins, stacks, (dq_ref, dk_ref, dv_ref), sums, (squares_ref,), held, refs = _split(refs, 8, many, 3, many, 1, 5)
    q_ref, qt_ref, k_ref, v_ref, do_ref, dot_ref, lse_ref, delta_ref = ins
    dq_s, dk_s, dv_s, beside_s, take_s = held
    heads = q_ref.shape[0]
    block_q = _step()
    steps = k_ref.shape[0] // TILE
    e = SCALE * LOG2E
    place = Place()
    parts = [Scatter(place, s, refs[_part(at, 9)]) for at, s in enumerate(stacks)]

    def travel(step, tick, *ticks):
        one, other = (n * steps * steps // 16 for n in ticks)

        if parts:
            @pl.when((tick == one) | (tick == other))
            def _():
                for part in parts:
                    getattr(part, step)(jnp.where(tick == other, 1, 0))

    @pl.when(block_q == 0)
    def _():
        for part in parts:
            part.load()
        if parts:
            meet(neighbours(place))
        for part in parts:
            part.begin()
        lane = lax.broadcasted_iota(jnp.int32, (HALF, HEAD), 1)

        def clear(n, _):
            dk_s[n] = jnp.zeros((HEAD, HALF), WIDE)
            dv_s[n] = jnp.zeros((HEAD, HALF), WIDE)

        def take(n, _):
            for which in range(2):
                mine = (lane % EIGHT == n) & (lane // (EIGHT * PARTS) == which)
                take_s[which, n] = jnp.where(mine, -1.0, 0.0).astype(LOW)

        _loop(2 * steps, clear)
        _loop(heads, take)

    dq_s[...] = jnp.zeros_like(dq_s)
    of = lambda n: (ALL, _part(n))
    lines = []
    for rest in (lse_ref[...] * (1 / SCALE), delta_ref[...]):
        for _ in range(PARTS):
            lines.append(rest.astype(LOW).astype(WIDE))
            rest = rest - lines[-1]
    lines.append(jnp.zeros((HEAD - EIGHT * len(lines), TILE), WIDE))
    beside_s[...] = jnp.concatenate(lines).T.astype(LOW)

    def block(keys, low):
        here = _at(keys * HALF, HALF)
        k, v = k_ref[here, :], v_ref[here, :]
        ok = _seen((TILE - low, HALF), 0, (2 * block_q - keys) * HALF + low)
        beside = lambda x: jnp.concatenate([x, beside_s[low:, :]], 1)
        score = lambda n: (_dot_t(beside(q_ref[n, low:, :]), jnp.concatenate([k, take_s[0, n]], 1)),
                           _dot_t(beside(do_ref[low:, _part(n)]), jnp.concatenate([v, take_s[1, n]], 1)))
        s, dp = score(0)
        dk, dv = None, None
        for n in range(heads):
            after = score(n + 1) if n + 1 < heads else (None, None)
            p = jnp.where(ok, jnp.exp2(s * e), 0.0)
            ds = (p * dp).astype(LOW)
            more_v, more_k = _dot(dot_ref[_part(n), low:], p.astype(LOW)), _dot(qt_ref[n, :, low:], ds)
            dv, dk = (dv + more_v, dk + more_k) if n else (more_v, more_k)
            dq_s[n, low:, :] += _dot(ds, k)
            s, dp = after
        dk_s[keys] += dk
        dv_s[keys] += dv

    def one(j, _):
        tick = block_q * block_q + j
        travel("step1", tick, 3, 4)
        travel("step2", tick, 7, 9)
        travel("step3", tick, 11, 13)
        travel("step4", tick, 14, 15)
        block(j, 0)

    _loop(2 * block_q + 1, one)
    block(2 * block_q + 1, HALF)
    for n in range(heads):
        dq_ref[of(n)] = (dq_s[n] * SCALE).astype(LOW)

    @pl.when(block_q == steps - 1)
    def _():
        def turn(n, _):
            here = _at(n * HALF, HALF)
            dk_ref[here, :] = (dk_s[n] * SCALE).T.astype(LOW)
            dv_ref[here, :] = dv_s[n].T.astype(LOW)

        _loop(2 * steps, turn)
        squares_ref[...] = sum((part.end(out) for part, out in zip(parts, sums)), jnp.zeros((EIGHT, HEAD), WIDE))
        for part in parts:
            part.sent()


def attend_back(q, qt, k, v, do, dot, lse, delta, stacks, number):
    heads, tokens, _ = q.shape
    wide, kv = _rows(heads * HEAD), _whole(tokens, HEAD)
    rows = [s.shape[2] for s in stacks]
    width = stacks[0].shape[3] if stacks else HEAD
    scratch = [pltpu.VMEM((heads, TILE, HEAD), WIDE)] + [pltpu.VMEM((tokens // HALF, HEAD, HALF), WIDE)] * 2
    scratch += [pltpu.VMEM((TILE, HEAD), LOW), pltpu.VMEM((2, heads, HALF, HEAD), LOW)]
    got = _call(lambda *refs: _attend_back_kernel(len(rows), refs), (tokens // TILE,),
                [_heads(heads), _head_columns(heads), kv, kv, wide, _columns(heads * HEAD)] + [_columns(EIGHT)] * 2 + [ANY] * len(rows),
                [_out((tokens, heads * HEAD), LOW, wide)] + [_out((tokens, HEAD), LOW, kv)] * 2
                + [_out((n, width), LOW, _whole(n, width)) for n in rows] + [_out((EIGHT, HEAD), WIDE, _whole(EIGHT, HEAD))],
                scratch + [s for n in rows for s in Scatter.scratch(n, width)],
                "attend_back", [q, qt, k, v, do, dot, lse, delta, *(far(s) for s in stacks)], 5 * heads * tokens * tokens * HEAD, collective_id=number, has_side_effects=True)
    return got[:3], got[3:-1], got[-1]


class Chunks:
    @staticmethod
    def scratch(d, hidden):
        n = hidden // TILE
        return [pltpu.VMEM((n, d, TILE), LOW)] * 2 + [pltpu.VMEM((n, TILE, d), LOW), pltpu.SemaphoreType.DMA((n, 3))]

    def __init__(self, number, refs, held):
        self.number, self.refs, self.held, self.sem = number, refs, held[:3], held[3]
        self.count = held[0].shape[0]

    def copies(self, c):
        units = _at(c * TILE, TILE)
        return [pltpu.make_async_copy(ref.at[at], held.at[c], self.sem.at[c, n]) for n, (ref, held, at) in enumerate(
            zip(self.refs, self.held, ((self.number, ALL, units), (self.number, ALL, units), (self.number, units, ALL))))]

    def fetch(self):
        @pl.when(_step() == 0)
        def _():
            for c in range(self.count):
                for copy in self.copies(c):
                    copy.start()

    def chunk(self, c):
        @pl.when(_step() == 0)
        def _():
            for copy in self.copies(c):
                copy.wait()

        return [held[c] for held in self.held]


def _slot(n):
    return lax.rem(n, 2)


class Passing:
    @staticmethod
    def scratch(many):
        return [pltpu.VMEM((2, TILE, TILE), WIDE)] * many + [pltpu.SemaphoreType.DMA((2, many))]

    def __init__(self, refs, held, out):
        self.refs, self.held, self.sem, self.out = refs, held[:-1], held[-1], out
        self.count = refs[0].shape[0]
        self.first, self.total = _step() * self.count, pl.num_programs(0) * self.count

    def _each(self, n):
        slot, chunk, rows = _slot(n), lax.rem(n, self.count), _at(lax.div(n, self.count) * TILE, TILE)
        for at, (ref, held) in enumerate(zip(self.refs, self.held)):
            ends = (held.at[slot], ref.at[chunk, rows, :])
            yield pltpu.make_async_copy(*(ends if self.out else ends[::-1]), self.sem.at[slot, at])

    def start(self, n):
        for copy in self._each(n):
            copy.start()

    def wait(self, n):
        for copy in self._each(n):
            copy.wait()


def _after_attention(o_ref, h_ref, wo_ref):
    return (h_ref[...].astype(WIDE) + _dot(o_ref[...], wo_ref[0]).astype(LOW).astype(WIDE)).astype(LOW)


def _middle_kernel(number, o_ref, h_ref, wo_ref, wg_ref, wu_ref, wd_ref, wq_ref, wk_ref, wv_ref, table_ref, mid_ref, next_ref, q_ref, k_ref, v_ref,
                   gate_ref, up_ref, b_s, total_s, *held):
    held, passed = _split(held, 4)
    chunks, passing = Chunks(number, (wg_ref, wu_ref, wd_ref), held), Passing((gate_ref, up_ref), passed, True)
    chunks.fetch()
    mid_ref[...] = _after_attention(o_ref, h_ref, wo_ref)
    mid = mid_ref[...].astype(WIDE)
    b_s[...] = (mid * _scale(mid)).astype(LOW)
    total_s[...] = jnp.zeros_like(total_s)

    def one(c, _):
        wg, wu, wd = chunks.chunk(c)
        n = passing.first + c
        pl.when(n > 1)(lambda: passing.wait(n - 2))
        gate, up = _dot(b_s[...], wg), _dot(b_s[...], wu)
        for slots, value in zip(passing.held, (gate, up)):
            slots[_slot(n)] = value
        total_s[...] += _dot((gate * jax.nn.sigmoid(gate) * up).astype(LOW), wd)
        passing.start(n)

    def two(c, _):
        one(2 * c, _)
        one(2 * c + 1, _)

    _loop(chunks.count // 2, two)
    after = (mid_ref[...].astype(WIDE) + total_s[...].astype(LOW).astype(WIDE)).astype(LOW)
    next_ref[...] = after
    _project(after.astype(WIDE), wq_ref, wk_ref, wv_ref, table_ref, q_ref, k_ref, v_ref)
    for left in (2, 1):
        pl.when(_last())(lambda: passing.wait(passing.first + chunks.count - left))


def middle(o, h, w, number, table):
    tokens, d = h.shape
    args = [o, h, w["wo"], *(far(w[n]) for n in ("w_gate", "w_up", "w_down")), *(w[n] for n in EARLY), table]
    specs = [_rows(o.shape[1]), _rows(d), _of_layer(w["wo"], number)] + [ANY] * 3
    specs += [_of_layer(w[n], number + 1) for n in ("wq", "wk", "wv")] + [_whole(*table.shape)]
    size = sum(x.size for x in w.values()) // w["wq"].shape[0]
    hidden = w["w_gate"].shape[2]
    return _call(functools.partial(_middle_kernel, number), (tokens // TILE,), specs,
                 [_out((tokens, d), LOW, _rows(d))] * 2 + _qkv_outs(tokens, o.shape[1] // HEAD) + [_out((hidden // TILE, tokens, TILE), WIDE, ANY)] * 2,
                 [pltpu.VMEM((TILE, d), LOW), pltpu.VMEM((TILE, d), WIDE)] + Chunks.scratch(d, hidden) + Passing.scratch(2),
                 "middle", args, 2 * tokens * size)


def _back_kernel(number, last, found, dy_ref, o_ref, turned_ref, h_ref, wo_ref, wg_ref, wu_ref, wd_ref, gate_ref, up_ref, dh_ref, do_ref, dot_ref, delta_ref, stack_ref,
                 mid_s, b_s, bt_s, dyt_s, db_s, wo_s, gate_s, up_s, down_s, out_s, out_sem, *held):
    first = _step() == 0
    held, passed = _split(held, 4)
    chunks, passing = Chunks(number, (wg_ref, wu_ref, wd_ref), held), None
    if not last:
        passing = Passing((gate_ref, up_ref), passed, False)
        pl.when(first)(lambda: passing.start(0))
    chunks.fetch()
    mid_s[...] = (_after_attention(o_ref, h_ref, wo_ref) if last else h_ref[...]).astype(WIDE)
    scale = _scale(mid_s[...])
    b = (mid_s[...] * scale).astype(LOW)
    b_s[...] = b
    bt_s[...] = b.T
    dyt_s[...] = dy_ref[...].T
    db_s[...] = jnp.zeros_like(db_s)

    def add(ref, at, more):
        ref[at] = jnp.where(first, 0.0, ref[at]) + more

    def one(c, _):
        wg, wu, wd = chunks.chunk(c)
        if last:
            gate, up = _dot(b_s[...], wg), _dot(b_s[...], wu)
        else:
            n = passing.first + c
            pl.when(n < passing.total - 1)(lambda: passing.start(n + 1))
            passing.wait(n)
            gate, up = (slots[_slot(n)] for slots in passing.held)
        dact = _dot_t(dy_ref[...], wd).astype(LOW).astype(WIDE)
        some = jax.nn.sigmoid(gate)
        silu = gate * some
        act = (silu * up).astype(LOW)
        dup = (dact * silu).astype(LOW)
        dgate = (dact * up * (some + silu * (1 - some))).astype(LOW)
        add(down_s, c, _dot(dyt_s[...], act))
        add(gate_s, c, _dot(bt_s[...], dgate))
        add(up_s, c, _dot(bt_s[...], dup))
        db_s[...] += _dot_t(dgate, wg) + _dot_t(dup, wu)

    _loop(chunks.count, one)
    dh = _norm_back(dy_ref[...].astype(WIDE), mid_s[...], scale, db_s[...])
    dh_ref[...] = dh
    do_ref[...] = _dot_t(dh, wo_ref[0]).astype(LOW)
    add(wo_s, ALL, _dot(turned_ref[...], dh))
    dot_ref[...] = do_ref[...].T
    heads = dot_ref.shape[0] // HEAD
    for n in range(heads):
        delta_ref[n : n + 1, :] = (dot_ref[_part(n), :].astype(WIDE) * turned_ref[_part(n), :].astype(WIDE)).sum(0, keepdims=True)
    delta_ref[heads:, :] = jnp.zeros((EIGHT - heads, TILE), WIDE)

    @pl.when(_last())
    def _():
        row = {name: (at, rows) for name, at, _, rows, column, _ in found if not column}
        every = ALL
        many = TILE // row["w_down"][1]

        def copies(c):
            for name in ("w_gate", "w_up", "w_down"):
                at, rows = row[name]
                here = (_at(c * many, many), pl.ds(at, rows)) if name == "w_down" else (every, pl.ds(pl.multiple_of(at + c * rows, EIGHT), rows))
                yield here, pltpu.make_async_copy(out_s.at[here], stack_ref.at[here], out_sem.at[c])

        def put(c, _):
            for (here, copy), value in zip(copies(c), (gate_s[c], up_s[c], down_s[c].T)):
                out_s[here] = value.reshape(-1, here[1].size, value.shape[1]).astype(LOW)
                copy.start()

        _loop(chunks.count, put)
        at, rows = row["wo"]
        here = (every, pl.ds(at, rows))
        out_s[here] = wo_s[...].reshape(DEVICES, rows, wo_s.shape[1]).astype(LOW)
        copy = pltpu.make_async_copy(out_s.at[here], stack_ref.at[here], out_sem.at[chunks.count])
        copy.start()
        for c in range(chunks.count):
            for _, some in copies(c):
                some.wait()
        copy.wait()


def _norm_back(dy, h, scale, db):
    return (dy + scale * (db - h * (scale * scale * jnp.mean(db * h, -1, keepdims=True)))).astype(LOW)


def back(dy, o, turned, h, gates, w, number, last):
    tokens, d = dy.shape
    args = [dy, o if last else far(o), turned, h, w["wo"], *(far(w[n]) for n in ("w_gate", "w_up", "w_down")), *gates]
    inner, hidden = o.shape[1], w["w_gate"].shape[2]
    n = hidden // TILE
    found, late, _ = pieces(shapes_of(w))
    scratch = [pltpu.VMEM((TILE, d), WIDE), pltpu.VMEM((TILE, d), LOW)] + [pltpu.VMEM((d, TILE), LOW)] * 2 + [pltpu.VMEM((TILE, d), WIDE)]
    scratch += [pltpu.VMEM((inner, d), WIDE)] + [pltpu.VMEM((n, d, TILE), WIDE)] * 3 + [pltpu.VMEM((DEVICES, late, d), LOW)]
    scratch += [pltpu.SemaphoreType.DMA((n + 1,))]
    return _call(functools.partial(_back_kernel, number, last, found), (tokens // TILE,),
                 [_rows(d), _rows(inner) if last else ANY, _columns(inner), _rows(d), _of_layer(w["wo"], number)] + [ANY] * 5,
                 [_out((tokens, d), LOW, _rows(d)), _out((tokens, inner), LOW, _rows(inner)), _out((inner, tokens), LOW, _columns(inner)),
                  _out((EIGHT, tokens), WIDE, _columns(EIGHT)), _out((DEVICES, late, d), LOW, ANY)],
                 scratch + Chunks.scratch(d, hidden) + ([] if last else Passing.scratch(2)), "back", args, 6 * tokens * d * (inner + 3 * hidden))


def _start_kernel(more, found, late, *refs):
    (h_ref, dq_ref, dk_ref, dv_ref, table_ref), backs, (stack_ref,), sums = _split(refs, 5, 5 * more, 1)
    if more:
        dh_ref, wq_ref, wk_ref, wv_ref, dx_ref = backs
    cos, sin = _turns(table_ref)
    more_by = [None] * len(sums)
    for rows in HALVES:
        h = h_ref[rows, :].astype(WIDE)
        scale = _scale(h)
        a_turned = (h * scale).astype(LOW).T
        dq = jnp.concatenate([_turn(dq_ref[rows, at : at + HEAD], cos[rows], -sin[rows]) for at in range(0, dq_ref.shape[1], HEAD)], 1)
        dk, dv = _turn(dk_ref[rows, :], cos[rows], -sin[rows]), dv_ref[rows, :]
        by = [_dot(a_turned, x) for x in (dq, dk, dv)]
        more_by = [x if y is None else x + y for x, y in zip(by, more_by)]
        if more:
            da = _dot_t(dq, wq_ref[0]) + _dot_t(dk, wk_ref[0]) + _dot_t(dv, wv_ref[0])
            dx_ref[rows, :] = _norm_back(dh_ref[rows, :].astype(WIDE), h, scale, da)
    for s, by in zip(sums, more_by):
        s[...] = jnp.where(_step() == 0, 0.0, s[...]) + by

    @pl.when(_last())
    def _():
        for name, row, lane, rows, column, columns in found:
            if name in EARLY:
                value = sums[EARLY.index(name)][:, pl.ds(column, columns)]
                stack_ref[:, pl.ds(row - late, rows), pl.ds(lane, columns)] = value.reshape(DEVICES, rows, columns).astype(LOW)


def start(h, dq, dk, dv, table, dh, w, number):
    tokens, d = h.shape
    more = number > 0
    shapes = [w[n].shape[1:] for n in EARLY]
    found, late, rows = pieces(shapes_of(w))
    args = [h, dq, dk, dv, table] + ([dh, *(w[n] for n in EARLY)] if more else [])
    specs = [_rows(d), _rows(dq.shape[1])] + [_rows(HEAD)] * 2 + [_whole(*table.shape)]
    specs += [_rows(d)] + [_of_layer(w[n], number) for n in EARLY] if more else []
    stack = (DEVICES, rows - late, d)
    outs = ([_out((tokens, d), LOW, _rows(d))] if more else []) + [_out(stack, LOW, _whole(*stack))]
    got = _call(functools.partial(_start_kernel, more, found, late), (tokens // TILE,), specs, outs,
                [pltpu.VMEM(s, WIDE) for s in shapes], "start", args, 4 * tokens * sum(s[0] * s[1] for s in shapes))
    return (got[0] if more else None), got[-1]


def gradients(x, dy, w):
    layers = w["wq"].shape[0]
    table = turns(x.shape[0])
    kept, h = [], x
    q, k, v = first(x, w, 0, table)
    for number in range(layers):
        o, turned, qt, lse = attend(q, k, v)
        kept.append([h, q, k, v, o, turned, qt, lse])
        if number < layers - 1:
            mid, h, q, k, v, *gates = middle(o, h, w, number, table)
            kept[number] += [mid, gates]
        else:
            kept[number] += [h, [h, h]]
    late, early, squares, waiting = [None] * layers, [None] * layers, [], []
    by_device = lambda stack: stack.reshape(SIDE * SIDE, CORES, *stack.shape[1:])
    for number in reversed(range(layers)):
        h, q, k, v, o, turned, qt, lse, mid, gates = kept[number]
        dh, do, dot, delta, stack = back(dy, o, turned, mid, gates, w, number, number == layers - 1)
        (dq, dk, dv), sums, square = attend_back(q, qt, k, v, do, dot, lse, delta, [by_device(stack), *waiting], number)
        late[number] = sums[0]
        if waiting:
            early[number + 1] = sums[1]
        squares.append(square)
        dy, stack = start(h, dq, dk, dv, table, dh, w, number)
        waiting = [by_device(stack)]
    return late, early, waiting[0], squares


class Place:
    def __init__(self):
        self.me = lax.axis_index("dp")
        self.core, self.chip = lax.rem(self.me, CORES), lax.div(self.me, CORES)
        self.at = (lax.div(self.chip, SIDE), lax.rem(self.chip, SIDE))
        self.partner = self.me + 1 - 2 * self.core

    def along(self, axis, by):
        x, y = (lax.rem(p + SIDE + by, SIDE) if a == axis else p for a, p in enumerate(self.at))
        return (x * SIDE + y) * CORES + self.core

    def shifted(self, axis, by):
        return lax.rem(self.at[axis] + SIDE + by, SIDE)


def neighbours(place, two=False):
    found = [place.partner] + [place.along(axis, by) for axis in range(2) for by in (1, -1)]
    return found + [place.along(axis, 2) for axis in range(2)] if two else found


def meet(devices):
    barrier = pltpu.get_barrier_semaphore()
    for d in devices:
        pl.semaphore_signal(barrier, inc=1, device_id={"dp": d}, device_id_type=WHERE)
    pl.semaphore_wait(barrier, len(devices))


def send(src, dst, sems, device):
    return pltpu.make_async_remote_copy(src_ref=src, dst_ref=dst, send_sem=sems[0], recv_sem=sems[1], device_id={"dp": device}, device_id_type=WHERE)


class Streams:
    def __init__(self, place):
        self.place = place

    def of(self, s):
        axis, way = lax.rem(s, 2), 1 - 2 * lax.div(s, 2)
        x, y = self.place.at
        across, down = SIDE - (SIDE - 1) * axis, 1 + (SIDE - 1) * axis
        return x + axis * (y - x), y + axis * (x - y), way, lambda i, j: i * across + j * down

    def device(self, chip):
        return chip * CORES + self.place.core


def near(place, by):
    return lax.rem(place + SIDE + by, SIDE)


class Scatter(Streams):
    @staticmethod
    def scratch(rows, width):
        chips, n = SIDE * SIDE, STREAMS
        shapes = [(chips, rows, width)] * 2 + [(n, 3, SIDE, rows, width // n)] * 2 + [(n, 3, rows, width // n)] * 2
        return [pltpu.VMEM(s, LOW) for s in shapes] + [pltpu.SemaphoreType.DMA((3,)), pltpu.SemaphoreType.DMA((n, 6)), pltpu.SemaphoreType.DMA((2, 2))]

    def __init__(self, place, given, scratch, direct=False):
        super().__init__(place)
        self.given, self.direct = given, direct
        self.straight = tuple(range(3))[not direct :]
        self.own, self.pair, self.s1, self.r1, self.s2, self.r2, self.ssem, self.rsem, self.sem = scratch
        self.rows, self.width = self.own.shape[1:]

    def _half(self, half):
        size = self.width // 2
        return _at(half * size, size)

    def _pair(self, half):
        lanes = self._half(half)
        return send(self.given.at[:, 1 - self.place.core, :, lanes], self.pair.at[ALL, ALL, lanes], (self.ssem.at[2], self.sem.at[half, 0]), self.place.partner)

    def _load(self, half):
        lanes = self._half(half)
        return pltpu.make_async_copy(self.given.at[:, self.place.core, :, lanes], self.own.at[ALL, ALL, lanes], self.sem.at[half, 1])

    def _stream(self, s):
        a, b, way, number = self.of(s)
        lanes = _at(s * HEAD, HEAD)
        along = (way, -way, 2) if self.direct else (way, -way, way)

        def move(n):
            axis, n = divmod(n, 3)
            to = number(a, near(b, along[n])) if axis else number(near(a, along[n]), b)
            src, dst, at = (self.s2, self.r2, n + 3) if axis else (self.s1, self.r1, n)
            return send(src.at[s, n], dst.at[s, n], (self.ssem.at[axis], self.rsem.at[s, at]), self.device(to))

        def chip(i, j):
            n = number(i, j)
            return self.own[n, :, lanes].astype(WIDE) + self.pair[n, :, lanes].astype(WIDE)

        def row(j):
            terms = self.straight
            return sum((self.r1[s, n, j].astype(WIDE) for n in terms), chip(a, j))

        return a, b, way, move, lanes, chip, row

    def _each(self, half, body):
        lax.fori_loop(2 * half, 2 * half + 2, lambda s, _: body(s, *self._stream(s)), None)

    def load(self):
        _loop(2, lambda half, _: self._load(half).start())

    def begin(self):
        _loop(2, lambda half, _: self._pair(half).start())

    def step1(self, half):
        self._load(half).wait()
        self._pair(half).wait_recv()

        def body(s, a, b, way, move, lanes, chip, row):
            to = (near(a, way), near(a, -way), near(a, 2)) if self.direct else (near(a, 2), near(a, -way))

            def one(j, _):
                for n, i in enumerate(to):
                    self.s1[s, n, j] = chip(i, j).astype(LOW)

            _loop(SIDE, one)
            for n in range(len(to)):
                move(n).start()

        self._each(half, body)

    def step2(self, half):
        def body(s, a, b, way, move, lanes, chip, row):
            move(0).wait_recv()

            def one(j, _):
                self.s1[s, 2, j] = (chip(near(a, way), j) + self.r1[s, 0, j].astype(WIDE)).astype(LOW)

            _loop(SIDE, one)
            move(2).start()

        self._each(half, body)

    def step3(self, half):
        def body(s, a, b, way, move, lanes, chip, row):
            for n in self.straight:
                move(n).wait_recv()
            to = (near(b, way), near(b, -way), near(b, 2)) if self.direct else (near(b, 2), near(b, -way))
            for n, j in enumerate(to):
                self.s2[s, n] = row(j).astype(LOW)
                move(3 + n).start()

        self._each(half, body)

    def step4(self, half):
        def body(s, a, b, way, move, lanes, chip, row):
            move(3).wait_recv()
            self.s2[s, 2] = (row(near(b, way)) + self.r2[s, 0].astype(WIDE)).astype(LOW)
            move(5).start()

        self._each(half, body)

    def end(self, out):
        def body(s, squares):
            a, b, way, move, lanes, chip, row = self._stream(s)
            terms = self.straight
            for n in terms:
                move(3 + n).wait_recv()
            out[:, lanes] = sum((self.r2[s, n].astype(WIDE) for n in terms), row(b)).astype(LOW)
            wide = out[:, lanes].astype(WIDE)
            return squares + (wide * wide).reshape(self.rows // EIGHT, EIGHT, HEAD).sum(0)

        return lax.fori_loop(0, STREAMS, body, jnp.zeros((EIGHT, HEAD), WIDE))

    def sent(self):
        for n, ref in enumerate((self.s1, self.s2, self.pair)):
            send(ref, ref, (self.ssem.at[n], self.rsem.at[0, 0]), self.place.partner).wait_send()


class Gather(Streams):
    @staticmethod
    def scratch():
        return [pltpu.SemaphoreType.DMA((4,)), pltpu.SemaphoreType.DMA((STREAMS, 15))]

    def __init__(self, place, out, scratch):
        super().__init__(place)
        self.out, (self.ssem, self.rsem) = out, scratch

    def _move(self, s, group, n, chip, to):
        ref = self.out.at[:, chip, self.place.core, :, _at(s * HEAD, HEAD)]
        return send(ref, ref, (self.ssem.at[group], self.ssem.at[3] if group == 2 else self.rsem.at[s, n]), to)

    def _stream(self, s):
        a, b, way, number = self.of(s)
        place = lambda p, k: near(p, jnp.where(k == 1, -way, jnp.where(k == 2, way, jnp.where(k == 3, 2, 0))))
        on1, back1, on2, back2 = number(near(a, way), b), number(near(a, -way), b), number(a, near(b, way)), number(a, near(b, -way))
        first = lambda n: self._move(s, 0, n, number(place(a, jnp.where(n == 2, 1, 0)), b), self.device(jnp.where(n == 1, back1, on1)))
        on = lambda k: self._move(s, 1, 3 + k, number(place(a, k), b), self.device(on2))
        back = lambda k: self._move(s, 1, 7 + k, number(place(a, k), b), self.device(back2))
        over = lambda k: self._move(s, 1, 11 + k, number(place(a, k), near(b, -way)), self.device(on2))
        pair = lambda k, r: self._move(s, 2, 0, number(place(a, k), place(b, r)), self.place.partner)
        return first, on, back, over, pair

    def run(self):
        def each(body):
            _loop(STREAMS, lambda s, _: body(*self._stream(s)))

        def spread(on, back, pair, k):
            on(k).start()
            back(k).start()
            pair(k, 0).start()

        def own(first, on, back, over, pair):
            first(0).start()
            first(1).start()

        each(own)
        each(lambda first, on, back, over, pair: spread(on, back, pair, 0))

        def arrive(k, _):
            def body(first, on, back, over, pair):
                first(k - 1).wait_recv()

                @pl.when(k == 1)
                def _():
                    first(2).start()

                spread(on, back, pair, k)

            each(body)

        lax.fori_loop(1, SIDE, arrive, None)

        def rows(k, _):
            def body(first, on, back, over, pair):
                on(k).wait_recv()
                over(k).start()
                pair(k, 1).start()
                back(k).wait_recv()
                pair(k, 2).start()

            each(body)

        _loop(SIDE, rows)

        def far(k, _):
            def body(first, on, back, over, pair):
                over(k).wait_recv()
                pair(k, 3).start()

            each(body)

        _loop(SIDE, far)

        for group, chips in enumerate((SIDE - 1, SIDE * (SIDE - 1), SIDE * SIDE)):
            ref = self.out.at[:, pl.ds(0, chips), 0]
            send(ref, ref, (self.ssem.at[group], self.ssem.at[3]), self.place.partner).wait_send()
        ref = self.out.at[:, :, 1 - self.place.core]
        send(ref, ref, (self.ssem.at[0], self.ssem.at[3]), self.place.partner).wait_recv()


def adamw(w, m, v, g):
    m = 0.9 * m + 0.1 * g
    v = 0.95 * v + 0.05 * g * g
    step = m * lax.rsqrt(v + 1e-8) + 0.1 * w
    return (w - 0.02 * step).astype(LOW), m, v


def _fetch(refs, held, sem):
    copies = [pltpu.make_async_copy(ref, to, sem.at[n]) for n, (ref, to) in enumerate(zip(refs, held, strict=True))]
    for copy in copies:
        copy.start()
    return copies


def _beside(sums_s, late_rows, layers):
    parts = (pl.ds(0, late_rows), pl.ds(late_rows, sums_s.shape[1] - late_rows))
    return [sums_s.at[layer, part] for part in parts for layer in range(layers)]


def _finish_kernel(shapes, layers, count, *refs):
    many = len(NAMES)
    sums, squares_refs, (stack,), w, m, v, outs, (sums_s,), squares_held, w_s, m_s, v_s, (sem,), part, square_refs, streams = _split(
        refs, 2 * layers - 1, layers, 1, many, many, many, 3, 1, layers, many, many, many, 1, 9, 3)
    all_ref, own_ref, factor_ref = outs
    squares_s, squares_r, square_sems = square_refs
    found, late_rows, rows = pieces(shapes)
    place = Place()
    scatter = Scatter(place, stack, part, True)
    scatter.load()
    meet(neighbours(place, True))
    scatter.begin()
    to = _beside(sums_s, late_rows, layers)
    own = to.pop(layers)
    loads = _fetch([*sums, *squares_refs, *(x.at[:, place.me] for x in w), *m, *v], [*to, *squares_held, *w_s, *m_s, *v_s], sem)
    _loop(2, lambda half, _: scatter.step1(half))
    for load in loads:
        load.wait()
    _loop(2, lambda half, _: scatter.step3(half))
    squares = scatter.end(own_ref)
    own[...] = own_ref[...]
    for ref in squares_held:
        squares += ref[...]
    x, y = place.at

    def share(n, squares):
        others = jnp.where(n == 0, 1, SIDE - 1)
        squares_s[n] = squares

        def to(by):
            chip = jnp.where(n == 1, near(x, by), x) * SIDE + jnp.where(n == 2, near(y, by), y)
            device = jnp.where(n == 0, place.partner, chip * CORES + place.core)
            return send(squares_s.at[n], squares_r.at[n, by], (square_sems.at[0, n, by], square_sems.at[1, n, by]), device)

        lax.fori_loop(1, others + 1, lambda by, _: to(by).start(), None)

        def arrive(by, total):
            to(by).wait()
            return total + squares_r[n, by]

        return lax.fori_loop(1, others + 1, arrive, squares)

    squares = lax.fori_loop(0, 3, share, squares)
    factor = jnp.minimum(1.0, 0.5 * lax.rsqrt(jnp.sum(squares) / count + 1e-30))
    factor_ref[...] = jnp.full(factor_ref.shape, factor, WIDE)

    def new(layer, _):
        for name, row, lane, size, column, columns in found:
            n, here, at = NAMES.index(name), (layer, ALL, pl.ds(column, columns)), (pl.ds(row, size), pl.ds(lane, columns))
            all_ref[(layer, place.chip, place.core, *at)] = adamw(w_s[n][here].astype(WIDE), m_s[n][here], v_s[n][here], sums_s[(layer, *at)].astype(WIDE) * factor)[0]

    _loop(layers, new)
    Gather(place, all_ref, streams).run()
    scatter.sent()


def _outputs_kernel(shapes, layers, *refs):
    many = len(NAMES)
    sums, (own_ref, factor_ref, all_ref), m, v, new_w, new_m, new_v, (sums_s,), m_s, v_s, (sem, out_sem) = _split(
        refs, 2 * layers - 1, 3, many, many, many, many, many, 1, many, many)
    found, late_rows, _ = pieces(shapes)
    to = _beside(sums_s, late_rows, layers)
    to.pop(layers)[...] = own_ref[...]
    loads = _fetch([*sums, *m, *v], [*to, *m_s, *v_s], sem)
    every = ALL
    copies = []
    for name, row, lane, size, column, columns in found:
        copies.append(pltpu.make_async_copy(all_ref.at[:, :, :, pl.ds(row, size), pl.ds(lane, columns)],
                                            new_w[NAMES.index(name)].at[:, :, :, :, pl.ds(column, columns)], out_sem))
        copies[-1].start()
    for load in loads:
        load.wait()
    factor = factor_ref[0:1, 0:1]

    def new(layer, _):
        for name, row, lane, size, column, columns in found:
            n, here = NAMES.index(name), (layer, every, pl.ds(column, columns))
            g = sums_s[layer, pl.ds(row, size), pl.ds(lane, columns)].astype(WIDE) * factor
            _, new_m[n][here], new_v[n][here] = adamw(g, m_s[n][here], v_s[n][here], g)

    _loop(layers, new)
    for copy in copies:
        copy.wait()


def finished(late, early, stack, squares, weights, m, v):
    layers = weights[0].shape[0]
    shapes = {name: w.shape[1:] for name, w in zip(NAMES, weights)}
    _, late_rows, rows = pieces(shapes)
    width = shapes["w_down"][1]
    blocks = [(layers, shapes[name][0] // DEVICES, shapes[name][1]) for name in NAMES]
    whole = pl.BlockSpec(memory_space=pltpu.VMEM)
    mine = rows - late_rows
    held = lambda arrays: [pltpu.VMEM(a.shape, a.dtype) for a in arrays]
    given = [*late, *early[1:], *squares]
    moments = [*m, *v]
    sums_s = pltpu.VMEM((layers, rows, width), LOW)
    every, own, factor = pl.pallas_call(
        functools.partial(_finish_kernel, shapes, layers, sum(w.size for w in weights)),
        out_shape=[pltpu.VMEM((layers, SIDE * SIDE, CORES, rows, width), LOW), jax.ShapeDtypeStruct((mine, width), LOW), jax.ShapeDtypeStruct((EIGHT, HEAD), WIDE)],
        in_specs=[ANY] * (len(given) + 1 + len(weights) + len(moments)),
        out_specs=[whole] * 3,
        scratch_shapes=[sums_s] + held(squares) + [pltpu.VMEM(b, LOW) for b in blocks] + held(moments)
        + [pltpu.SemaphoreType.DMA((len(given) + len(weights) + len(moments),))] + Scatter.scratch(mine, width)
        + [pltpu.VMEM((3, EIGHT, HEAD), WIDE), pltpu.VMEM((3, SIDE, EIGHT, HEAD), WIDE), pltpu.SemaphoreType.DMA((2, 3, SIDE))] + Gather.scratch(),
        compiler_params=pltpu.CompilerParams(collective_id=layers, has_side_effects=True, vmem_limit_bytes=VMEM // 2),
        name="finish",
    )(*(far(x) for x in (*given, stack, *(w.reshape(layers, DEVICES, *b[1:]) for w, b in zip(weights, blocks)), *moments)))
    given = [*late, *early[1:]]
    out = pl.pallas_call(
        functools.partial(_outputs_kernel, shapes, layers),
        out_shape=[jax.ShapeDtypeStruct((layers, SIDE * SIDE, CORES, *b[1:]), LOW) for b in blocks] + [jax.ShapeDtypeStruct(b, WIDE) for b in blocks * 2],
        in_specs=[ANY] * len(given) + [whole] * 3 + [ANY] * len(moments),
        out_specs=[ANY] * len(blocks) + [whole] * len(moments),
        scratch_shapes=[sums_s] + held(moments) + [pltpu.SemaphoreType.DMA((len(given) + len(moments),)), pltpu.SemaphoreType.DMA],
        compiler_params=pltpu.CompilerParams(vmem_limit_bytes=VMEM // 6),
        name="outputs",
    )(*(far(x) for x in given), own, factor, pltpu.with_memory_space_constraint(every, pltpu.VMEM), *(far(x) for x in moments))
    return (*(o.reshape(layers, *shapes[name]) for name, o in zip(NAMES, out[:7])), *out[7:])


def solution(mesh):

    def step(x, dy, *arrays):
        weights, m, v, _ = _split(arrays, *[len(NAMES)] * 3)
        return finished(*gradients(x[0], dy[0], dict(zip(NAMES, weights))), weights, m, v)

    states, all_of, cut_rows, many = P(("rep", "dp")), P(), P(None, "dp"), len(NAMES)
    return jax.shard_map(
        step,
        mesh=mesh,
        in_specs=(states, states) + (all_of,) * many + (cut_rows,) * 2 * many,
        out_specs=(P("rep"),) * many + (P("rep", "dp"),) * 2 * many,
        check_vma=False,
    )
```

```python
import functools

import jax
import jax.numpy as jnp
import numpy as np
from jax import lax
from jax.experimental import pallas as pl
from jax.experimental.pallas import tpu as pltpu
from jax.sharding import PartitionSpec as P

NAMES = ("wq", "wk", "wv", "wo", "w_gate", "w_up", "w_down")
HEAD = 128
THETA = 10000
NEG = -1e30
HIDDEN = 2 * NEG
LOG2E = 1.4426950408889634
VMEM = 60 * 2**20
TILE = 512
HALF = TILE // 2
HALVES = (slice(0, HALF), slice(HALF, TILE))
SHORT = 64
AHEAD = 3
EIGHT = 8
PARTS = 3
SCALE = HEAD**-0.5
LOW, WIDE = jnp.bfloat16, jnp.float32
ANY = pl.BlockSpec(memory_space=pl.ANY)
ALL = slice(None)

SIDE, CORES = 4, 2
DEVICES = SIDE * SIDE * CORES
STREAMS = 4
WHERE = pl.DeviceIdType.MESH
LATE, EARLY = ("w_gate", "w_up", "w_down", "wo"), ("wq", "wk", "wv")


def pieces(shapes):
    width, row, found = shapes["w_down"][1], 0, []
    for name in LATE:
        rows, cols = shapes[name][0] // DEVICES, shapes[name][1]
        for column in range(0, cols, width):
            found.append((name, row, 0, rows, column, width))
            row += rows
    late, lane = row, 0
    for name in EARLY:
        rows, cols = shapes[name][0] // DEVICES, shapes[name][1]
        for column in range(0, cols, HEAD):
            found.append((name, row, lane, rows, column, HEAD))
            lane = (lane + HEAD) % width
            row += rows if lane == 0 else 0
    return found, late, row


def shapes_of(w):
    return {name: x.shape[1:] for name, x in w.items()}


def _dot(a, b, ca=1, cb=0):
    return lax.dot_general(a, b, (((ca,), (cb,)), ((), ())), preferred_element_type=WIDE)


def _dot_t(a, b):
    return _dot(a, b, 1, 1)


def _loop(count, body):
    lax.fori_loop(0, count, body, None)


def _at(first, size):
    return pl.ds(pl.multiple_of(first, size), size)


def _part(n, size=HEAD):
    return slice(n * size, n * size + size)


def _step():
    return pl.program_id(0)


def _last():
    return _step() == pl.num_programs(0) - 1


def _seen(shape, queries, ahead=0):
    place = [lax.broadcasted_iota(jnp.int32, shape, axis) for axis in (queries, 1 - queries)]
    return place[0] + ahead >= place[1]


def _split(refs, *counts):
    groups = []
    for count in counts:
        groups.append(refs[:count])
        refs = refs[count:]
    return *groups, refs


def far(x):
    return pltpu.with_memory_space_constraint(x, pltpu.HBM)


def _call(kernel, grid, ins, outs, scratch, name, args, flops, **params):
    moved = sum(a.size * a.dtype.itemsize for a in (*args, *(o[0] for o in outs)))
    return pl.pallas_call(
        kernel,
        grid=grid,
        in_specs=ins,
        out_specs=[o[1] for o in outs],
        out_shape=[o[0] for o in outs],
        scratch_shapes=scratch,
        compiler_params=pltpu.CompilerParams(dimension_semantics=("arbitrary",), vmem_limit_bytes=VMEM, **params),
        cost_estimate=pl.CostEstimate(flops=flops, transcendentals=0, bytes_accessed=moved),
        name=name,
    )(*args)


def _rows(cols):
    return pl.BlockSpec((TILE, cols), lambda i: (i, 0))


def _heads(n):
    return pl.BlockSpec((n, TILE, HEAD), lambda i: (0, i, 0))


def _whole(*shape):
    return pl.BlockSpec(shape, lambda i: (0,) * len(shape))


def _of_layer(w, number):
    return pl.BlockSpec((1, *w.shape[1:]), lambda i: (number, 0, 0))


def _out(shape, dtype, spec):
    return jax.ShapeDtypeStruct(shape, dtype), spec


def _scale(h):
    return lax.rsqrt(jnp.mean(h * h, -1, keepdims=True) + 1e-6)


def _turn(t, cos, sin):
    t = t.astype(WIDE)
    return (t * cos + pltpu.roll(t, HEAD // 2, 1) * sin).astype(LOW)


def turns(tokens):
    half = HEAD // 2
    places = np.concatenate([np.arange(SHORT), np.arange(0, tokens, SHORT)])
    angle = places[:, None] * float(THETA) ** (-np.arange(half) / half)
    return jnp.asarray(np.concatenate([np.cos(angle), np.sin(angle)], 1), WIDE)


def _both(t):
    r = pltpu.roll(t, HEAD // 2, 1)
    first = lax.broadcasted_iota(jnp.int32, t.shape, 1) < HEAD // 2
    return jnp.where(first, t, r), jnp.where(first, -r, t)


def _turns(table_ref, step):
    cos, sin = _both(table_ref[:SHORT, :])
    many = TILE // SHORT
    far = _both(table_ref[pl.ds(pl.multiple_of(SHORT + step * many, many), many), :])
    coses, sines = [], []
    for n in range(many):
        far_cos, far_sin = (t[n : n + 1, :] for t in far)
        coses.append(far_cos * cos - far_sin * sin)
        sines.append(far_sin * cos + far_cos * sin)
    return jnp.concatenate(coses, 0), jnp.concatenate(sines, 0)


def _project(h, wq_ref, wk_ref, wv_ref, table_ref, q_ref, k_ref, v_ref):
    cos, sin = _turns(table_ref, _step())
    for here in HALVES:
        a = (h[here] * _scale(h[here])).astype(LOW)
        q = _dot(a, wq_ref[0]).astype(LOW)
        for n in range(q_ref.shape[0]):
            q_ref[n, here, :] = _turn(q[:, _part(n)], cos[here], sin[here])
        k_ref[here, :] = _turn(_dot(a, wk_ref[0]).astype(LOW), cos[here], sin[here])
        v_ref[here, :] = _dot(a, wv_ref[0]).astype(LOW)


def _first_kernel(h_ref, *refs):
    _project(h_ref[...].astype(WIDE), *refs)


def _qkv_outs(tokens, heads):
    return [_out((heads, tokens, HEAD), LOW, _heads(heads))] + [_out((tokens, HEAD), LOW, _rows(HEAD))] * 2


def first(h, w, number, table):
    tokens, d = h.shape
    args = [h, w["wq"], w["wk"], w["wv"], table]
    cols = w["wq"].shape[2]
    return _call(_first_kernel, (tokens // TILE,), [_rows(d)] + [_of_layer(x, number) for x in args[1:4]] + [_whole(*table.shape)],
                 _qkv_outs(tokens, cols // HEAD), [], "first", args, 2 * tokens * d * (cols + 2 * HEAD))


def _attend_kernel(q_ref, k_ref, v_ref, o_ref, turned_ref, qt_ref, lse_ref, top_s, mix_s):
    heads = q_ref.shape[0]
    block_q = _step()
    e = SCALE * LOG2E
    top_s[...] = jnp.full(top_s.shape, NEG, WIDE)
    mix_s[...] = jnp.zeros(mix_s.shape, WIDE)
    def block(first_half, halves, low, masked):
        size = halves * HALF
        here = _at(first_half * HALF, size)
        k, values = k_ref[here, :], jnp.concatenate([v_ref[here, :].T, jnp.ones((EIGHT, size), LOW)])
        if masked:
            ok = _seen((size, TILE - low), 1)
        score = lambda n: _dot_t(k, q_ref[n, low:, :])
        ready = [score(n) for n in range(AHEAD)]
        for n in range(heads):
            if n + AHEAD < heads:
                ready.append(score(n + AHEAD))
            s = jnp.where(ok, ready[n], HIDDEN) if masked else ready[n]
            row = slice(n, n + 1)
            old = top_s[row, low:]
            top = jnp.maximum(old, s.max(0, keepdims=True))
            top_s[row, low:] = top
            mix_s[n, :, low:] = mix_s[n, :, low:] * jnp.exp2((old - top) * e) + _dot(values, jnp.exp2((s - top) * e).astype(LOW))

    _loop(block_q, lambda j, _: block(2 * j, 2, 0, False))
    block(2 * block_q, 1, 0, True)
    block(2 * block_q + 1, 1, HALF, True)
    for n in range(heads):
        total, row = mix_s[n, HEAD : HEAD + 1, :], slice(n, n + 1)
        turned = (mix_s[n, :HEAD, :] * (1 / total)).astype(LOW)
        turned_ref[_part(n), :] = turned
        o_ref[:, _part(n)] = turned.T
        qt_ref[n] = q_ref[n].T
        lse_ref[row, :] = top_s[row, :] * SCALE + jnp.log(total)
    lse_ref[heads:, :] = jnp.zeros((EIGHT - heads, TILE), WIDE)


def _columns(rows):
    return pl.BlockSpec((rows, TILE), lambda i: (0, i))


def _head_columns(heads):
    return pl.BlockSpec((heads, HEAD, TILE), lambda i: (0, 0, i))


def attend(q, k, v):
    heads, tokens, _ = q.shape
    inner = heads * HEAD
    return _call(_attend_kernel, (tokens // TILE,), [_heads(heads), _whole(tokens, HEAD), _whole(tokens, HEAD)],
                 [_out((tokens, inner), LOW, _rows(inner)), _out((inner, tokens), LOW, _columns(inner)),
                  _out((heads, HEAD, tokens), LOW, _head_columns(heads)), _out((EIGHT, tokens), WIDE, _columns(EIGHT))],
                 [pltpu.VMEM((heads, TILE), WIDE), pltpu.VMEM((heads, HEAD + EIGHT, TILE), WIDE)],
                 "attend", [q, k, v], 2 * heads * tokens * tokens * HEAD)


def _attend_back_kernel(many, refs):
    ins, stacks, (dq_ref, dk_ref, dv_ref), sums, (squares_ref,), held, refs = _split(refs, 8, many, 3, many, 1, 5)
    q_ref, qt_ref, k_ref, v_ref, do_ref, dot_ref, lse_ref, delta_ref = ins
    dq_s, dk_s, dv_s, beside_s, take_s = held
    heads = q_ref.shape[0]
    block_q = _step()
    steps = k_ref.shape[0] // TILE
    e = SCALE * LOG2E
    place = Place()
    parts = [Scatter(place, s, refs[_part(at, 9)]) for at, s in enumerate(stacks)]

    def travel(step, tick, *ticks):
        one, other = (n * steps * steps // 16 for n in ticks)

        if parts:
            @pl.when((tick == one) | (tick == other))
            def _():
                for part in parts:
                    getattr(part, step)(jnp.where(tick == other, 1, 0))

    @pl.when(block_q == 0)
    def _():
        for part in parts:
            part.load()
        if parts:
            meet(neighbours(place))
        for part in parts:
            part.begin()
        lane = lax.broadcasted_iota(jnp.int32, (HALF, HEAD), 1)

        def clear(n, _):
            dk_s[n] = jnp.zeros((HEAD, HALF), WIDE)
            dv_s[n] = jnp.zeros((HEAD, HALF), WIDE)

        def take(n, _):
            for which in range(2):
                mine = (lane % EIGHT == n) & (lane // (EIGHT * PARTS) == which)
                take_s[which, n] = jnp.where(mine, -1.0, 0.0).astype(LOW)

        _loop(2 * steps, clear)
        _loop(heads, take)

    dq_s[...] = jnp.zeros_like(dq_s)
    of = lambda n: (ALL, _part(n))
    lines = []
    for rest in (lse_ref[...] * (1 / SCALE), delta_ref[...]):
        for _ in range(PARTS):
            lines.append(rest.astype(LOW).astype(WIDE))
            rest = rest - lines[-1]
    lines.append(jnp.zeros((HEAD - EIGHT * len(lines), TILE), WIDE))
    beside_s[...] = jnp.concatenate(lines).T.astype(LOW)

    def block(keys, low):
        here = _at(keys * HALF, HALF)
        k, v = k_ref[here, :], v_ref[here, :]
        ok = _seen((TILE - low, HALF), 0, (2 * block_q - keys) * HALF + low)
        beside = lambda x: jnp.concatenate([x, beside_s[low:, :]], 1)
        score = lambda n: (_dot_t(beside(q_ref[n, low:, :]), jnp.concatenate([k, take_s[0, n]], 1)),
                           _dot_t(beside(do_ref[low:, _part(n)]), jnp.concatenate([v, take_s[1, n]], 1)))
        s, dp = score(0)
        dk, dv = None, None
        for n in range(heads):
            after = score(n + 1) if n + 1 < heads else (None, None)
            p = jnp.where(ok, jnp.exp2(s * e), 0.0)
            ds = (p * dp).astype(LOW)
            more_v, more_k = _dot(dot_ref[_part(n), low:], p.astype(LOW)), _dot(qt_ref[n, :, low:], ds)
            dv, dk = (dv + more_v, dk + more_k) if n else (more_v, more_k)
            dq_s[n, low:, :] += _dot(ds, k)
            s, dp = after
        dk_s[keys] += dk
        dv_s[keys] += dv

    def one(j, _):
        tick = block_q * block_q + j
        travel("step1", tick, 3, 4)
        travel("step2", tick, 7, 9)
        travel("step3", tick, 11, 13)
        travel("step4", tick, 14, 15)
        block(j, 0)

    _loop(2 * block_q + 1, one)
    block(2 * block_q + 1, HALF)
    for n in range(heads):
        dq_ref[of(n)] = (dq_s[n] * SCALE).astype(LOW)

    @pl.when(block_q == steps - 1)
    def _():
        def turn(n, _):
            here = _at(n * HALF, HALF)
            dk_ref[here, :] = (dk_s[n] * SCALE).T.astype(LOW)
            dv_ref[here, :] = dv_s[n].T.astype(LOW)

        _loop(2 * steps, turn)
        squares_ref[...] = sum((part.end(out) for part, out in zip(parts, sums)), jnp.zeros((EIGHT, HEAD), WIDE))
        for part in parts:
            part.sent()


def attend_back(q, qt, k, v, do, dot, lse, delta, stacks, number):
    heads, tokens, _ = q.shape
    wide, kv = _rows(heads * HEAD), _whole(tokens, HEAD)
    rows = [s.shape[2] for s in stacks]
    width = stacks[0].shape[3] if stacks else HEAD
    scratch = [pltpu.VMEM((heads, TILE, HEAD), WIDE)] + [pltpu.VMEM((tokens // HALF, HEAD, HALF), WIDE)] * 2
    scratch += [pltpu.VMEM((TILE, HEAD), LOW), pltpu.VMEM((2, heads, HALF, HEAD), LOW)]
    got = _call(lambda *refs: _attend_back_kernel(len(rows), refs), (tokens // TILE,),
                [_heads(heads), _head_columns(heads), kv, kv, wide, _columns(heads * HEAD)] + [_columns(EIGHT)] * 2 + [ANY] * len(rows),
                [_out((tokens, heads * HEAD), LOW, wide)] + [_out((tokens, HEAD), LOW, kv)] * 2
                + [_out((n, width), LOW, _whole(n, width)) for n in rows] + [_out((EIGHT, HEAD), WIDE, _whole(EIGHT, HEAD))],
                scratch + [s for n in rows for s in Scatter.scratch(n, width)],
                "attend_back", [q, qt, k, v, do, dot, lse, delta, *(far(s) for s in stacks)], 5 * heads * tokens * tokens * HEAD, collective_id=number, has_side_effects=True)
    return got[:3], got[3:-1], got[-1]


class Chunks:
    @staticmethod
    def scratch(d, hidden):
        n = hidden // TILE
        return [pltpu.VMEM((n, d, TILE), LOW)] * 2 + [pltpu.VMEM((n, TILE, d), LOW), pltpu.SemaphoreType.DMA((n, 3))]

    def __init__(self, number, refs, held):
        self.number, self.refs, self.held, self.sem = number, refs, held[:3], held[3]
        self.count = held[0].shape[0]

    def copies(self, c):
        units = _at(c * TILE, TILE)
        return [pltpu.make_async_copy(ref.at[at], held.at[c], self.sem.at[c, n]) for n, (ref, held, at) in enumerate(
            zip(self.refs, self.held, ((self.number, ALL, units), (self.number, ALL, units), (self.number, units, ALL))))]

    def fetch(self):
        @pl.when(_step() == 0)
        def _():
            for c in range(self.count):
                for copy in self.copies(c):
                    copy.start()

    def chunk(self, c):
        @pl.when(_step() == 0)
        def _():
            for copy in self.copies(c):
                copy.wait()

        return [held[c] for held in self.held]


def _slot(n):
    return lax.rem(n, 2)


class Passing:
    @staticmethod
    def scratch(many):
        return [pltpu.VMEM((2, TILE, TILE), WIDE)] * many + [pltpu.SemaphoreType.DMA((2, many))]

    def __init__(self, refs, held, out):
        self.refs, self.held, self.sem, self.out = refs, held[:-1], held[-1], out
        self.count = refs[0].shape[0]
        self.first, self.total = _step() * self.count, pl.num_programs(0) * self.count

    def _each(self, n):
        slot, chunk, rows = _slot(n), lax.rem(n, self.count), _at(lax.div(n, self.count) * TILE, TILE)
        for at, (ref, held) in enumerate(zip(self.refs, self.held)):
            ends = (held.at[slot], ref.at[chunk, rows, :])
            yield pltpu.make_async_copy(*(ends if self.out else ends[::-1]), self.sem.at[slot, at])

    def start(self, n):
        for copy in self._each(n):
            copy.start()

    def wait(self, n):
        for copy in self._each(n):
            copy.wait()


def _after_attention(o_ref, h_ref, wo_ref):
    return (h_ref[...].astype(WIDE) + _dot(o_ref[...], wo_ref[0]).astype(LOW).astype(WIDE)).astype(LOW)


def _middle_kernel(number, o_ref, h_ref, wo_ref, wg_ref, wu_ref, wd_ref, wq_ref, wk_ref, wv_ref, table_ref, mid_ref, next_ref, q_ref, k_ref, v_ref,
                   gate_ref, up_ref, b_s, total_s, *held):
    held, passed = _split(held, 4)
    chunks, passing = Chunks(number, (wg_ref, wu_ref, wd_ref), held), Passing((gate_ref, up_ref), passed, True)
    chunks.fetch()
    mid_ref[...] = _after_attention(o_ref, h_ref, wo_ref)
    mid = mid_ref[...].astype(WIDE)
    b_s[...] = (mid * _scale(mid)).astype(LOW)
    total_s[...] = jnp.zeros_like(total_s)

    def one(c, _):
        wg, wu, wd = chunks.chunk(c)
        n = passing.first + c
        pl.when(n > 1)(lambda: passing.wait(n - 2))
        gate, up = _dot(b_s[...], wg), _dot(b_s[...], wu)
        for slots, value in zip(passing.held, (gate, up)):
            slots[_slot(n)] = value
        total_s[...] += _dot((gate * jax.nn.sigmoid(gate) * up).astype(LOW), wd)
        passing.start(n)

    def two(c, _):
        one(2 * c, _)
        one(2 * c + 1, _)

    _loop(chunks.count // 2, two)
    after = (mid_ref[...].astype(WIDE) + total_s[...].astype(LOW).astype(WIDE)).astype(LOW)
    next_ref[...] = after
    _project(after.astype(WIDE), wq_ref, wk_ref, wv_ref, table_ref, q_ref, k_ref, v_ref)
    for left in (2, 1):
        pl.when(_last())(lambda: passing.wait(passing.first + chunks.count - left))


def middle(o, h, w, number, table):
    tokens, d = h.shape
    args = [o, h, w["wo"], *(far(w[n]) for n in ("w_gate", "w_up", "w_down")), *(w[n] for n in EARLY), table]
    specs = [_rows(o.shape[1]), _rows(d), _of_layer(w["wo"], number)] + [ANY] * 3
    specs += [_of_layer(w[n], number + 1) for n in ("wq", "wk", "wv")] + [_whole(*table.shape)]
    size = sum(x.size for x in w.values()) // w["wq"].shape[0]
    hidden = w["w_gate"].shape[2]
    return _call(functools.partial(_middle_kernel, number), (tokens // TILE,), specs,
                 [_out((tokens, d), LOW, _rows(d))] * 2 + _qkv_outs(tokens, o.shape[1] // HEAD) + [_out((hidden // TILE, tokens, TILE), WIDE, ANY)] * 2,
                 [pltpu.VMEM((TILE, d), LOW), pltpu.VMEM((TILE, d), WIDE)] + Chunks.scratch(d, hidden) + Passing.scratch(2),
                 "middle", args, 2 * tokens * size)


def _back_kernel(number, last, found, dy_ref, o_ref, turned_ref, h_ref, wo_ref, wg_ref, wu_ref, wd_ref, gate_ref, up_ref, dh_ref, do_ref, dot_ref, delta_ref, stack_ref,
                 mid_s, b_s, bt_s, dyt_s, db_s, wo_s, gate_s, up_s, down_s, out_s, out_sem, *held):
    first = _step() == 0
    held, passed = _split(held, 4)
    chunks, passing = Chunks(number, (wg_ref, wu_ref, wd_ref), held), None
    if not last:
        passing = Passing((gate_ref, up_ref), passed, False)
        pl.when(first)(lambda: passing.start(0))
    chunks.fetch()
    mid_s[...] = (_after_attention(o_ref, h_ref, wo_ref) if last else h_ref[...]).astype(WIDE)
    scale = _scale(mid_s[...])
    b = (mid_s[...] * scale).astype(LOW)
    b_s[...] = b
    bt_s[...] = b.T
    dyt_s[...] = dy_ref[...].T
    db_s[...] = jnp.zeros_like(db_s)

    def add(ref, at, more):
        ref[at] = jnp.where(first, 0.0, ref[at]) + more

    def one(c, _):
        wg, wu, wd = chunks.chunk(c)
        if last:
            gate, up = _dot(b_s[...], wg), _dot(b_s[...], wu)
        else:
            n = passing.first + c
            pl.when(n < passing.total - 1)(lambda: passing.start(n + 1))
            passing.wait(n)
            gate, up = (slots[_slot(n)] for slots in passing.held)
        dact = _dot_t(dy_ref[...], wd).astype(LOW).astype(WIDE)
        some = jax.nn.sigmoid(gate)
        silu = gate * some
        act = (silu * up).astype(LOW)
        dup = (dact * silu).astype(LOW)
        dgate = (dact * up * (some + silu * (1 - some))).astype(LOW)
        add(down_s, c, _dot(dyt_s[...], act))
        add(gate_s, c, _dot(bt_s[...], dgate))
        add(up_s, c, _dot(bt_s[...], dup))
        db_s[...] += _dot_t(dgate, wg) + _dot_t(dup, wu)

    _loop(chunks.count, one)
    dh = _norm_back(dy_ref[...].astype(WIDE), mid_s[...], scale, db_s[...])
    dh_ref[...] = dh
    do_ref[...] = _dot_t(dh, wo_ref[0]).astype(LOW)
    add(wo_s, ALL, _dot(turned_ref[...], dh))
    dot_ref[...] = do_ref[...].T
    heads = dot_ref.shape[0] // HEAD
    for n in range(heads):
        delta_ref[n : n + 1, :] = (dot_ref[_part(n), :].astype(WIDE) * turned_ref[_part(n), :].astype(WIDE)).sum(0, keepdims=True)
    delta_ref[heads:, :] = jnp.zeros((EIGHT - heads, TILE), WIDE)

    @pl.when(_last())
    def _():
        row = {name: (at, rows) for name, at, _, rows, column, _ in found if not column}
        every = ALL
        many = TILE // row["w_down"][1]

        def copies(c):
            for name in ("w_gate", "w_up", "w_down"):
                at, rows = row[name]
                here = (_at(c * many, many), pl.ds(at, rows)) if name == "w_down" else (every, pl.ds(pl.multiple_of(at + c * rows, EIGHT), rows))
                yield here, pltpu.make_async_copy(out_s.at[here], stack_ref.at[here], out_sem.at[c])

        def put(c, _):
            for (here, copy), value in zip(copies(c), (gate_s[c], up_s[c], down_s[c].T)):
                out_s[here] = value.reshape(-1, here[1].size, value.shape[1]).astype(LOW)
                copy.start()

        _loop(chunks.count, put)
        at, rows = row["wo"]
        here = (every, pl.ds(at, rows))
        out_s[here] = wo_s[...].reshape(DEVICES, rows, wo_s.shape[1]).astype(LOW)
        copy = pltpu.make_async_copy(out_s.at[here], stack_ref.at[here], out_sem.at[chunks.count])
        copy.start()
        for c in range(chunks.count):
            for _, some in copies(c):
                some.wait()
        copy.wait()


def _norm_back(dy, h, scale, db):
    return (dy + scale * (db - h * (scale * scale * jnp.mean(db * h, -1, keepdims=True)))).astype(LOW)


def back(dy, o, turned, h, gates, w, number, last):
    tokens, d = dy.shape
    args = [dy, o if last else far(o), turned, h, w["wo"], *(far(w[n]) for n in ("w_gate", "w_up", "w_down")), *gates]
    inner, hidden = o.shape[1], w["w_gate"].shape[2]
    n = hidden // TILE
    found, late, _ = pieces(shapes_of(w))
    scratch = [pltpu.VMEM((TILE, d), WIDE), pltpu.VMEM((TILE, d), LOW)] + [pltpu.VMEM((d, TILE), LOW)] * 2 + [pltpu.VMEM((TILE, d), WIDE)]
    scratch += [pltpu.VMEM((inner, d), WIDE)] + [pltpu.VMEM((n, d, TILE), WIDE)] * 3 + [pltpu.VMEM((DEVICES, late, d), LOW)]
    scratch += [pltpu.SemaphoreType.DMA((n + 1,))]
    return _call(functools.partial(_back_kernel, number, last, found), (tokens // TILE,),
                 [_rows(d), _rows(inner) if last else ANY, _columns(inner), _rows(d), _of_layer(w["wo"], number)] + [ANY] * 5,
                 [_out((tokens, d), LOW, _rows(d)), _out((tokens, inner), LOW, _rows(inner)), _out((inner, tokens), LOW, _columns(inner)),
                  _out((EIGHT, tokens), WIDE, _columns(EIGHT)), _out((DEVICES, late, d), LOW, ANY)],
                 scratch + Chunks.scratch(d, hidden) + ([] if last else Passing.scratch(2)), "back", args, 6 * tokens * d * (inner + 3 * hidden))


def _start_sums(step, at, h_ref, dq_ref, dk_ref, dv_ref, table_ref, sums, backs=None):
    cos, sin = _turns(table_ref, step)
    more_by = [None] * len(sums)
    for half in HALVES:
        rows = _at(at + half.start, HALF)
        h = h_ref[rows, :].astype(WIDE)
        scale = _scale(h)
        a_turned = (h * scale).astype(LOW).T
        dq = jnp.concatenate([_turn(dq_ref[rows, _part(n)], cos[half], -sin[half]) for n in range(dq_ref.shape[1] // HEAD)], 1)
        dk, dv = _turn(dk_ref[rows, :], cos[half], -sin[half]), dv_ref[rows, :]
        by = [_dot(a_turned, x) for x in (dq, dk, dv)]
        more_by = [x if y is None else x + y for x, y in zip(by, more_by)]
        if backs:
            dh_ref, wq_ref, wk_ref, wv_ref, dx_ref = backs
            da = _dot_t(dq, wq_ref[0]) + _dot_t(dk, wk_ref[0]) + _dot_t(dv, wv_ref[0])
            dx_ref[rows, :] = _norm_back(dh_ref[rows, :].astype(WIDE), h, scale, da)
    for s, by in zip(sums, more_by):
        s[...] = jnp.where(step == 0, 0.0, s[...]) + by


def _stack_early(stack_ref, sums, found, late):
    for name, row, lane, rows, column, columns in found:
        if name in EARLY:
            value = sums[EARLY.index(name)][:, pl.ds(column, columns)]
            stack_ref[..., pl.ds(row - late, rows), pl.ds(lane, columns)] = value.reshape(*stack_ref.shape[:-2], rows, columns).astype(LOW)


def _start_kernel(found, late, *refs):
    ins, backs, (stack_ref,), sums = _split(refs, 5, 5, 1)
    _start_sums(_step(), 0, *ins, sums, backs)
    pl.when(_last())(lambda: _stack_early(stack_ref, sums, found, late))


def start(h, dq, dk, dv, table, dh, w, number):
    tokens, d = h.shape
    found, late, rows = pieces(shapes_of(w))
    weights = [w[n] for n in EARLY]
    specs = [_rows(d), _rows(dq.shape[1])] + [_rows(HEAD)] * 2 + [_whole(*table.shape), _rows(d)] + [_of_layer(x, number) for x in weights]
    stack = (DEVICES, rows - late, d)
    return _call(functools.partial(_start_kernel, found, late), (tokens // TILE,), specs, [_out((tokens, d), LOW, _rows(d)), _out(stack, LOW, _whole(*stack))],
                 [pltpu.VMEM(x.shape[1:], WIDE) for x in weights], "start", [h, dq, dk, dv, table, dh, *weights], 4 * tokens * sum(x[0].size for x in weights))


def gradients(x, dy, w):
    layers = w["wq"].shape[0]
    table = turns(x.shape[0])
    kept, h = [], x
    q, k, v = first(x, w, 0, table)
    for number in range(layers):
        o, turned, qt, lse = attend(q, k, v)
        kept.append([h, q, k, v, o, turned, qt, lse])
        if number < layers - 1:
            mid, h, q, k, v, *gates = middle(o, h, w, number, table)
            kept[number] += [mid, gates]
        else:
            kept[number] += [h, [h, h]]
    late, early, squares, waiting = [None] * layers, [None] * layers, [], []
    by_device = lambda stack: stack.reshape(SIDE * SIDE, CORES, *stack.shape[1:])
    for number in reversed(range(layers)):
        h, q, k, v, o, turned, qt, lse, mid, gates = kept[number]
        dh, do, dot, delta, stack = back(dy, o, turned, mid, gates, w, number, number == layers - 1)
        (dq, dk, dv), sums, square = attend_back(q, qt, k, v, do, dot, lse, delta, [by_device(stack), *waiting], number)
        late[number] = sums[0]
        if waiting:
            early[number + 1] = sums[1]
        squares.append(square)
        if number:
            dy, stack = start(h, dq, dk, dv, table, dh, w, number)
            waiting = [by_device(stack)]
    return late, early, (h, dq, dk, dv, table), squares


class Place:
    def __init__(self):
        self.me = lax.axis_index("dp")
        self.core, self.chip = lax.rem(self.me, CORES), lax.div(self.me, CORES)
        self.at = (lax.div(self.chip, SIDE), lax.rem(self.chip, SIDE))
        self.partner = self.me + 1 - 2 * self.core

    def along(self, axis, by):
        x, y = (lax.rem(p + SIDE + by, SIDE) if a == axis else p for a, p in enumerate(self.at))
        return (x * SIDE + y) * CORES + self.core

    def shifted(self, axis, by):
        return lax.rem(self.at[axis] + SIDE + by, SIDE)


def neighbours(place, two=False):
    found = [place.partner] + [place.along(axis, by) for axis in range(2) for by in (1, -1)]
    return found + [place.along(axis, 2) for axis in range(2)] if two else found


def meet(devices, between=None):
    barrier = pltpu.get_barrier_semaphore()
    for d in devices:
        pl.semaphore_signal(barrier, inc=1, device_id={"dp": d}, device_id_type=WHERE)
    if between:
        between()
    pl.semaphore_wait(barrier, len(devices))


def send(src, dst, sems, device):
    return pltpu.make_async_remote_copy(src_ref=src, dst_ref=dst, send_sem=sems[0], recv_sem=sems[1], device_id={"dp": device}, device_id_type=WHERE)


class Streams:
    def __init__(self, place):
        self.place = place

    def of(self, s):
        axis, way = lax.rem(s, 2), 1 - 2 * lax.div(s, 2)
        x, y = self.place.at
        across, down = SIDE - (SIDE - 1) * axis, 1 + (SIDE - 1) * axis
        return x + axis * (y - x), y + axis * (x - y), way, lambda i, j: i * across + j * down

    def device(self, chip):
        return chip * CORES + self.place.core


def near(place, by):
    return lax.rem(place + SIDE + by, SIDE)


class Scatter(Streams):
    @staticmethod
    def scratch(rows, width):
        chips, n = SIDE * SIDE, STREAMS
        shapes = [(chips, rows, width)] * 2 + [(n, 3, SIDE, rows, width // n)] * 2 + [(n, 3, rows, width // n)] * 2
        return [pltpu.VMEM(s, LOW) for s in shapes] + [pltpu.SemaphoreType.DMA((3,)), pltpu.SemaphoreType.DMA((n, 6)), pltpu.SemaphoreType.DMA((2, 2))]

    def __init__(self, place, given, scratch, direct=False):
        super().__init__(place)
        self.given, self.direct = given, direct
        self.straight = tuple(range(3))[not direct :]
        self.own, self.pair, self.s1, self.r1, self.s2, self.r2, self.ssem, self.rsem, self.sem = scratch
        self.rows, self.width = self.pair.shape[1:]

    def _half(self, half):
        size = self.width // 2
        return _at(half * size, size)

    def _pair(self, half):
        lanes = self._half(half)
        return send(self.given.at[:, 1 - self.place.core, :, lanes], self.pair.at[ALL, ALL, lanes], (self.ssem.at[2], self.sem.at[half, 0]), self.place.partner)

    def _load(self, half):
        lanes = self._half(half)
        return pltpu.make_async_copy(self.given.at[:, self.place.core, :, lanes], self.own.at[ALL, ALL, lanes], self.sem.at[half, 1])

    def _stream(self, s):
        a, b, way, number = self.of(s)
        lanes = _at(s * HEAD, HEAD)
        along = (way, -way, 2) if self.direct else (way, -way, way)

        def move(n):
            axis, n = divmod(n, 3)
            to = number(a, near(b, along[n])) if axis else number(near(a, along[n]), b)
            src, dst, at = (self.s2, self.r2, n + 3) if axis else (self.s1, self.r1, n)
            return send(src.at[s, n], dst.at[s, n], (self.ssem.at[axis], self.rsem.at[s, at]), self.device(to))

        def chip(i, j):
            n = number(i, j)
            own = self.given[n, self.place.core, :, lanes] if self.direct else self.own[n, :, lanes]
            return own.astype(WIDE) + self.pair[n, :, lanes].astype(WIDE)

        def row(j):
            terms = self.straight
            return sum((self.r1[s, n, j].astype(WIDE) for n in terms), chip(a, j))

        return a, b, way, move, lanes, chip, row

    def _each(self, half, body):
        lax.fori_loop(2 * half, 2 * half + 2, lambda s, _: body(s, *self._stream(s)), None)

    def load(self):
        _loop(2, lambda half, _: self._load(half).start())

    def begin(self):
        _loop(2, lambda half, _: self._pair(half).start())

    def step1(self, half):
        if not self.direct:
            self._load(half).wait()
        self._pair(half).wait_recv()

        def body(s, a, b, way, move, lanes, chip, row):
            to = (near(a, way), near(a, -way), near(a, 2)) if self.direct else (near(a, 2), near(a, -way))

            def one(j, _):
                for n, i in enumerate(to):
                    self.s1[s, n, j] = chip(i, j).astype(LOW)

            _loop(SIDE, one)
            for n in range(len(to)):
                move(n).start()

        self._each(half, body)

    def step2(self, half):
        def body(s, a, b, way, move, lanes, chip, row):
            move(0).wait_recv()

            def one(j, _):
                self.s1[s, 2, j] = (chip(near(a, way), j) + self.r1[s, 0, j].astype(WIDE)).astype(LOW)

            _loop(SIDE, one)
            move(2).start()

        self._each(half, body)

    def step3(self, half):
        def body(s, a, b, way, move, lanes, chip, row):
            for n in self.straight:
                move(n).wait_recv()
            to = (near(b, way), near(b, -way), near(b, 2)) if self.direct else (near(b, 2), near(b, -way))
            for n, j in enumerate(to):
                self.s2[s, n] = row(j).astype(LOW)
                move(3 + n).start()

        self._each(half, body)

    def step4(self, half):
        def body(s, a, b, way, move, lanes, chip, row):
            move(3).wait_recv()
            self.s2[s, 2] = (row(near(b, way)) + self.r2[s, 0].astype(WIDE)).astype(LOW)
            move(5).start()

        self._each(half, body)

    def end(self, out):
        def body(s, squares):
            a, b, way, move, lanes, chip, row = self._stream(s)
            terms = self.straight
            for n in terms:
                move(3 + n).wait_recv()
            out[:, lanes] = sum((self.r2[s, n].astype(WIDE) for n in terms), row(b)).astype(LOW)
            wide = out[:, lanes].astype(WIDE)
            return squares + (wide * wide).reshape(self.rows // EIGHT, EIGHT, HEAD).sum(0)

        return lax.fori_loop(0, STREAMS, body, jnp.zeros((EIGHT, HEAD), WIDE))

    def sent(self):
        for n, ref in enumerate((self.s1, self.s2, self.pair)):
            send(ref, ref, (self.ssem.at[n], self.rsem.at[0, 0]), self.place.partner).wait_send()


class Gather(Streams):
    @staticmethod
    def scratch():
        return [pltpu.SemaphoreType.DMA((4,)), pltpu.SemaphoreType.DMA((STREAMS, 15))]

    def __init__(self, place, out, scratch):
        super().__init__(place)
        self.out, (self.ssem, self.rsem) = out, scratch

    def _move(self, s, group, n, chip, to):
        ref = self.out.at[:, chip, self.place.core, :, _at(s * HEAD, HEAD)]
        return send(ref, ref, (self.ssem.at[group], self.ssem.at[3] if group == 2 else self.rsem.at[s, n]), to)

    def _stream(self, s):
        a, b, way, number = self.of(s)
        place = lambda p, k: near(p, jnp.where(k == 1, -way, jnp.where(k == 2, way, jnp.where(k == 3, 2, 0))))
        on1, back1, on2, back2 = number(near(a, way), b), number(near(a, -way), b), number(a, near(b, way)), number(a, near(b, -way))
        first = lambda n: self._move(s, 0, n, number(place(a, jnp.where(n == 2, 1, 0)), b), self.device(jnp.where(n == 1, back1, on1)))
        on = lambda k: self._move(s, 1, 3 + k, number(place(a, k), b), self.device(on2))
        back = lambda k: self._move(s, 1, 7 + k, number(place(a, k), b), self.device(back2))
        over = lambda k: self._move(s, 1, 11 + k, number(place(a, k), near(b, -way)), self.device(on2))
        pair = lambda k, r: self._move(s, 2, 0, number(place(a, k), place(b, r)), self.place.partner)
        return first, on, back, over, pair

    def run(self):
        def each(body):
            _loop(STREAMS, lambda s, _: body(*self._stream(s)))

        def spread(on, back, pair, k):
            on(k).start()
            back(k).start()
            pair(k, 0).start()

        def own(first, on, back, over, pair):
            first(0).start()
            first(1).start()

        each(own)
        each(lambda first, on, back, over, pair: spread(on, back, pair, 0))

        def arrive(k, _):
            def body(first, on, back, over, pair):
                first(k - 1).wait_recv()

                @pl.when(k == 1)
                def _():
                    first(2).start()

                spread(on, back, pair, k)

            each(body)

        lax.fori_loop(1, SIDE, arrive, None)

        def rows(k, _):
            def body(first, on, back, over, pair):
                on(k).wait_recv()
                over(k).start()
                pair(k, 1).start()
                back(k).wait_recv()
                pair(k, 2).start()

            each(body)

        _loop(SIDE, rows)

        def far(k, _):
            def body(first, on, back, over, pair):
                over(k).wait_recv()
                pair(k, 3).start()

            each(body)

        _loop(SIDE, far)

        for group, chips in enumerate((SIDE - 1, SIDE * (SIDE - 1), SIDE * SIDE)):
            ref = self.out.at[:, pl.ds(0, chips), 0]
            send(ref, ref, (self.ssem.at[group], self.ssem.at[3]), self.place.partner).wait_send()
        ref = self.out.at[:, :, 1 - self.place.core]
        send(ref, ref, (self.ssem.at[0], self.ssem.at[3]), self.place.partner).wait_recv()


def adamw(w, m, v, g):
    m = 0.9 * m + 0.1 * g
    v = 0.95 * v + 0.05 * g * g
    step = m * lax.rsqrt(v + 1e-8) + 0.1 * w
    return (w - 0.02 * step).astype(LOW), m, v


def _fetch(refs, held, sem):
    copies = [pltpu.make_async_copy(ref, to, sem.at[n]) for n, (ref, to) in enumerate(zip(refs, held, strict=True))]
    for copy in copies:
        copy.start()
    return copies


def _beside(sums_s, late_rows, layers):
    parts = (pl.ds(0, late_rows), pl.ds(late_rows, sums_s.shape[1] - late_rows))
    return [sums_s.at[layer, part] for part in parts for layer in range(layers)]


def _finish_kernel(shapes, layers, count, *refs):
    many = len(NAMES)
    sums, squares_refs, (table_ref,), ends, w, m, v, outs, (sums_s, sem, stack, end_sem), ends_s, totals, squares_held, w_s, m_s, v_s, part, square_refs, streams = _split(
        refs, 2 * layers - 1, layers, 1, 4, many, many, many, 3, 4, 4, len(EARLY), layers, many, many, many, 9, 3)
    all_ref, own_ref, factor_ref = outs
    squares_s, squares_r, square_sems = square_refs
    found, late_rows, rows = pieces(shapes)
    place = Place()
    steps = ends_s[0].shape[0] // TILE

    def tiles(step):
        rows = _at(step * TILE, TILE)
        return [pltpu.make_async_copy(ref.at[rows], held.at[rows], end_sem.at[step, n]) for n, (ref, held) in enumerate(zip(ends, ends_s))]

    for step in range(steps):
        for copy in tiles(step):
            copy.start()
    to = _beside(sums_s, late_rows, layers)
    own = to.pop(layers)
    loads = _fetch([*sums, *squares_refs, *(x.at[:, place.me] for x in w), *m, *v], [*to, *squares_held, *w_s, *m_s, *v_s], sem)

    def last_gradients():
        def one(step, _):
            for copy in tiles(step):
                copy.wait()
            _start_sums(step, step * TILE, *ends_s, table_ref, totals)

        _loop(steps, one)
        _stack_early(stack, totals, found, late_rows)

    scatter = Scatter(place, stack, part, True)
    meet(neighbours(place, True), last_gradients)
    scatter.begin()
    _loop(2, lambda half, _: scatter.step1(half))
    for load in loads:
        load.wait()
    _loop(2, lambda half, _: scatter.step3(half))
    squares = scatter.end(own_ref)
    own[...] = own_ref[...]
    for ref in squares_held:
        squares += ref[...]
    x, y = place.at

    def share(n, squares):
        others = jnp.where(n == 0, 1, SIDE - 1)
        squares_s[n] = squares

        def to(by):
            chip = jnp.where(n == 1, near(x, by), x) * SIDE + jnp.where(n == 2, near(y, by), y)
            device = jnp.where(n == 0, place.partner, chip * CORES + place.core)
            return send(squares_s.at[n], squares_r.at[n, by], (square_sems.at[0, n, by], square_sems.at[1, n, by]), device)

        lax.fori_loop(1, others + 1, lambda by, _: to(by).start(), None)

        def arrive(by, total):
            to(by).wait()
            return total + squares_r[n, by]

        return lax.fori_loop(1, others + 1, arrive, squares)

    squares = lax.fori_loop(0, 3, share, squares)
    factor = jnp.minimum(1.0, 0.5 * lax.rsqrt(jnp.sum(squares) / count + 1e-30))
    factor_ref[...] = jnp.full(factor_ref.shape, factor, WIDE)

    def new(layer, _):
        for name, row, lane, size, column, columns in found:
            n, here, at = NAMES.index(name), (layer, ALL, pl.ds(column, columns)), (pl.ds(row, size), pl.ds(lane, columns))
            all_ref[(layer, place.chip, place.core, *at)] = adamw(w_s[n][here].astype(WIDE), m_s[n][here], v_s[n][here], sums_s[(layer, *at)].astype(WIDE) * factor)[0]

    _loop(layers, new)
    Gather(place, all_ref, streams).run()
    scatter.sent()


def _outputs_kernel(shapes, layers, *refs):
    many = len(NAMES)
    sums, (own_ref, factor_ref, all_ref), m, v, new_w, new_m, new_v, (sums_s,), m_s, v_s, (sem, out_sem) = _split(
        refs, 2 * layers - 1, 3, many, many, many, many, many, 1, many, many)
    found, late_rows, _ = pieces(shapes)
    to = _beside(sums_s, late_rows, layers)
    to.pop(layers)[...] = own_ref[...]
    loads = _fetch([*sums, *m, *v], [*to, *m_s, *v_s], sem)
    every = ALL
    copies = []
    for name, row, lane, size, column, columns in found:
        copies.append(pltpu.make_async_copy(all_ref.at[:, :, :, pl.ds(row, size), pl.ds(lane, columns)],
                                            new_w[NAMES.index(name)].at[:, :, :, :, pl.ds(column, columns)], out_sem))
        copies[-1].start()
    for load in loads:
        load.wait()
    factor = factor_ref[0:1, 0:1]

    def new(layer, _):
        for name, row, lane, size, column, columns in found:
            n, here = NAMES.index(name), (layer, every, pl.ds(column, columns))
            g = sums_s[layer, pl.ds(row, size), pl.ds(lane, columns)].astype(WIDE) * factor
            _, new_m[n][here], new_v[n][here] = adamw(g, m_s[n][here], v_s[n][here], g)

    _loop(layers, new)
    for copy in copies:
        copy.wait()


def finished(late, early, ends, squares, weights, m, v):
    layers = weights[0].shape[0]
    shapes = {name: w.shape[1:] for name, w in zip(NAMES, weights)}
    _, late_rows, rows = pieces(shapes)
    width = shapes["w_down"][1]
    blocks = [(layers, shapes[name][0] // DEVICES, shapes[name][1]) for name in NAMES]
    whole = pl.BlockSpec(memory_space=pltpu.VMEM)
    mine = rows - late_rows
    held = lambda arrays: [pltpu.VMEM(a.shape, a.dtype) for a in arrays]
    given = [*late, *early[1:], *squares]
    *ends, table = ends
    moments = [*m, *v]
    sums_s = pltpu.VMEM((layers, rows, width), LOW)
    every, own, factor = pl.pallas_call(
        functools.partial(_finish_kernel, shapes, layers, sum(w.size for w in weights)),
        out_shape=[pltpu.VMEM((layers, SIDE * SIDE, CORES, rows, width), LOW), jax.ShapeDtypeStruct((mine, width), LOW), jax.ShapeDtypeStruct((EIGHT, HEAD), WIDE)],
        in_specs=[ANY] * len(given) + [whole] + [ANY] * (len(ends) + len(weights) + len(moments)),
        out_specs=[whole] * 3,
        scratch_shapes=[sums_s, pltpu.SemaphoreType.DMA((len(given) + len(weights) + len(moments),)), pltpu.VMEM((SIDE * SIDE, CORES, mine, width), LOW),
                        pltpu.SemaphoreType.DMA((ends[0].shape[0] // TILE, len(ends)))]
        + held(ends) + [pltpu.VMEM(shapes[n], WIDE) for n in EARLY] + held(squares) + [pltpu.VMEM(b, LOW) for b in blocks] + held(moments)
        + Scatter.scratch(mine, width)
        + [pltpu.VMEM((3, EIGHT, HEAD), WIDE), pltpu.VMEM((3, SIDE, EIGHT, HEAD), WIDE), pltpu.SemaphoreType.DMA((2, 3, SIDE))] + Gather.scratch(),
        compiler_params=pltpu.CompilerParams(collective_id=layers, has_side_effects=True, vmem_limit_bytes=VMEM // 2),
        name="finish",
    )(*(far(x) for x in given), table, *(far(x) for x in (*ends, *(w.reshape(layers, DEVICES, *b[1:]) for w, b in zip(weights, blocks)), *moments)))
    given = [*late, *early[1:]]
    out = pl.pallas_call(
        functools.partial(_outputs_kernel, shapes, layers),
        out_shape=[jax.ShapeDtypeStruct((layers, SIDE * SIDE, CORES, *b[1:]), LOW) for b in blocks] + [jax.ShapeDtypeStruct(b, WIDE) for b in blocks * 2],
        in_specs=[ANY] * len(given) + [whole] * 3 + [ANY] * len(moments),
        out_specs=[ANY] * len(blocks) + [whole] * len(moments),
        scratch_shapes=[sums_s] + held(moments) + [pltpu.SemaphoreType.DMA((len(given) + len(moments),)), pltpu.SemaphoreType.DMA],
        compiler_params=pltpu.CompilerParams(vmem_limit_bytes=VMEM // 6),
        name="outputs",
    )(*(far(x) for x in given), own, factor, pltpu.with_memory_space_constraint(every, pltpu.VMEM), *(far(x) for x in moments))
    return (*(o.reshape(layers, *shapes[name]) for name, o in zip(NAMES, out[:7])), *out[7:])


def solution(mesh):

    def step(x, dy, *arrays):
        weights, m, v, _ = _split(arrays, *[len(NAMES)] * 3)
        return finished(*gradients(x[0], dy[0], dict(zip(NAMES, weights))), weights, m, v)

    states, all_of, cut_rows, many = P(("rep", "dp")), P(), P(None, "dp"), len(NAMES)
    return jax.shard_map(
        step,
        mesh=mesh,
        in_specs=(states, states) + (all_of,) * many + (cut_rows,) * 2 * many,
        out_specs=(P("rep"),) * many + (P("rep", "dp"),) * 2 * many,
        check_vma=False,
    )
```

```python
import functools

import jax
import jax.numpy as jnp
import numpy as np
from jax import lax
from jax.experimental import pallas as pl
from jax.experimental.pallas import tpu as pltpu
from jax.sharding import PartitionSpec as P

NAMES = ("wq", "wk", "wv", "wo", "w_gate", "w_up", "w_down")
HEAD = 128
THETA = 10000
NEG = -1e30
HIDDEN = 2 * NEG
LOG2E = 1.4426950408889634
VMEM = 60 * 2**20
TILE = 512
HALF = TILE // 2
HALVES = (slice(0, HALF), slice(HALF, TILE))
SHORT = 64
AHEAD, BEFORE = 3, 2
EIGHT = 8
PARTS = 3
SCALE = HEAD**-0.5
LOW, WIDE = jnp.bfloat16, jnp.float32
ANY = pl.BlockSpec(memory_space=pl.ANY)
ALL = slice(None)

SIDE, CORES = 4, 2
DEVICES = SIDE * SIDE * CORES
STREAMS = 4
WHERE = pl.DeviceIdType.MESH
LATE, EARLY = ("w_gate", "w_up", "w_down", "wo"), ("wq", "wk", "wv")


def pieces(shapes):
    width, row, found = shapes["w_down"][1], 0, []
    for name in LATE:
        rows, cols = shapes[name][0] // DEVICES, shapes[name][1]
        for column in range(0, cols, width):
            found.append((name, row, 0, rows, column, width))
            row += rows
    late, lane = row, 0
    for name in EARLY:
        rows, cols = shapes[name][0] // DEVICES, shapes[name][1]
        for column in range(0, cols, HEAD):
            found.append((name, row, lane, rows, column, HEAD))
            lane = (lane + HEAD) % width
            row += rows if lane == 0 else 0
    return found, late, row


def shapes_of(w):
    return {name: x.shape[1:] for name, x in w.items()}


def _dot(a, b, ca=1, cb=0):
    return lax.dot_general(a, b, (((ca,), (cb,)), ((), ())), preferred_element_type=WIDE)


def _dot_t(a, b):
    return _dot(a, b, 1, 1)


def _loop(count, body):
    lax.fori_loop(0, count, body, None)


def _at(first, size):
    return pl.ds(pl.multiple_of(first, size), size)


def _part(n, size=HEAD):
    return slice(n * size, n * size + size)


def _step():
    return pl.program_id(0)


def _last():
    return _step() == pl.num_programs(0) - 1


def _seen(shape, queries, ahead=0):
    place = [lax.broadcasted_iota(jnp.int32, shape, axis) for axis in (queries, 1 - queries)]
    return place[0] + ahead >= place[1]


def _split(refs, *counts):
    groups = []
    for count in counts:
        groups.append(refs[:count])
        refs = refs[count:]
    return *groups, refs


def far(x):
    return pltpu.with_memory_space_constraint(x, pltpu.HBM)


def _call(kernel, grid, ins, outs, scratch, name, args, flops, **params):
    moved = sum(a.size * a.dtype.itemsize for a in (*args, *(o[0] for o in outs)))
    return pl.pallas_call(
        kernel,
        grid=grid,
        in_specs=ins,
        out_specs=[o[1] for o in outs],
        out_shape=[o[0] for o in outs],
        scratch_shapes=scratch,
        compiler_params=pltpu.CompilerParams(dimension_semantics=("arbitrary",), vmem_limit_bytes=VMEM, **params),
        cost_estimate=pl.CostEstimate(flops=flops, transcendentals=0, bytes_accessed=moved),
        name=name,
    )(*args)


def _rows(cols):
    return pl.BlockSpec((TILE, cols), lambda i: (i, 0))


def _heads(n):
    return pl.BlockSpec((n, TILE, HEAD), lambda i: (0, i, 0))


def _whole(*shape):
    return pl.BlockSpec(shape, lambda i: (0,) * len(shape))


def _of_layer(w, number):
    return pl.BlockSpec((1, *w.shape[1:]), lambda i: (number, 0, 0))


def _out(shape, dtype, spec):
    return jax.ShapeDtypeStruct(shape, dtype), spec


def _scale(h):
    return lax.rsqrt(jnp.mean(h * h, -1, keepdims=True) + 1e-6)


def _turn(t, cos, sin):
    t = t.astype(WIDE)
    return (t * cos + pltpu.roll(t, HEAD // 2, 1) * sin).astype(LOW)


def turns(tokens):
    half = HEAD // 2
    places = np.concatenate([np.arange(SHORT), np.arange(0, tokens, SHORT)])
    angle = places[:, None] * float(THETA) ** (-np.arange(half) / half)
    return jnp.asarray(np.concatenate([np.cos(angle), np.sin(angle)], 1), WIDE)


def _both(t):
    r = pltpu.roll(t, HEAD // 2, 1)
    first = lax.broadcasted_iota(jnp.int32, t.shape, 1) < HEAD // 2
    return jnp.where(first, t, r), jnp.where(first, -r, t)


def _turns(table_ref, step):
    cos, sin = _both(table_ref[:SHORT, :])
    many = TILE // SHORT
    far = _both(table_ref[pl.ds(pl.multiple_of(SHORT + step * many, many), many), :])
    coses, sines = [], []
    for n in range(many):
        far_cos, far_sin = (t[n : n + 1, :] for t in far)
        coses.append(far_cos * cos - far_sin * sin)
        sines.append(far_sin * cos + far_cos * sin)
    return jnp.concatenate(coses, 0), jnp.concatenate(sines, 0)


def _project(h, wq_ref, wk_ref, wv_ref, table_ref, q_ref, k_ref, v_ref):
    cos, sin = _turns(table_ref, _step())
    for here in HALVES:
        a = (h[here] * _scale(h[here])).astype(LOW)
        q = _dot(a, wq_ref[0]).astype(LOW)
        for n in range(q_ref.shape[0]):
            q_ref[n, here, :] = _turn(q[:, _part(n)], cos[here], sin[here])
        k_ref[here, :] = _turn(_dot(a, wk_ref[0]).astype(LOW), cos[here], sin[here])
        v_ref[here, :] = _dot(a, wv_ref[0]).astype(LOW)


def _first_kernel(h_ref, *refs):
    _project(h_ref[...].astype(WIDE), *refs)


def _qkv_outs(tokens, heads):
    return [_out((heads, tokens, HEAD), LOW, _heads(heads))] + [_out((tokens, HEAD), LOW, _rows(HEAD))] * 2


def first(h, w, number, table):
    tokens, d = h.shape
    args = [h, w["wq"], w["wk"], w["wv"], table]
    cols = w["wq"].shape[2]
    return _call(_first_kernel, (tokens // TILE,), [_rows(d)] + [_of_layer(x, number) for x in args[1:4]] + [_whole(*table.shape)],
                 _qkv_outs(tokens, cols // HEAD), [], "first", args, 2 * tokens * d * (cols + 2 * HEAD))


def _attend_kernel(q_ref, k_ref, v_ref, o_ref, turned_ref, qt_ref, lse_ref, top_s, mix_s):
    heads = q_ref.shape[0]
    block_q = _step()
    e = SCALE * LOG2E
    top_s[...] = jnp.full(top_s.shape, NEG, WIDE)
    mix_s[...] = jnp.zeros(mix_s.shape, WIDE)
    def block(first_half, halves, low, masked):
        size = halves * HALF
        here = _at(first_half * HALF, size)
        k, values = k_ref[here, :], jnp.concatenate([v_ref[here, :].T, jnp.ones((EIGHT, size), LOW)])
        if masked:
            ok = _seen((size, TILE - low), 1)
        score = lambda n: _dot_t(k, q_ref[n, low:, :])
        ready = [score(n) for n in range(AHEAD)]
        for n in range(heads):
            if n + AHEAD < heads:
                ready.append(score(n + AHEAD))
            s = jnp.where(ok, ready[n], HIDDEN) if masked else ready[n]
            row = slice(n, n + 1)
            old = top_s[row, low:]
            top = jnp.maximum(old, s.max(0, keepdims=True))
            top_s[row, low:] = top
            mix_s[n, :, low:] = mix_s[n, :, low:] * jnp.exp2((old - top) * e) + _dot(values, jnp.exp2((s - top) * e).astype(LOW))

    _loop(block_q, lambda j, _: block(2 * j, 2, 0, False))
    block(2 * block_q, 1, 0, True)
    block(2 * block_q + 1, 1, HALF, True)
    for n in range(heads):
        total, row = mix_s[n, HEAD : HEAD + 1, :], slice(n, n + 1)
        turned = (mix_s[n, :HEAD, :] * (1 / total)).astype(LOW)
        turned_ref[_part(n), :] = turned
        o_ref[:, _part(n)] = turned.T
        qt_ref[n] = q_ref[n].T
        lse_ref[row, :] = top_s[row, :] * SCALE + jnp.log(total)
    lse_ref[heads:, :] = jnp.zeros((EIGHT - heads, TILE), WIDE)


def _columns(rows):
    return pl.BlockSpec((rows, TILE), lambda i: (0, i))


def _head_columns(heads):
    return pl.BlockSpec((heads, HEAD, TILE), lambda i: (0, 0, i))


def attend(q, k, v):
    heads, tokens, _ = q.shape
    inner = heads * HEAD
    return _call(_attend_kernel, (tokens // TILE,), [_heads(heads), _whole(tokens, HEAD), _whole(tokens, HEAD)],
                 [_out((tokens, inner), LOW, _rows(inner)), _out((inner, tokens), LOW, _columns(inner)),
                  _out((heads, HEAD, tokens), LOW, _head_columns(heads)), _out((EIGHT, tokens), WIDE, _columns(EIGHT))],
                 [pltpu.VMEM((heads, TILE), WIDE), pltpu.VMEM((heads, HEAD + EIGHT, TILE), WIDE)],
                 "attend", [q, k, v], 2 * heads * tokens * tokens * HEAD)


def _attend_back_kernel(many, refs):
    ins, stacks, (dq_ref, dk_ref, dv_ref), sums, (squares_ref,), held, refs = _split(refs, 8, many, 3, many, 1, 5)
    q_ref, qt_ref, k_ref, v_ref, do_ref, dot_ref, lse_ref, delta_ref = ins
    dq_s, dk_s, dv_s, beside_s, take_s = held
    heads = q_ref.shape[0]
    block_q = _step()
    steps = k_ref.shape[0] // TILE
    e = SCALE * LOG2E
    place = Place()
    parts = [Scatter(place, s, refs[_part(at, 9)]) for at, s in enumerate(stacks)]

    def travel(step, tick, *ticks):
        one, other = (n * steps * steps // 16 for n in ticks)

        if parts:
            @pl.when((tick == one) | (tick == other))
            def _():
                for part in parts:
                    getattr(part, step)(jnp.where(tick == other, 1, 0))

    @pl.when(block_q == 0)
    def _():
        for part in parts:
            part.load()
        if parts:
            meet(neighbours(place))
        for part in parts:
            part.begin()
        lane = lax.broadcasted_iota(jnp.int32, (HALF, HEAD), 1)

        def clear(n, _):
            dk_s[n] = jnp.zeros((HEAD, HALF), WIDE)
            dv_s[n] = jnp.zeros((HEAD, HALF), WIDE)

        def take(n, _):
            for which in range(2):
                mine = (lane % EIGHT == n) & (lane // (EIGHT * PARTS) == which)
                take_s[which, n] = jnp.where(mine, -1.0, 0.0).astype(LOW)

        _loop(2 * steps, clear)
        _loop(heads, take)

    dq_s[...] = jnp.zeros_like(dq_s)
    of = lambda n: (ALL, _part(n))
    lines = []
    for rest in (lse_ref[...] * (1 / SCALE), delta_ref[...]):
        for _ in range(PARTS):
            lines.append(rest.astype(LOW).astype(WIDE))
            rest = rest - lines[-1]
    lines.append(jnp.zeros((HEAD - EIGHT * len(lines), TILE), WIDE))
    beside_s[...] = jnp.concatenate(lines).T.astype(LOW)

    def block(keys, low):
        here = _at(keys * HALF, HALF)
        k, v = k_ref[here, :], v_ref[here, :]
        ok = _seen((TILE - low, HALF), 0, (2 * block_q - keys) * HALF + low)
        beside = lambda x: jnp.concatenate([x, beside_s[low:, :]], 1)
        score = lambda n: (_dot_t(beside(q_ref[n, low:, :]), jnp.concatenate([k, take_s[0, n]], 1)),
                           _dot_t(beside(do_ref[low:, _part(n)]), jnp.concatenate([v, take_s[1, n]], 1)))
        ready = [score(n) for n in range(BEFORE)]
        dk, dv = None, None
        for n in range(heads):
            if n + BEFORE < heads:
                ready.append(score(n + BEFORE))
            s, dp = ready[n]
            p = jnp.where(ok, jnp.exp2(s * e), 0.0)
            ds = (p * dp).astype(LOW)
            more_v, more_k = _dot(dot_ref[_part(n), low:], p.astype(LOW)), _dot(qt_ref[n, :, low:], ds)
            dv, dk = (dv + more_v, dk + more_k) if n else (more_v, more_k)
            dq_s[n, low:, :] += _dot(ds, k)
        dk_s[keys] += dk
        dv_s[keys] += dv

    def one(j, _):
        tick = block_q * block_q + j
        travel("step1", tick, 3, 4)
        travel("step2", tick, 7, 9)
        travel("step3", tick, 11, 13)
        travel("step4", tick, 14, 15)
        block(j, 0)

    _loop(2 * block_q + 1, one)
    block(2 * block_q + 1, HALF)
    for n in range(heads):
        dq_ref[of(n)] = (dq_s[n] * SCALE).astype(LOW)

    @pl.when(block_q == steps - 1)
    def _():
        def turn(n, _):
            here = _at(n * HALF, HALF)
            dk_ref[here, :] = (dk_s[n] * SCALE).T.astype(LOW)
            dv_ref[here, :] = dv_s[n].T.astype(LOW)

        _loop(2 * steps, turn)
        squares_ref[...] = sum((part.end(out) for part, out in zip(parts, sums)), jnp.zeros((EIGHT, HEAD), WIDE))
        for part in parts:
            part.sent()


def attend_back(q, qt, k, v, do, dot, lse, delta, stacks, number):
    heads, tokens, _ = q.shape
    wide, kv = _rows(heads * HEAD), _whole(tokens, HEAD)
    rows = [s.shape[2] for s in stacks]
    width = stacks[0].shape[3] if stacks else HEAD
    scratch = [pltpu.VMEM((heads, TILE, HEAD), WIDE)] + [pltpu.VMEM((tokens // HALF, HEAD, HALF), WIDE)] * 2
    scratch += [pltpu.VMEM((TILE, HEAD), LOW), pltpu.VMEM((2, heads, HALF, HEAD), LOW)]
    got = _call(lambda *refs: _attend_back_kernel(len(rows), refs), (tokens // TILE,),
                [_heads(heads), _head_columns(heads), kv, kv, wide, _columns(heads * HEAD)] + [_columns(EIGHT)] * 2 + [ANY] * len(rows),
                [_out((tokens, heads * HEAD), LOW, wide)] + [_out((tokens, HEAD), LOW, kv)] * 2
                + [_out((n, width), LOW, _whole(n, width)) for n in rows] + [_out((EIGHT, HEAD), WIDE, _whole(EIGHT, HEAD))],
                scratch + [s for n in rows for s in Scatter.scratch(n, width)],
                "attend_back", [q, qt, k, v, do, dot, lse, delta, *(far(s) for s in stacks)], 5 * heads * tokens * tokens * HEAD, collective_id=number, has_side_effects=True)
    return got[:3], got[3:-1], got[-1]


class Chunks:
    @staticmethod
    def scratch(d, hidden):
        n = hidden // TILE
        return [pltpu.VMEM((n, d, TILE), LOW)] * 2 + [pltpu.VMEM((n, TILE, d), LOW), pltpu.SemaphoreType.DMA((n, 3))]

    def __init__(self, number, refs, held):
        self.number, self.refs, self.held, self.sem = number, refs, held[:3], held[3]
        self.count = held[0].shape[0]

    def copies(self, c):
        units = _at(c * TILE, TILE)
        return [pltpu.make_async_copy(ref.at[at], held.at[c], self.sem.at[c, n]) for n, (ref, held, at) in enumerate(
            zip(self.refs, self.held, ((self.number, ALL, units), (self.number, ALL, units), (self.number, units, ALL))))]

    def fetch(self):
        @pl.when(_step() == 0)
        def _():
            for c in range(self.count):
                for copy in self.copies(c):
                    copy.start()

    def chunk(self, c):
        @pl.when(_step() == 0)
        def _():
            for copy in self.copies(c):
                copy.wait()

        return [held[c] for held in self.held]


def _slot(n):
    return lax.rem(n, 2)


class Passing:
    @staticmethod
    def scratch(many):
        return [pltpu.VMEM((2, TILE, TILE), WIDE)] * many + [pltpu.SemaphoreType.DMA((2, many))]

    def __init__(self, refs, held, out):
        self.refs, self.held, self.sem, self.out = refs, held[:-1], held[-1], out
        self.count = refs[0].shape[0]
        self.first, self.total = _step() * self.count, pl.num_programs(0) * self.count

    def _each(self, n):
        slot, chunk, rows = _slot(n), lax.rem(n, self.count), _at(lax.div(n, self.count) * TILE, TILE)
        for at, (ref, held) in enumerate(zip(self.refs, self.held)):
            ends = (held.at[slot], ref.at[chunk, rows, :])
            yield pltpu.make_async_copy(*(ends if self.out else ends[::-1]), self.sem.at[slot, at])

    def start(self, n):
        for copy in self._each(n):
            copy.start()

    def wait(self, n):
        for copy in self._each(n):
            copy.wait()


def _after_attention(o_ref, h_ref, wo_ref):
    return (h_ref[...].astype(WIDE) + _dot(o_ref[...], wo_ref[0]).astype(LOW).astype(WIDE)).astype(LOW)


def _middle_kernel(number, o_ref, h_ref, wo_ref, wg_ref, wu_ref, wd_ref, wq_ref, wk_ref, wv_ref, table_ref, mid_ref, next_ref, q_ref, k_ref, v_ref,
                   gate_ref, up_ref, b_s, total_s, *held):
    held, passed = _split(held, 4)
    chunks, passing = Chunks(number, (wg_ref, wu_ref, wd_ref), held), Passing((gate_ref, up_ref), passed, True)
    chunks.fetch()
    mid_ref[...] = _after_attention(o_ref, h_ref, wo_ref)
    mid = mid_ref[...].astype(WIDE)
    b_s[...] = (mid * _scale(mid)).astype(LOW)
    total_s[...] = jnp.zeros_like(total_s)

    def one(c, _):
        wg, wu, wd = chunks.chunk(c)
        n = passing.first + c
        pl.when(n > 1)(lambda: passing.wait(n - 2))
        gate, up = _dot(b_s[...], wg), _dot(b_s[...], wu)
        for slots, value in zip(passing.held, (gate, up)):
            slots[_slot(n)] = value
        total_s[...] += _dot((gate * jax.nn.sigmoid(gate) * up).astype(LOW), wd)
        passing.start(n)

    def two(c, _):
        one(2 * c, _)
        one(2 * c + 1, _)

    _loop(chunks.count // 2, two)
    after = (mid_ref[...].astype(WIDE) + total_s[...].astype(LOW).astype(WIDE)).astype(LOW)
    next_ref[...] = after
    _project(after.astype(WIDE), wq_ref, wk_ref, wv_ref, table_ref, q_ref, k_ref, v_ref)
    for left in (2, 1):
        pl.when(_last())(lambda: passing.wait(passing.first + chunks.count - left))


def middle(o, h, w, number, table):
    tokens, d = h.shape
    args = [o, h, w["wo"], *(far(w[n]) for n in ("w_gate", "w_up", "w_down")), *(w[n] for n in EARLY), table]
    specs = [_rows(o.shape[1]), _rows(d), _of_layer(w["wo"], number)] + [ANY] * 3
    specs += [_of_layer(w[n], number + 1) for n in ("wq", "wk", "wv")] + [_whole(*table.shape)]
    size = sum(x.size for x in w.values()) // w["wq"].shape[0]
    hidden = w["w_gate"].shape[2]
    return _call(functools.partial(_middle_kernel, number), (tokens // TILE,), specs,
                 [_out((tokens, d), LOW, _rows(d))] * 2 + _qkv_outs(tokens, o.shape[1] // HEAD) + [_out((hidden // TILE, tokens, TILE), WIDE, ANY)] * 2,
                 [pltpu.VMEM((TILE, d), LOW), pltpu.VMEM((TILE, d), WIDE)] + Chunks.scratch(d, hidden) + Passing.scratch(2),
                 "middle", args, 2 * tokens * size)


def _back_kernel(number, last, found, dy_ref, o_ref, turned_ref, h_ref, wo_ref, wg_ref, wu_ref, wd_ref, gate_ref, up_ref, dh_ref, do_ref, dot_ref, delta_ref, stack_ref,
                 mid_s, b_s, bt_s, dyt_s, db_s, wo_s, gate_s, up_s, down_s, out_s, out_sem, *held):
    first = _step() == 0
    held, passed = _split(held, 4)
    chunks, passing = Chunks(number, (wg_ref, wu_ref, wd_ref), held), None
    if not last:
        passing = Passing((gate_ref, up_ref), passed, False)
        pl.when(first)(lambda: passing.start(0))
    chunks.fetch()
    mid_s[...] = (_after_attention(o_ref, h_ref, wo_ref) if last else h_ref[...]).astype(WIDE)
    scale = _scale(mid_s[...])
    b = (mid_s[...] * scale).astype(LOW)
    b_s[...] = b
    bt_s[...] = b.T
    dyt_s[...] = dy_ref[...].T
    db_s[...] = jnp.zeros_like(db_s)

    def add(ref, at, more):
        ref[at] = jnp.where(first, 0.0, ref[at]) + more

    def one(c, _):
        wg, wu, wd = chunks.chunk(c)
        if last:
            gate, up = _dot(b_s[...], wg), _dot(b_s[...], wu)
        else:
            n = passing.first + c
            pl.when(n < passing.total - 1)(lambda: passing.start(n + 1))
            passing.wait(n)
            gate, up = (slots[_slot(n)] for slots in passing.held)
        dact = _dot_t(dy_ref[...], wd).astype(LOW).astype(WIDE)
        some = jax.nn.sigmoid(gate)
        silu = gate * some
        act = (silu * up).astype(LOW)
        dup = (dact * silu).astype(LOW)
        dgate = (dact * up * (some + silu * (1 - some))).astype(LOW)
        add(down_s, c, _dot(dyt_s[...], act))
        add(gate_s, c, _dot(bt_s[...], dgate))
        add(up_s, c, _dot(bt_s[...], dup))
        db_s[...] += _dot_t(dgate, wg) + _dot_t(dup, wu)

    _loop(chunks.count, one)
    dh = _norm_back(dy_ref[...].astype(WIDE), mid_s[...], scale, db_s[...])
    dh_ref[...] = dh
    do_ref[...] = _dot_t(dh, wo_ref[0]).astype(LOW)
    add(wo_s, ALL, _dot(turned_ref[...], dh))
    dot_ref[...] = do_ref[...].T
    heads = dot_ref.shape[0] // HEAD
    for n in range(heads):
        delta_ref[n : n + 1, :] = (dot_ref[_part(n), :].astype(WIDE) * turned_ref[_part(n), :].astype(WIDE)).sum(0, keepdims=True)
    delta_ref[heads:, :] = jnp.zeros((EIGHT - heads, TILE), WIDE)

    @pl.when(_last())
    def _():
        row = {name: (at, rows) for name, at, _, rows, column, _ in found if not column}
        every = ALL
        many = TILE // row["w_down"][1]

        def copies(c):
            for name in ("w_gate", "w_up", "w_down"):
                at, rows = row[name]
                here = (_at(c * many, many), pl.ds(at, rows)) if name == "w_down" else (every, pl.ds(pl.multiple_of(at + c * rows, EIGHT), rows))
                yield here, pltpu.make_async_copy(out_s.at[here], stack_ref.at[here], out_sem.at[c])

        def put(c, _):
            for (here, copy), value in zip(copies(c), (gate_s[c], up_s[c], down_s[c].T)):
                out_s[here] = value.reshape(-1, here[1].size, value.shape[1]).astype(LOW)
                copy.start()

        _loop(chunks.count, put)
        at, rows = row["wo"]
        here = (every, pl.ds(at, rows))
        out_s[here] = wo_s[...].reshape(DEVICES, rows, wo_s.shape[1]).astype(LOW)
        copy = pltpu.make_async_copy(out_s.at[here], stack_ref.at[here], out_sem.at[chunks.count])
        copy.start()
        for c in range(chunks.count):
            for _, some in copies(c):
                some.wait()
        copy.wait()


def _norm_back(dy, h, scale, db):
    return (dy + scale * (db - h * (scale * scale * jnp.mean(db * h, -1, keepdims=True)))).astype(LOW)


def back(dy, o, turned, h, gates, w, number, last):
    tokens, d = dy.shape
    args = [dy, o if last else far(o), turned, h, w["wo"], *(far(w[n]) for n in ("w_gate", "w_up", "w_down")), *gates]
    inner, hidden = o.shape[1], w["w_gate"].shape[2]
    n = hidden // TILE
    found, late, _ = pieces(shapes_of(w))
    scratch = [pltpu.VMEM((TILE, d), WIDE), pltpu.VMEM((TILE, d), LOW)] + [pltpu.VMEM((d, TILE), LOW)] * 2 + [pltpu.VMEM((TILE, d), WIDE)]
    scratch += [pltpu.VMEM((inner, d), WIDE)] + [pltpu.VMEM((n, d, TILE), WIDE)] * 3 + [pltpu.VMEM((DEVICES, late, d), LOW)]
    scratch += [pltpu.SemaphoreType.DMA((n + 1,))]
    return _call(functools.partial(_back_kernel, number, last, found), (tokens // TILE,),
                 [_rows(d), _rows(inner) if last else ANY, _columns(inner), _rows(d), _of_layer(w["wo"], number)] + [ANY] * 5,
                 [_out((tokens, d), LOW, _rows(d)), _out((tokens, inner), LOW, _rows(inner)), _out((inner, tokens), LOW, _columns(inner)),
                  _out((EIGHT, tokens), WIDE, _columns(EIGHT)), _out((DEVICES, late, d), LOW, ANY)],
                 scratch + Chunks.scratch(d, hidden) + ([] if last else Passing.scratch(2)), "back", args, 6 * tokens * d * (inner + 3 * hidden))


def _start_sums(step, at, h_ref, dq_ref, dk_ref, dv_ref, table_ref, sums, backs=None):
    cos, sin = _turns(table_ref, step)
    more_by = [None] * len(sums)
    for half in HALVES:
        rows = _at(at + half.start, HALF)
        h = h_ref[rows, :].astype(WIDE)
        scale = _scale(h)
        a_turned = (h * scale).astype(LOW).T
        dq = jnp.concatenate([_turn(dq_ref[rows, _part(n)], cos[half], -sin[half]) for n in range(dq_ref.shape[1] // HEAD)], 1)
        dk, dv = _turn(dk_ref[rows, :], cos[half], -sin[half]), dv_ref[rows, :]
        by = [_dot(a_turned, x) for x in (dq, dk, dv)]
        more_by = [x if y is None else x + y for x, y in zip(by, more_by)]
        if backs:
            dh_ref, wq_ref, wk_ref, wv_ref, dx_ref = backs
            da = _dot_t(dq, wq_ref[0]) + _dot_t(dk, wk_ref[0]) + _dot_t(dv, wv_ref[0])
            dx_ref[rows, :] = _norm_back(dh_ref[rows, :].astype(WIDE), h, scale, da)
    for s, by in zip(sums, more_by):
        s[...] = jnp.where(step == 0, 0.0, s[...]) + by


def _stack_early(stack_ref, sums, found, late):
    for name, row, lane, rows, column, columns in found:
        if name in EARLY:
            value = sums[EARLY.index(name)][:, pl.ds(column, columns)]
            stack_ref[..., pl.ds(row - late, rows), pl.ds(lane, columns)] = value.reshape(*stack_ref.shape[:-2], rows, columns).astype(LOW)


def _start_kernel(found, late, *refs):
    ins, backs, (stack_ref,), sums = _split(refs, 5, 5, 1)
    _start_sums(_step(), 0, *ins, sums, backs)
    pl.when(_last())(lambda: _stack_early(stack_ref, sums, found, late))


def start(h, dq, dk, dv, table, dh, w, number):
    tokens, d = h.shape
    found, late, rows = pieces(shapes_of(w))
    weights = [w[n] for n in EARLY]
    specs = [_rows(d), _rows(dq.shape[1])] + [_rows(HEAD)] * 2 + [_whole(*table.shape), _rows(d)] + [_of_layer(x, number) for x in weights]
    stack = (DEVICES, rows - late, d)
    return _call(functools.partial(_start_kernel, found, late), (tokens // TILE,), specs, [_out((tokens, d), LOW, _rows(d)), _out(stack, LOW, _whole(*stack))],
                 [pltpu.VMEM(x.shape[1:], WIDE) for x in weights], "start", [h, dq, dk, dv, table, dh, *weights], 4 * tokens * sum(x[0].size for x in weights))


def gradients(x, dy, w):
    layers = w["wq"].shape[0]
    table = turns(x.shape[0])
    kept, h = [], x
    q, k, v = first(x, w, 0, table)
    for number in range(layers):
        o, turned, qt, lse = attend(q, k, v)
        kept.append([h, q, k, v, o, turned, qt, lse])
        if number < layers - 1:
            mid, h, q, k, v, *gates = middle(o, h, w, number, table)
            kept[number] += [mid, gates]
        else:
            kept[number] += [h, [h, h]]
    late, early, squares, waiting = [None] * layers, [None] * layers, [], []
    by_device = lambda stack: stack.reshape(SIDE * SIDE, CORES, *stack.shape[1:])
    for number in reversed(range(layers)):
        h, q, k, v, o, turned, qt, lse, mid, gates = kept[number]
        dh, do, dot, delta, stack = back(dy, o, turned, mid, gates, w, number, number == layers - 1)
        (dq, dk, dv), sums, square = attend_back(q, qt, k, v, do, dot, lse, delta, [by_device(stack), *waiting], number)
        late[number] = sums[0]
        if waiting:
            early[number + 1] = sums[1]
        squares.append(square)
        if number:
            dy, stack = start(h, dq, dk, dv, table, dh, w, number)
            waiting = [by_device(stack)]
    return late, early, (h, dq, dk, dv, table), squares


class Place:
    def __init__(self):
        self.me = lax.axis_index("dp")
        self.core, self.chip = lax.rem(self.me, CORES), lax.div(self.me, CORES)
        self.at = (lax.div(self.chip, SIDE), lax.rem(self.chip, SIDE))
        self.partner = self.me + 1 - 2 * self.core

    def along(self, axis, by):
        x, y = (lax.rem(p + SIDE + by, SIDE) if a == axis else p for a, p in enumerate(self.at))
        return (x * SIDE + y) * CORES + self.core

    def shifted(self, axis, by):
        return lax.rem(self.at[axis] + SIDE + by, SIDE)


def neighbours(place, two=False):
    found = [place.partner] + [place.along(axis, by) for axis in range(2) for by in (1, -1)]
    return found + [place.along(axis, 2) for axis in range(2)] if two else found


def meet(devices, between=None):
    barrier = pltpu.get_barrier_semaphore()
    for d in devices:
        pl.semaphore_signal(barrier, inc=1, device_id={"dp": d}, device_id_type=WHERE)
    if between:
        between()
    pl.semaphore_wait(barrier, len(devices))


def send(src, dst, sems, device):
    return pltpu.make_async_remote_copy(src_ref=src, dst_ref=dst, send_sem=sems[0], recv_sem=sems[1], device_id={"dp": device}, device_id_type=WHERE)


class Streams:
    def __init__(self, place):
        self.place = place

    def of(self, s):
        axis, way = lax.rem(s, 2), 1 - 2 * lax.div(s, 2)
        x, y = self.place.at
        across, down = SIDE - (SIDE - 1) * axis, 1 + (SIDE - 1) * axis
        return x + axis * (y - x), y + axis * (x - y), way, lambda i, j: i * across + j * down

    def device(self, chip):
        return chip * CORES + self.place.core


def near(place, by):
    return lax.rem(place + SIDE + by, SIDE)


class Scatter(Streams):
    @staticmethod
    def scratch(rows, width):
        chips, n = SIDE * SIDE, STREAMS
        shapes = [(chips, rows, width)] * 2 + [(n, 3, SIDE, rows, width // n)] * 2 + [(n, 3, rows, width // n)] * 2
        return [pltpu.VMEM(s, LOW) for s in shapes] + [pltpu.SemaphoreType.DMA((3,)), pltpu.SemaphoreType.DMA((n, 6)), pltpu.SemaphoreType.DMA((2, 2))]

    def __init__(self, place, given, scratch, direct=False):
        super().__init__(place)
        self.given, self.direct = given, direct
        self.straight = tuple(range(3))[not direct :]
        self.own, self.pair, self.s1, self.r1, self.s2, self.r2, self.ssem, self.rsem, self.sem = scratch
        self.rows, self.width = self.pair.shape[1:]

    def _half(self, half):
        size = self.width // 2
        return _at(half * size, size)

    def _pair(self, half):
        lanes = self._half(half)
        return send(self.given.at[:, 1 - self.place.core, :, lanes], self.pair.at[ALL, ALL, lanes], (self.ssem.at[2], self.sem.at[half, 0]), self.place.partner)

    def _load(self, half):
        lanes = self._half(half)
        return pltpu.make_async_copy(self.given.at[:, self.place.core, :, lanes], self.own.at[ALL, ALL, lanes], self.sem.at[half, 1])

    def _stream(self, s):
        a, b, way, number = self.of(s)
        lanes = _at(s * HEAD, HEAD)
        along = (way, -way, 2) if self.direct else (way, -way, way)

        def move(n):
            axis, n = divmod(n, 3)
            to = number(a, near(b, along[n])) if axis else number(near(a, along[n]), b)
            src, dst, at = (self.s2, self.r2, n + 3) if axis else (self.s1, self.r1, n)
            return send(src.at[s, n], dst.at[s, n], (self.ssem.at[axis], self.rsem.at[s, at]), self.device(to))

        def chip(i, j):
            n = number(i, j)
            own = self.given[n, self.place.core, :, lanes] if self.direct else self.own[n, :, lanes]
            return own.astype(WIDE) + self.pair[n, :, lanes].astype(WIDE)

        def row(j):
            terms = self.straight
            return sum((self.r1[s, n, j].astype(WIDE) for n in terms), chip(a, j))

        return a, b, way, move, lanes, chip, row

    def _each(self, half, body):
        lax.fori_loop(2 * half, 2 * half + 2, lambda s, _: body(s, *self._stream(s)), None)

    def load(self):
        _loop(2, lambda half, _: self._load(half).start())

    def begin(self):
        _loop(2, lambda half, _: self._pair(half).start())

    def step1(self, half):
        if not self.direct:
            self._load(half).wait()
        self._pair(half).wait_recv()

        def body(s, a, b, way, move, lanes, chip, row):
            to = (near(a, way), near(a, -way), near(a, 2)) if self.direct else (near(a, 2), near(a, -way))

            def one(j, _):
                for n, i in enumerate(to):
                    self.s1[s, n, j] = chip(i, j).astype(LOW)

            _loop(SIDE, one)
            for n in range(len(to)):
                move(n).start()

        self._each(half, body)

    def step2(self, half):
        def body(s, a, b, way, move, lanes, chip, row):
            move(0).wait_recv()

            def one(j, _):
                self.s1[s, 2, j] = (chip(near(a, way), j) + self.r1[s, 0, j].astype(WIDE)).astype(LOW)

            _loop(SIDE, one)
            move(2).start()

        self._each(half, body)

    def step3(self, half):
        def body(s, a, b, way, move, lanes, chip, row):
            for n in self.straight:
                move(n).wait_recv()
            to = (near(b, way), near(b, -way), near(b, 2)) if self.direct else (near(b, 2), near(b, -way))
            for n, j in enumerate(to):
                self.s2[s, n] = row(j).astype(LOW)
                move(3 + n).start()

        self._each(half, body)

    def step4(self, half):
        def body(s, a, b, way, move, lanes, chip, row):
            move(3).wait_recv()
            self.s2[s, 2] = (row(near(b, way)) + self.r2[s, 0].astype(WIDE)).astype(LOW)
            move(5).start()

        self._each(half, body)

    def end(self, out):
        def body(s, squares):
            a, b, way, move, lanes, chip, row = self._stream(s)
            terms = self.straight
            for n in terms:
                move(3 + n).wait_recv()
            out[:, lanes] = sum((self.r2[s, n].astype(WIDE) for n in terms), row(b)).astype(LOW)
            wide = out[:, lanes].astype(WIDE)
            return squares + (wide * wide).reshape(self.rows // EIGHT, EIGHT, HEAD).sum(0)

        return lax.fori_loop(0, STREAMS, body, jnp.zeros((EIGHT, HEAD), WIDE))

    def sent(self):
        for n, ref in enumerate((self.s1, self.s2, self.pair)):
            send(ref, ref, (self.ssem.at[n], self.rsem.at[0, 0]), self.place.partner).wait_send()


class Gather(Streams):
    @staticmethod
    def scratch():
        return [pltpu.SemaphoreType.DMA((4,)), pltpu.SemaphoreType.DMA((STREAMS, 15))]

    def __init__(self, place, out, scratch):
        super().__init__(place)
        self.out, (self.ssem, self.rsem) = out, scratch

    def _move(self, s, group, n, chip, to):
        ref = self.out.at[:, chip, self.place.core, :, _at(s * HEAD, HEAD)]
        return send(ref, ref, (self.ssem.at[group], self.ssem.at[3] if group == 2 else self.rsem.at[s, n]), to)

    def _stream(self, s):
        a, b, way, number = self.of(s)
        place = lambda p, k: near(p, jnp.where(k == 1, -way, jnp.where(k == 2, way, jnp.where(k == 3, 2, 0))))
        on1, back1, on2, back2 = number(near(a, way), b), number(near(a, -way), b), number(a, near(b, way)), number(a, near(b, -way))
        first = lambda n: self._move(s, 0, n, number(place(a, jnp.where(n == 2, 1, 0)), b), self.device(jnp.where(n == 1, back1, on1)))
        on = lambda k: self._move(s, 1, 3 + k, number(place(a, k), b), self.device(on2))
        back = lambda k: self._move(s, 1, 7 + k, number(place(a, k), b), self.device(back2))
        over = lambda k: self._move(s, 1, 11 + k, number(place(a, k), near(b, -way)), self.device(on2))
        pair = lambda k, r: self._move(s, 2, 0, number(place(a, k), place(b, r)), self.place.partner)
        return first, on, back, over, pair

    def run(self):
        def each(body):
            _loop(STREAMS, lambda s, _: body(*self._stream(s)))

        def spread(on, back, pair, k):
            on(k).start()
            back(k).start()
            pair(k, 0).start()

        def own(first, on, back, over, pair):
            first(0).start()
            first(1).start()

        each(own)
        each(lambda first, on, back, over, pair: spread(on, back, pair, 0))

        def arrive(k, _):
            def body(first, on, back, over, pair):
                first(k - 1).wait_recv()

                @pl.when(k == 1)
                def _():
                    first(2).start()

                spread(on, back, pair, k)

            each(body)

        lax.fori_loop(1, SIDE, arrive, None)

        def rows(k, _):
            def body(first, on, back, over, pair):
                on(k).wait_recv()
                over(k).start()
                pair(k, 1).start()
                back(k).wait_recv()
                pair(k, 2).start()

            each(body)

        _loop(SIDE, rows)

        def far(k, _):
            def body(first, on, back, over, pair):
                over(k).wait_recv()
                pair(k, 3).start()

            each(body)

        _loop(SIDE, far)

        for group, chips in enumerate((SIDE - 1, SIDE * (SIDE - 1), SIDE * SIDE)):
            ref = self.out.at[:, pl.ds(0, chips), 0]
            send(ref, ref, (self.ssem.at[group], self.ssem.at[3]), self.place.partner).wait_send()
        ref = self.out.at[:, :, 1 - self.place.core]
        send(ref, ref, (self.ssem.at[0], self.ssem.at[3]), self.place.partner).wait_recv()


def adamw(w, m, v, g):
    m = 0.9 * m + 0.1 * g
    v = 0.95 * v + 0.05 * g * g
    step = m * lax.rsqrt(v + 1e-8) + 0.1 * w
    return (w - 0.02 * step).astype(LOW), m, v


def _fetch(refs, held, sem):
    copies = [pltpu.make_async_copy(ref, to, sem.at[n]) for n, (ref, to) in enumerate(zip(refs, held, strict=True))]
    for copy in copies:
        copy.start()
    return copies


def _beside(sums_s, late_rows, layers):
    parts = (pl.ds(0, late_rows), pl.ds(late_rows, sums_s.shape[1] - late_rows))
    return [sums_s.at[layer, part] for part in parts for layer in range(layers)]


def _finish_kernel(shapes, layers, count, *refs):
    many = len(NAMES)
    sums, squares_refs, (table_ref,), ends, w, m, v, outs, (sums_s, sem, stack, end_sem), ends_s, totals, squares_held, w_s, m_s, v_s, part, square_refs, streams = _split(
        refs, 2 * layers - 1, layers, 1, 4, many, many, many, 3, 4, 4, len(EARLY), layers, many, many, many, 9, 3)
    all_ref, own_ref, factor_ref = outs
    squares_s, squares_r, square_sems = square_refs
    found, late_rows, rows = pieces(shapes)
    place = Place()
    steps = ends_s[0].shape[0] // TILE

    def tiles(step):
        rows = _at(step * TILE, TILE)
        return [pltpu.make_async_copy(ref.at[rows], held.at[rows], end_sem.at[step, n]) for n, (ref, held) in enumerate(zip(ends, ends_s))]

    for step in range(steps):
        for copy in tiles(step):
            copy.start()
    to = _beside(sums_s, late_rows, layers)
    own = to.pop(layers)
    loads = _fetch([*sums, *squares_refs, *(x.at[:, place.me] for x in w), *m, *v], [*to, *squares_held, *w_s, *m_s, *v_s], sem)

    def last_gradients():
        def one(step, _):
            for copy in tiles(step):
                copy.wait()
            _start_sums(step, step * TILE, *ends_s, table_ref, totals)

        _loop(steps, one)
        _stack_early(stack, totals, found, late_rows)

    scatter = Scatter(place, stack, part, True)
    meet(neighbours(place, True), last_gradients)
    scatter.begin()
    _loop(2, lambda half, _: scatter.step1(half))
    for load in loads:
        load.wait()
    _loop(2, lambda half, _: scatter.step3(half))
    squares = scatter.end(own_ref)
    own[...] = own_ref[...]
    for ref in squares_held:
        squares += ref[...]
    x, y = place.at

    def share(n, squares):
        others = jnp.where(n == 0, 1, SIDE - 1)
        squares_s[n] = squares

        def to(by):
            chip = jnp.where(n == 1, near(x, by), x) * SIDE + jnp.where(n == 2, near(y, by), y)
            device = jnp.where(n == 0, place.partner, chip * CORES + place.core)
            return send(squares_s.at[n], squares_r.at[n, by], (square_sems.at[0, n, by], square_sems.at[1, n, by]), device)

        lax.fori_loop(1, others + 1, lambda by, _: to(by).start(), None)

        def arrive(by, total):
            to(by).wait()
            return total + squares_r[n, by]

        return lax.fori_loop(1, others + 1, arrive, squares)

    squares = lax.fori_loop(0, 3, share, squares)
    factor = jnp.minimum(1.0, 0.5 * lax.rsqrt(jnp.sum(squares) / count + 1e-30))
    factor_ref[...] = jnp.full(factor_ref.shape, factor, WIDE)

    def new(layer, _):
        for name, row, lane, size, column, columns in found:
            n, here, at = NAMES.index(name), (layer, ALL, pl.ds(column, columns)), (pl.ds(row, size), pl.ds(lane, columns))
            all_ref[(layer, place.chip, place.core, *at)] = adamw(w_s[n][here].astype(WIDE), m_s[n][here], v_s[n][here], sums_s[(layer, *at)].astype(WIDE) * factor)[0]

    _loop(layers, new)
    Gather(place, all_ref, streams).run()
    scatter.sent()


def _outputs_kernel(shapes, layers, *refs):
    many = len(NAMES)
    sums, (own_ref, factor_ref, all_ref), m, v, new_w, new_m, new_v, (sums_s,), m_s, v_s, (sem, out_sem) = _split(
        refs, 2 * layers - 1, 3, many, many, many, many, many, 1, many, many)
    found, late_rows, _ = pieces(shapes)
    to = _beside(sums_s, late_rows, layers)
    to.pop(layers)[...] = own_ref[...]
    loads = _fetch([*sums, *m, *v], [*to, *m_s, *v_s], sem)
    every = ALL
    copies = []
    for name, row, lane, size, column, columns in found:
        copies.append(pltpu.make_async_copy(all_ref.at[:, :, :, pl.ds(row, size), pl.ds(lane, columns)],
                                            new_w[NAMES.index(name)].at[:, :, :, :, pl.ds(column, columns)], out_sem))
        copies[-1].start()
    for load in loads:
        load.wait()
    factor = factor_ref[0:1, 0:1]

    def new(layer, _):
        for name, row, lane, size, column, columns in found:
            n, here = NAMES.index(name), (layer, every, pl.ds(column, columns))
            g = sums_s[layer, pl.ds(row, size), pl.ds(lane, columns)].astype(WIDE) * factor
            _, new_m[n][here], new_v[n][here] = adamw(g, m_s[n][here], v_s[n][here], g)

    _loop(layers, new)
    for copy in copies:
        copy.wait()


def finished(late, early, ends, squares, weights, m, v):
    layers = weights[0].shape[0]
    shapes = {name: w.shape[1:] for name, w in zip(NAMES, weights)}
    _, late_rows, rows = pieces(shapes)
    width = shapes["w_down"][1]
    blocks = [(layers, shapes[name][0] // DEVICES, shapes[name][1]) for name in NAMES]
    whole = pl.BlockSpec(memory_space=pltpu.VMEM)
    mine = rows - late_rows
    held = lambda arrays: [pltpu.VMEM(a.shape, a.dtype) for a in arrays]
    given = [*late, *early[1:], *squares]
    *ends, table = ends
    moments = [*m, *v]
    sums_s = pltpu.VMEM((layers, rows, width), LOW)
    every, own, factor = pl.pallas_call(
        functools.partial(_finish_kernel, shapes, layers, sum(w.size for w in weights)),
        out_shape=[pltpu.VMEM((layers, SIDE * SIDE, CORES, rows, width), LOW), jax.ShapeDtypeStruct((mine, width), LOW), jax.ShapeDtypeStruct((EIGHT, HEAD), WIDE)],
        in_specs=[ANY] * len(given) + [whole] + [ANY] * (len(ends) + len(weights) + len(moments)),
        out_specs=[whole] * 3,
        scratch_shapes=[sums_s, pltpu.SemaphoreType.DMA((len(given) + len(weights) + len(moments),)), pltpu.VMEM((SIDE * SIDE, CORES, mine, width), LOW),
                        pltpu.SemaphoreType.DMA((ends[0].shape[0] // TILE, len(ends)))]
        + held(ends) + [pltpu.VMEM(shapes[n], WIDE) for n in EARLY] + held(squares) + [pltpu.VMEM(b, LOW) for b in blocks] + held(moments)
        + Scatter.scratch(mine, width)
        + [pltpu.VMEM((3, EIGHT, HEAD), WIDE), pltpu.VMEM((3, SIDE, EIGHT, HEAD), WIDE), pltpu.SemaphoreType.DMA((2, 3, SIDE))] + Gather.scratch(),
        compiler_params=pltpu.CompilerParams(collective_id=layers, has_side_effects=True, vmem_limit_bytes=VMEM // 2),
        name="finish",
    )(*(far(x) for x in given), table, *(far(x) for x in (*ends, *(w.reshape(layers, DEVICES, *b[1:]) for w, b in zip(weights, blocks)), *moments)))
    given = [*late, *early[1:]]
    out = pl.pallas_call(
        functools.partial(_outputs_kernel, shapes, layers),
        out_shape=[jax.ShapeDtypeStruct((layers, SIDE * SIDE, CORES, *b[1:]), LOW) for b in blocks] + [jax.ShapeDtypeStruct(b, WIDE) for b in blocks * 2],
        in_specs=[ANY] * len(given) + [whole] * 3 + [ANY] * len(moments),
        out_specs=[ANY] * len(blocks) + [whole] * len(moments),
        scratch_shapes=[sums_s] + held(moments) + [pltpu.SemaphoreType.DMA((len(given) + len(moments),)), pltpu.SemaphoreType.DMA],
        compiler_params=pltpu.CompilerParams(vmem_limit_bytes=VMEM // 6),
        name="outputs",
    )(*(far(x) for x in given), own, factor, pltpu.with_memory_space_constraint(every, pltpu.VMEM), *(far(x) for x in moments))
    return (*(o.reshape(layers, *shapes[name]) for name, o in zip(NAMES, out[:7])), *out[7:])


def solution(mesh):

    def step(x, dy, *arrays):
        weights, m, v, _ = _split(arrays, *[len(NAMES)] * 3)
        return finished(*gradients(x[0], dy[0], dict(zip(NAMES, weights))), weights, m, v)

    states, all_of, cut_rows, many = P(("rep", "dp")), P(), P(None, "dp"), len(NAMES)
    return jax.shard_map(
        step,
        mesh=mesh,
        in_specs=(states, states) + (all_of,) * many + (cut_rows,) * 2 * many,
        out_specs=(P("rep"),) * many + (P("rep", "dp"),) * 2 * many,
        check_vma=False,
    )
```
